32 devices in a mesh: slab: 4 (over y, core), pencil: 8 (over z, x).
Axes of the slice: x: 2, y: 2, z: 4, core: 2. Of those that a mesh axis runs over, the one named last changes fastest.
Arguments:
- density: float32 [128, 768, 512], P('pencil', None, 'slab'), may hold values from -6 to 6
- source: float32 [128, 768, 512], P('pencil', None, 'slab'), may hold values from -6 to 8
- coupling: float32 [3], replicated, may hold values from 0.25 to 2, as said below
- width_inverse: float32 [6, 128, 128], replicated, as said below
- height_inverse: float32 [1, 128, 128], replicated, as said below
- depth_inverse: float32 [4, 128, 128], replicated, as said below
Outputs:
- stepped: float32 [128, 768, 512], P('pencil', None, 'slab')
The draws below stay inside these ranges and needn't reach their ends.
Inputs may be any that keep to these rules, and one draw needn't show every extreme that they name: coupling holds three positive coefficients. `width_inverse`: block i is the inverse of the i-th pivot block of the block LU factorization of the tridiagonal line matrix with diagonal 1 + 2 s and off-diagonals -s, s the matching coupling. `height_inverse`: as for width_inverse, for the height lines. `depth_inverse`: as for width_inverse, for the depth lines.
All inputs are finite; a program needn't handle non-finite values.
Results may differ from the reference program's by a relative error of at most 0.00027.
Values sent between devices are 32-bit elements; how exact they have to be, the bound alone decides.
A program may use at most 128 MiB of HBM per device.

```python
import jax
import jax.numpy as jnp
from jax import lax

BLOCK = 128
NX = 768
NY = 128
NZ = 512


def coupling_values(key):
    folded = jax.random.fold_in(key, 7)
    uniform_draw = jax.random.uniform(folded, (3,), jnp.float32)
    return 0.25 * jnp.exp(uniform_draw * jnp.log(8.0))


def block_inverses(strength, count):
    identity = jnp.eye(BLOCK, dtype=jnp.float32)
    beside = jnp.eye(BLOCK, k=1, dtype=jnp.float32) + jnp.eye(BLOCK, k=-1, dtype=jnp.float32)
    tridiag = (1.0 + 2.0 * strength) * identity - strength * beside
    corner_unit = jnp.zeros((BLOCK, BLOCK), jnp.float32).at[0, 0].set(1.0)
    matrices = []
    corner = jnp.float32(0.0)
    for number in range(count):
        pivot = tridiag - strength * strength * corner * corner_unit
        inverse = jnp.linalg.inv(pivot)
        matrices.append(inverse)
        corner = inverse[BLOCK - 1, BLOCK - 1]
    return jnp.stack(matrices)


def draw_source(key, part):
    rough = jnp.clip(jax.random.normal(jax.random.fold_in(key, 11), (NY, NX, NZ), jnp.float32), -6.0, 6.0)
    return rough


def draw_coupling(key, part):
    return coupling_values(key)


def draw_width_inverse(key, part):
    return block_inverses(coupling_values(key)[0], NX // BLOCK)


def draw_height_inverse(key, part):
    return block_inverses(coupling_values(key)[1], NY // BLOCK)


def draw_depth_inverse(key, part):
    return block_inverses(coupling_values(key)[2], NZ // BLOCK)


def levels(own_key, dims, split, low, largest):
    def one(position, parts):
        heights = jax.random.uniform(jax.random.fold_in(jax.random.fold_in(own_key, 6), position), (parts,), jnp.float32, low / len(split), largest / len(split))
        return jnp.repeat(jnp.exp(heights), dims[position] // parts).reshape((-1,) + (1,) * (len(dims) - position - 1))

    gain = one(*split[0])
    for cut in split[1:]:
        gain = gain * one(*cut)
    return gain


def bell_draw(own_key, extent, deviation, most, pieces=(), kind=jnp.bfloat16):
    values = jax.random.normal(own_key, extent, jnp.float32) * deviation
    if len(pieces) > 0:
        values = levels(own_key, extent, pieces, -0.22, 0.18) * values
    return jnp.clip(values, min=-most, max=most).astype(kind)


def setup_inputs(seed: int = 0) -> dict:
    streams_of = jax.random.split(jax.random.key(seed), 7)
    return {
        "density": bell_draw(streams_of[0], (NY, NX, NZ), 1.0, 6.0, ((0, 8), (2, 4)), jnp.float32),
        "source": draw_source(jax.random.fold_in(streams_of[6], 71), 0),
        "coupling": draw_coupling(jax.random.fold_in(streams_of[6], 71), 0),
        "width_inverse": draw_width_inverse(jax.random.fold_in(streams_of[6], 71), 0),
        "height_inverse": draw_height_inverse(jax.random.fold_in(streams_of[6], 71), 0),
        "depth_inverse": draw_depth_inverse(jax.random.fold_in(streams_of[6], 71), 0),
    }


def solve_inner(rhs, inverses, strength):
    outer, length, inner = rhs.shape
    size = inverses.shape[1]
    count = length // size
    blocked = rhs.reshape(outer, count, size, inner)

    def forward(current, state):
        result, carry = state
        piece = lax.dynamic_index_in_dim(blocked, current, 1, keepdims=False)
        matrix = lax.dynamic_index_in_dim(inverses, current, 0, keepdims=False)
        value = jnp.einsum('pkq,jk->pjq', piece, matrix, precision=lax.Precision.HIGHEST)
        value = value + strength * matrix[:, 0][None, :, None] * carry[:, None, :]
        result = lax.dynamic_update_index_in_dim(result, value, current, 1)
        return (result, value[:, size - 1, :])
    start = (jnp.zeros_like(blocked), jnp.zeros((outer, inner), blocked.dtype))
    halfway, unused = lax.fori_loop(0, count, forward, start)

    def backward(step, state):
        result, carry = state
        current = count - 1 - step
        value = lax.dynamic_index_in_dim(result, current, 1, keepdims=False)
        matrix = lax.dynamic_index_in_dim(inverses, current, 0, keepdims=False)
        value = value + strength * matrix[:, size - 1][None, :, None] * carry[:, None, :]
        result = lax.dynamic_update_index_in_dim(result, value, current, 1)
        return (result, value[:, 0, :])
    final, unused = lax.fori_loop(0, count, backward, (halfway, jnp.zeros((outer, inner), blocked.dtype)))
    return final.reshape(outer, length, inner)

def solve_last(rhs, inverses, strength):
    rows, length = rhs.shape
    size = inverses.shape[1]
    count = length // size
    blocked = rhs.reshape(rows, count, size)

    def forward(current, state):
        result, carry = state
        piece = lax.dynamic_index_in_dim(blocked, current, 1, keepdims=False)
        matrix = lax.dynamic_index_in_dim(inverses, current, 0, keepdims=False)
        value = jnp.einsum('pk,jk->pj', piece, matrix, precision=lax.Precision.HIGHEST)
        value = value + strength * matrix[:, 0][None, :] * carry[:, None]
        result = lax.dynamic_update_index_in_dim(result, value, current, 1)
        return (result, value[:, size - 1])
    halfway, unused = lax.fori_loop(0, count, forward, (jnp.zeros_like(blocked), jnp.zeros((rows,), blocked.dtype)))

    def backward(step, state):
        result, carry = state
        current = count - 1 - step
        value = lax.dynamic_index_in_dim(result, current, 1, keepdims=False)
        matrix = lax.dynamic_index_in_dim(inverses, current, 0, keepdims=False)
        value = value + strength * matrix[:, size - 1][None, :] * carry[:, None]
        result = lax.dynamic_update_index_in_dim(result, value, current, 1)
        return (result, value[:, 0])
    final, unused = lax.fori_loop(0, count, backward, (halfway, jnp.zeros((rows,), blocked.dtype)))
    return final.reshape(rows, length)

def second_difference(values, axis):
    widths = [(0, 0), (0, 0), (0, 0)]
    widths[axis] = (1, 1)
    padded = jnp.pad(values, widths)
    length = values.shape[axis]
    upper = lax.slice_in_dim(padded, 2, length + 2, axis=axis)
    lower = lax.slice_in_dim(padded, 0, length, axis=axis)
    return upper + lower - 2.0 * values

def reference(density, source, coupling, width_inverse, height_inverse, depth_inverse):
    along_width = second_difference(density, 1)
    along_height = second_difference(density, 0)
    along_depth = second_difference(density, 2)
    explicit = 2.0 * (coupling[0] * along_width + coupling[1] * along_height + coupling[2] * along_depth) + source
    width_step = solve_inner(explicit, width_inverse, coupling[0])
    height_step = solve_inner(width_step.reshape(1, NY, NX * NZ), height_inverse, coupling[1]).reshape(NY, NX, NZ)
    depth_step = solve_last(height_step.reshape(NY * NX, NZ), depth_inverse, coupling[2]).reshape(NY, NX, NZ)
    return density + depth_step
```

```python
import jax
import jax.numpy as jnp
from jax import lax
from jax.experimental import pallas as pl
from jax.experimental.pallas import tpu as pltpu
from jax.sharding import PartitionSpec as P

F32, BF16 = jnp.float32, jnp.bfloat16
MESH = pl.DeviceIdType.MESH


def split(value):
    high = value.astype(BF16)
    return high, (value - high.astype(F32)).astype(BF16)


def both(value, axis):
    return jnp.concatenate(split(value), axis=axis)


def dot(a, b, dims):
    return lax.dot_general(a, b, (dims, ((), ())), preferred_element_type=F32)


def ends_of(plane):
    width, depth = plane.shape
    row = lax.broadcasted_iota(jnp.int32, (depth, depth), 0)
    lane = lax.broadcasted_iota(jnp.int32, (depth, depth), 1)
    lines = []
    for column in (0, depth - 1):
        pieces = []
        for start in range(0, width, depth):
            edge = plane[start : start + depth, column : column + 1]
            pieces.append(jnp.sum(jnp.where(row == lane, edge, 0.0), axis=0, keepdims=True))
        lines.append(jnp.concatenate(pieces, axis=1))
    return jnp.concatenate(lines, axis=0)


def rows_of(pieces, width):
    row = lax.broadcasted_iota(jnp.int32, (16, width), 0)
    value = jnp.zeros((16, width), F32)
    for number, piece in enumerate(pieces):
        value = jnp.where(row == number, piece.astype(F32), value)
    return value.astype(BF16)


def solve_group(rhs, strength, width_ref, mixed_ref, depth_mixed):
    count, size = width_ref.shape[:2]
    depth = size
    total = rhs.shape[1]
    high, low = split(rhs)
    local, starts, stops = [], [], []
    for i in range(count):
        part = slice(i * size, (i + 1) * size)
        product = dot(mixed_ref[i], jnp.concatenate([high[part], low[part]], 0), ((1,), (0,)))
        local.append(product[:size] + product[size:])
        starts.append(strength * width_ref[i, :, 0:1])
        stops.append(strength * width_ref[i, :, size - 1 : size])
    carry = jnp.zeros((1, total), F32)
    ahead, heads = [], []
    for i in range(count):
        ahead.append(carry)
        heads.append(local[i][0:1] + starts[i][0:1] * carry)
        carry = local[i][size - 1 :] + starts[i][size - 1 :] * carry
    carry = jnp.zeros((1, total), F32)
    solved = [None] * count
    for i in reversed(range(count)):
        solved[i] = local[i] + starts[i] * ahead[i] + stops[i] * carry
        carry = heads[i] + stops[i][0:1] * carry
    solved = jnp.concatenate(solved, axis=0)
    answers = []
    for start in range(0, total, depth):
        product = dot(both(solved[:, start : start + depth], 1), depth_mixed, ((1,), (0,)))
        answers.append(product[:, :depth] + product[:, depth:])
    return answers


class Heights:
    def __init__(self, strength, lanes):
        self.shape = (1, lanes)
        self.strength = jnp.full(self.shape, strength, F32)
        root = (1.0 + 2.0 * self.strength + jnp.sqrt(1.0 + 4.0 * self.strength)) * 0.5
        self.log_ratio = jnp.log(self.strength / root)

    def power(self, index):
        return jnp.exp(jnp.full(self.shape, index, jnp.int32).astype(F32) * self.log_ratio)

    def tail(self, count):
        return 1.0 - self.power(2 * count)

    def beside(self, count):
        return self.power(1) * self.tail(count) / self.tail(count + 1)

    def enter(self, count, j):
        return self.power(j + 1) * self.tail(count - j) / self.tail(count + 1)


def rows_solve(pieces, strength, width_ref, mixed_ref):
    count, size = width_ref.shape[:2]
    local = []
    for i in range(count):
        product = dot(both(pieces[i], 1), mixed_ref[i], ((1,), (1,)))
        local.append(product[:, :size] + product[:, size:])
    carry = jnp.zeros((pieces[0].shape[0], 1), F32)
    ahead, heads = [], []
    for i in range(count):
        start = strength * width_ref[i, 0:1]
        ahead.append(start * carry)
        heads.append(local[i][:, 0:1] + start[:, 0:1] * carry)
        carry = local[i][:, size - 1 :] + start[:, size - 1 :] * carry
    carry = jnp.zeros((pieces[0].shape[0], 1), F32)
    solved = [None] * count
    for i in reversed(range(count)):
        stop = strength * width_ref[i, size - 1 : size]
        solved[i] = local[i] + ahead[i] + stop * carry
        carry = heads[i] + stop[:, 0:1] * carry
    return solved


def step_kernel(
    group, pencils, slabs, chunk,
    coupling,
    rho_hbm, source_hbm, width_ref, depth_ref,
    z_ref, face_ref, coef_ref,
    rho_ref, source_ref, y_ref, mixed_ref, mixed_depth,
    pair_out, pair_in, block, up_out, up_in, down_out, down_in, back_out, final,
    ends, gathered, carries, late, late_in,
    load_sem, pair_send, pair_recv, up_send, up_recv, down_send, down_recv,
    back_send, back_recv, early_send, early_recv, late_send, late_recv,
):
    planes, width, depth = z_ref.shape
    groups = planes // group
    count, size = width_ref.shape[:2]
    half = width // 2
    seg = final.shape[1] // 2
    extra = seg - half
    chunks = seg // chunk
    strips = half // depth
    pad = 8
    me, slab = lax.axis_index("pencil"), lax.axis_index("slab")
    outer = pencils // 2
    z, x = lax.div(me, 2), lax.rem(me, 2)
    pair = z * 2 + 1 - x
    above_me = lax.rem(me + 2, pencils)
    below_me = lax.rem(me + pencils - 2, pencils)

    barrier = pltpu.get_barrier_semaphore()
    for peer in (pair, above_me, below_me):
        pl.semaphore_signal(barrier, inc=1, device_id={"pencil": peer}, device_id_type=MESH)
    for k in range(1, slabs):
        pl.semaphore_signal(
            barrier, inc=1, device_id={"slab": lax.rem(slab + k, slabs)}, device_id_type=MESH
        )

    loads = {}

    def load(key, src, dst, start, rows, shift):
        number = loads.setdefault(key, len(loads))
        return pltpu.make_async_copy(
            src.at[:, pl.ds(pl.multiple_of(start, 8), rows)],
            dst.at[:, pl.ds(pl.multiple_of(start + shift, 8), rows)],
            load_sem.at[number],
        )

    def rim(h, side):
        start = h * half + side * (half - 8)
        return load(("rim", h, side), rho_hbm, rho_ref, start, 8, pad)

    def main(turn, h, piece):
        low = 8 if piece == 0 else piece * depth
        high = half - 8 if piece == strips - 1 else (piece + 1) * depth
        return load(("rho", turn, piece), rho_hbm, rho_ref, h * half + low, high - low, pad)

    def other(turn, h, piece):
        start = h * half + piece * depth
        return load(("source", turn, piece), source_hbm, source_ref, start, depth, 0)

    for h in (0, 1):
        for side in (0, 1):
            rim(h, side).start()
    for turn, h in ((0, 1 - x), (1, x)):
        for piece in range(strips):
            main(turn, h, piece).start()
            other(turn, h, piece).start()

    rho_ref[:, :pad] = jnp.zeros((planes, pad, depth), F32)
    rho_ref[:, pad + width :] = jnp.zeros((planes, pad, depth), F32)
    for i in range(count):
        high, low = split(width_ref[i])
        mixed_ref[i, :size, :size] = high
        mixed_ref[i, :size, size:] = high
        mixed_ref[i, size:, :size] = low
        mixed_ref[i, size:, size:] = jnp.zeros_like(low)
    high, low = split(depth_ref[slab])
    mixed_depth[:size, :size] = high
    mixed_depth[size:, :size] = high
    mixed_depth[:size, size:] = low
    mixed_depth[size:, size:] = jnp.zeros_like(low)

    heights = Heights(coupling[1], depth)
    for j in range(planes):
        coef_ref[j : j + 1] = heights.enter(planes, j)
    strength = heights.strength
    ahead = [heights.beside(j + 1) for j in range(planes)]
    pivot = [value / strength for value in ahead]
    near, far = heights.enter(planes, 0), heights.enter(planes, planes - 1)
    gain = 1.0 / (1.0 - near * near)
    near2, far2 = heights.enter(2 * planes, 0), heights.enter(2 * planes, 2 * planes - 1)
    under = heights.beside(2 * planes * z)
    over = heights.beside(2 * planes * (outer - 1 - z))
    under_gain, over_gain = 1.0 / (1.0 - under * near2), 1.0 / (1.0 - over * near2)
    det = 1.0 / ((1.0 - under * near2) * (1.0 - over * near2) - under * over * far2 * far2)
    k_uu, k_uo = (1.0 - over * near2) * det, under * far2 * det
    k_oo, k_ou = (1.0 - under * near2) * det, over * far2 * det

    lane = lax.broadcasted_iota(jnp.int32, (1, depth), 1)
    across, along = coupling[0], coupling[2]
    k_here = 2.0 - 4.0 * across - 4.0 * along
    k_before = jnp.where(lane == 0, 0.0, jnp.full((1, depth), 2.0 * along, F32))
    k_after = jnp.where(lane == depth - 1, 0.0, jnp.full((1, depth), 2.0 * along, F32))

    def back_sweep(at, value):
        for j in reversed(range(planes)):
            if j == planes - 1:
                y = pivot[j] * value
            else:
                y = pivot[j] * (y_ref[j, at] + strength * y)
            y_ref[j, at] = y
        return y

    def sweep(h, row, rows):
        base = pl.multiple_of(pad + h * half + row, 8)
        at = pl.ds(pl.multiple_of(h * seg + row, 8), rows)
        from_source = pl.ds(pl.multiple_of(h * half + row, 8), rows)
        value = None
        for j in range(planes):
            rho = rho_ref[j, pl.ds(base, rows)]
            beside = rho_ref[j, pl.ds(base - 1, rows)] + rho_ref[j, pl.ds(base + 1, rows)]
            rhs = (
                source_ref[j, from_source]
                + k_here * rho
                + (2.0 * across) * beside
                + k_before * pltpu.roll(rho, 1, 1)
                + k_after * pltpu.roll(rho, depth - 1, 1)
            )
            value = rhs if j == 0 else rhs + ahead[j - 1] * value
            y_ref[j, at] = value
        last = pivot[planes - 1] * value
        first = back_sweep(at, value)
        return first, last

    def edge_sweep(h):
        at = pl.ds(pl.multiple_of(h * seg + half, 8), extra)
        value = None
        row = lax.broadcasted_iota(jnp.int32, (depth, depth), 0)
        column = lax.broadcasted_iota(jnp.int32, (depth, depth), 1)

        def gather(j, unused):
            lines = []
            for edge in (0, depth - 1):
                for strip in range(strips):
                    start = pl.multiple_of(pad + h * half + strip * depth, 8)
                    piece = rho_ref[j, pl.ds(start, depth)][:, edge : edge + 1]
                    lines.append(jnp.sum(jnp.where(row == column, piece, 0.0), axis=0, keepdims=True))
            lines.append(jnp.zeros((extra - 2 * strips, depth), F32))
            y_ref[j, at] = jnp.concatenate(lines, axis=0)
            return unused

        lax.fori_loop(0, planes, gather, 0)
        for j in range(planes):
            rhs = y_ref[j, at]
            value = rhs if j == 0 else rhs + ahead[j - 1] * value
            y_ref[j, at] = value
        last = pivot[planes - 1] * value
        first = back_sweep(at, value)
        return first, last

    def remote(source, target, send, recv, peer, axis="pencil"):
        return pltpu.make_async_remote_copy(
            src_ref=source, dst_ref=target, send_sem=send, recv_sem=recv,
            device_id={axis: peer}, device_id_type=MESH,
        )

    def rows_at(c, shift=0):
        return pl.ds(pl.multiple_of(c * chunk + shift, 8), chunk)

    def to_pair(c):
        at = rows_at(c)
        return remote(
            pair_out.at[:, at], pair_in.at[:, at], pair_send.at[c], pair_recv.at[c], pair
        )

    def to_above(c):
        at = rows_at(c)
        return remote(up_out.at[at], up_in.at[at], up_send.at[c], up_recv.at[c], above_me)

    def to_below(c):
        at = rows_at(c)
        return remote(
            down_out.at[at], down_in.at[at], down_send.at[c], down_recv.at[c], below_me
        )

    def to_back(c):
        return remote(
            back_out.at[:, rows_at(c)], final.at[:, rows_at(c, x * seg)],
            back_send.at[c], back_recv.at[c], pair,
        )

    for turn, h in ((0, 1 - x), (1, x)):
        if turn == 0:
            for hh in (0, 1):
                for side in (0, 1):
                    rim(hh, side).wait()
        ready = 0
        for c in range(chunks):
            need = min(strips, -(-(c * chunk + chunk + 1) // depth))
            while ready < need:
                main(turn, h, ready).wait()
                other(turn, h, ready).wait()
                ready += 1
            row = c * chunk
            at = pl.ds(row, min(chunk, half - row))
            first, last = sweep(h, row, min(chunk, half - row))
            if turn == 0:
                pair_out[0, at] = first
                pair_out[1, at] = last
            if c == chunks - 1:
                at = pl.ds(half, extra)
                first, last = edge_sweep(h)
                if turn == 0:
                    pair_out[0, at] = first
                    pair_out[1, at] = last
            if turn == 0:
                if c == 0:
                    pl.semaphore_wait(barrier, 3 + slabs - 1)
                to_pair(c).start()

    @pl.when(z == 0)
    def _():
        up_in[...] = jnp.zeros_like(up_in)

    @pl.when(z == outer - 1)
    def _():
        down_in[...] = jnp.zeros_like(down_in)

    def faces_of(c):
        at, mine = rows_at(c), rows_at(c, x * seg)
        own_first, own_last = y_ref[0, mine], y_ref[planes - 1, mine]
        its_first, its_last = pair_in[0, at], pair_in[1, at]
        lower = x == 0
        return (
            jnp.where(lower, own_first, its_first),
            jnp.where(lower, own_last, its_last),
            jnp.where(lower, its_first, own_first),
            jnp.where(lower, its_last, own_last),
        )

    def do_pair(c):
        to_pair(c).wait_recv()
        at = rows_at(c)
        f0, l0, f1, l1 = faces_of(c)
        block[0, at] = f0 + far * gain * (f1 + near * l0)
        block[1, at] = l1 + far * gain * (l0 + near * f1)

    def do_up(c):
        @pl.when(z > 0)
        def _():
            to_above(c).wait_recv()

        at = rows_at(c)

        @pl.when(z < outer - 1)
        def _():
            up_out[at] = block[1, at] + far2 * under_gain * (up_in[at] + under * block[0, at])
            to_above(c).start()

    def do_down(c):
        @pl.when(z < outer - 1)
        def _():
            to_below(c).wait_recv()

        at = rows_at(c)

        @pl.when(z > 0)
        def _():
            down_out[at] = block[0, at] + far2 * over_gain * (down_in[at] + over * block[1, at])
            to_below(c).start()

    def do_final(c):
        at, mine = rows_at(c), rows_at(c, x * seg)
        low = up_in[at] + under * block[0, at]
        high = down_in[at] + over * block[1, at]
        enter = k_uu * low + k_uo * high
        leave = k_ou * low + k_oo * high
        f0, l0, f1, l1 = faces_of(c)
        l0 = l0 + far * enter
        f1 = f1 + far * leave
        inner_low = gain * (l0 + near * f1)
        inner_high = gain * (f1 + near * l0)
        lower = x == 0
        final[0, mine] = jnp.where(lower, enter, inner_low)
        final[1, mine] = jnp.where(lower, inner_high, leave)
        back_out[0, at] = jnp.where(lower, inner_low, enter)
        back_out[1, at] = jnp.where(lower, leave, inner_high)
        to_back(c).start()

    def blocks_at(i):
        return pl.ds(i // strips * seg + i % strips * size, size)

    def solve_planes(index):
        base = index * group
        rhs = jnp.concatenate(
            [
                jnp.concatenate(
                    [
                        y_ref[base + g, blocks_at(i)]
                        - 2.0 * rho_ref[base + g, pl.ds(pad + i * size, size)]
                        for i in range(count)
                    ],
                    axis=0,
                )
                for g in range(group)
            ],
            axis=1,
        )
        answers = solve_group(rhs, coupling[0], width_ref, mixed_ref, mixed_depth[...])
        for g in range(group):
            z_ref[base + g] = answers[g] + rho_ref[base + g, pl.ds(pad, width)]
            lines = ends_of(answers[g])
            ends[0, pl.ds(base + g, 1)] = lines[0:1]
            ends[1, pl.ds(base + g, 1)] = lines[1:2]

    before_me = jnp.where(slab > 0, slab - 1, 0)
    corner = depth_ref[before_me, size - 1 : size, size - 1 : size]
    corner = jnp.where(slab > 0, corner, jnp.zeros_like(corner))

    def link(d, row, column):
        return coupling[2] * depth_ref[d, row : row + 1, column : column + 1]

    def with_edges(edge, ends_value, v_first, v_own):
        row = 0 if edge == 0 else size - 1
        return ends_value + 2.0 * v_own + (2.0 * coupling[2] * corner * link(slab, row, 0)) * v_first

    def early_edges():
        pieces = []
        for i in range(count):
            h, strip = i // strips, i % strips
            rows = [
                y_ref[:, h * seg + half + edge * strips + strip, :] for edge in (0, 1)
            ]
            pieces.append(jnp.concatenate(rows, axis=0))
        value = jnp.concatenate(rows_solve(pieces, coupling[0], width_ref, mixed_ref), axis=1)
        first, last = value[:planes], value[planes:]
        carries[0] = first
        ends[0] = with_edges(0, ends[0], first, first)
        ends[1] = with_edges(1, ends[1], first, last)
        for k in range(1, slabs):
            early(k).start()
        gathered[slab] = ends[...]

    def early(k):
        return remote(
            ends, gathered.at[slab], early_send.at[k - 1], early_recv.at[k - 1],
            lax.rem(slab + k, slabs), "slab",
        )

    def last_link(k):
        return remote(
            late.at[pl.ds(0, 4)], late_in.at[slab, pl.ds(0, 4)],
            late_send.at[k - 1], late_recv.at[k - 1],
            lax.rem(slab + k, slabs), "slab",
        )

    def chain(first_of, last_of, v_first):
        zero = jnp.zeros_like(v_first)
        forward = [zero]
        for d in range(slabs - 1):
            forward.append(last_of(d) + link(d, size - 1, 0) * forward[d])
        backward = [zero] * slabs
        for d in range(slabs - 1, 0, -1):
            backward[d - 1] = (
                first_of(d) + link(d, 0, 0) * forward[d] + link(d, 0, size - 1) * backward[d]
            )
        carry_in, carry_next = forward[0], backward[0]
        for d in range(1, slabs):
            carry_in = jnp.where(slab == d, forward[d], carry_in)
            carry_next = jnp.where(slab == d, backward[d], carry_next)
        return carry_in + (2.0 * coupling[2] * corner) * v_first, carry_next

    def spread(carry_in, carry_next):
        in_high, in_low = split(coupling[2] * depth_ref[slab, 0:1])
        next_high, next_low = split(coupling[2] * depth_ref[slab, size - 1 : size])
        rhs = rows_of((in_high, in_high, in_low, next_high, next_high, next_low), depth)
        a_high, a_low = split(carry_in)
        b_high, b_low = split(carry_next)
        lhs = rows_of((a_high, a_low, a_high, b_high, b_low, b_high), width)
        return dot(lhs, rhs, ((0,), (0,)))

    per_tick = 2
    busy = -(-groups // per_tick)
    ticks = max(chunks + outer - 1, busy + 1)

    def tick(t, unused):
        @pl.when(t < chunks)
        def _():
            do_pair(t)

        up = t - z

        @pl.when((up >= 0) & (up < chunks))
        def _():
            do_up(up)

        down = t - (outer - 1 - z)

        @pl.when((down >= 0) & (down < chunks))
        def _():
            do_down(down)

        done = t - jnp.maximum(z, outer - 1 - z)

        @pl.when((done >= 0) & (done < chunks))
        def _():
            do_final(done)

        @pl.when(t < busy)
        def _():
            def one(k, same):
                solve_planes(t * per_tick + k)
                return same

            lax.fori_loop(0, per_tick, one, 0)

        @pl.when(t == busy)
        def _():
            early_edges()

        return unused

    lax.fori_loop(0, ticks, tick, 0)

    for k in range(1, slabs):
        early(k).wait()
    carry_in, carry_next = chain(
        lambda d: gathered[d, 0], lambda d: gathered[d, 1], carries[0]
    )
    carries[0] = carry_in
    carries[1] = carry_next

    def finish_plane(j, unused):
        z_ref[j] = z_ref[j] + spread(carries[0, pl.ds(j, 1)], carries[1, pl.ds(j, 1)])
        return unused

    lax.fori_loop(0, planes, finish_plane, 0)

    def wait_back(c, unused):
        to_back(c).wait()
        return unused

    lax.fori_loop(0, chunks, wait_back, 0)
    rhs = jnp.concatenate(
        [
            jnp.concatenate([final[side, blocks_at(i)] for i in range(count)], axis=0)
            for side in range(2)
        ],
        axis=1,
    )
    answers = solve_group(rhs, coupling[0], width_ref, mixed_ref, mixed_depth[...])
    pieces = []
    for i in range(count):
        h, strip = i // strips, i % strips
        rows = [
            final[side, h * seg + half + edge * strips + strip, :].reshape(1, depth)
            for edge in (0, 1) for side in (0, 1)
        ]
        rows.append(jnp.zeros((4, depth), F32))
        pieces.append(jnp.concatenate(rows, axis=0))
    value = jnp.concatenate(rows_solve(pieces, coupling[0], width_ref, mixed_ref), axis=1)
    lines = [ends_of(answers[side]) for side in range(2)]
    for edge in range(2):
        for side in range(2):
            own = value[edge * 2 + side : edge * 2 + side + 1]
            late[edge * 2 + side : edge * 2 + side + 1] = with_edges(
                edge, lines[side][edge : edge + 1], value[side : side + 1], own
            )
    for k in range(1, slabs):
        last_link(k).start()
    late_in[slab, 0:4] = late[0:4]
    for k in range(1, slabs):
        last_link(k).wait()
    carry_in, carry_next = chain(
        lambda d: late_in[d, 0:2], lambda d: late_in[d, 2:4], value[0:2]
    )
    for side in range(2):
        face_ref[side] = answers[side] + spread(
            carry_in[side : side + 1], carry_next[side : side + 1]
        )

    def wait_sent(c, unused):
        to_pair(c).wait_send()

        @pl.when(z < outer - 1)
        def _():
            to_above(c).wait_send()

        @pl.when(z > 0)
        def _():
            to_below(c).wait_send()

        return unused

    lax.fori_loop(0, chunks, wait_sent, 0)


def finish_kernel(parts, z_ref, face_ref, coef_ref, out_hbm, out_ref, sem):
    planes, width, depth = z_ref.shape
    rows = width // parts

    def store(c):
        at = pl.ds(pl.multiple_of(c * rows, 8), rows)
        return pltpu.make_async_copy(out_ref.at[:, at], out_hbm.at[:, at], sem.at[c])

    def part(c, unused):
        at = pl.ds(pl.multiple_of(c * rows, 8), rows)
        enter, leave = face_ref[0, at], face_ref[1, at]
        for j in range(planes):
            k = planes - 1 - j
            out_ref[j, at] = z_ref[j, at] + coef_ref[j : j + 1] * enter + coef_ref[k : k + 1] * leave
        store(c).start()
        return unused

    lax.fori_loop(0, parts, part, 0)

    def drain(c, unused):
        store(c).wait()
        return unused

    lax.fori_loop(0, parts, drain, 0)


def per_device(density, source, coupling, width_inverse, height_inverse, depth_inverse):
    planes, width, depth = density.shape
    pencils, slabs = lax.axis_size("pencil"), lax.axis_size("slab")
    blocks, size = width_inverse.shape[:2]
    group = 2
    half = width // 2
    extra = -(-2 * half // depth // 8) * 8
    seg = half + extra
    chunks = next(k for k in range(5, seg) if seg // 8 % k == 0)
    chunk = seg // chunks
    vmem = pl.BlockSpec(memory_space=pltpu.VMEM)
    hbm = pl.BlockSpec(memory_space=pl.ANY)
    smem = pl.BlockSpec(memory_space=pltpu.SMEM)
    dma = pltpu.SemaphoreType.DMA
    field = jax.ShapeDtypeStruct((planes, width, depth), F32)
    faces = jax.ShapeDtypeStruct((2, width, depth), F32)
    table = jax.ShapeDtypeStruct((planes, depth), F32)
    line = pltpu.VMEM((seg, depth), F32)
    two = pltpu.VMEM((2, seg, depth), F32)
    steps = dma((chunks,))
    peers = dma((slabs - 1,))
    z, face, table = pl.pallas_call(
        lambda *refs: step_kernel(group, pencils, slabs, chunk, *refs),
        out_shape=(field, faces, table),
        in_specs=[smem, hbm, hbm, vmem, vmem],
        out_specs=(vmem, vmem, vmem),
        scratch_shapes=[
            pltpu.VMEM((planes, width + 16, depth), F32),
            pltpu.VMEM((planes, width, depth), F32),
            pltpu.VMEM((planes, 2 * seg, depth), F32),
            pltpu.VMEM((blocks, 2 * size, 2 * size), BF16),
            pltpu.VMEM((2 * size, 2 * size), BF16),
            two, two, two, line, line, line, line, two,
            pltpu.VMEM((2, 2 * seg, depth), F32),
            pltpu.VMEM((2, planes, width), F32),
            pltpu.VMEM((slabs, 2, planes, width), F32),
            pltpu.VMEM((2, planes, width), F32),
            pltpu.VMEM((8, width), F32),
            pltpu.VMEM((slabs, 8, width), F32),
            dma((4 + 4 * (half // depth),)),
            steps, steps, steps, steps, steps, steps, steps, steps,
            peers, peers, peers, peers,
        ],
        compiler_params=pltpu.CompilerParams(
            vmem_limit_bytes=44 * 1024 * 1024, collective_id=0, has_side_effects=True
        ),
    )(coupling, density, source, width_inverse, depth_inverse)

    parts = 8
    return pl.pallas_call(
        lambda *refs: finish_kernel(parts, *refs),
        out_shape=field,
        in_specs=[vmem, vmem, vmem],
        out_specs=hbm,
        scratch_shapes=[pltpu.VMEM((planes, width, depth), F32), dma((parts,))],
        compiler_params=pltpu.CompilerParams(vmem_limit_bytes=32 * 1024 * 1024),
    )(z, face, table)


def solution(mesh):
    in_specs = (P("pencil", None, "slab"), P("pencil", None, "slab"), P(), P(), P(), P())
    out_specs = P("pencil", None, "slab")
    return jax.shard_map(
        per_device, mesh=mesh, in_specs=in_specs, out_specs=out_specs, check_vma=False
    )
```

```python
import jax
import jax.numpy as jnp
from jax import lax
from jax.experimental import pallas as pl
from jax.experimental.pallas import tpu as pltpu
from jax.sharding import PartitionSpec as P

F32, BF16 = jnp.float32, jnp.bfloat16
MESH = pl.DeviceIdType.MESH


def split(value):
    high = value.astype(BF16)
    return high, (value - high.astype(F32)).astype(BF16)


def both(value, axis):
    return jnp.concatenate(split(value), axis=axis)


def dot(a, b, dims):
    return lax.dot_general(a, b, (dims, ((), ())), preferred_element_type=F32)


def ends_of(plane):
    width, depth = plane.shape
    row = lax.broadcasted_iota(jnp.int32, (depth, depth), 0)
    lane = lax.broadcasted_iota(jnp.int32, (depth, depth), 1)
    lines = []
    for column in (0, depth - 1):
        pieces = []
        for start in range(0, width, depth):
            edge = plane[start : start + depth, column : column + 1]
            pieces.append(jnp.sum(jnp.where(row == lane, edge, 0.0), axis=0, keepdims=True))
        lines.append(jnp.concatenate(pieces, axis=1))
    return jnp.concatenate(lines, axis=0)


def rows_of(pieces, width):
    row = lax.broadcasted_iota(jnp.int32, (16, width), 0)
    value = jnp.zeros((16, width), F32)
    for number, piece in enumerate(pieces):
        value = jnp.where(row == number, piece.astype(F32), value)
    return value.astype(BF16)


def solve_group(rhs, strength, width_ref, mixed_ref, depth_mixed):
    count, size = width_ref.shape[:2]
    depth = size
    total = rhs.shape[1]
    high, low = split(rhs)
    local, starts, stops = [], [], []
    for i in range(count):
        part = slice(i * size, (i + 1) * size)
        product = dot(mixed_ref[i], jnp.concatenate([high[part], low[part]], 0), ((1,), (0,)))
        local.append(product[:size] + product[size:])
        starts.append(strength * width_ref[i, :, 0:1])
        stops.append(strength * width_ref[i, :, size - 1 : size])
    carry = jnp.zeros((1, total), F32)
    ahead, heads = [], []
    for i in range(count):
        ahead.append(carry)
        heads.append(local[i][0:1] + starts[i][0:1] * carry)
        carry = local[i][size - 1 :] + starts[i][size - 1 :] * carry
    carry = jnp.zeros((1, total), F32)
    solved = [None] * count
    for i in reversed(range(count)):
        solved[i] = local[i] + starts[i] * ahead[i] + stops[i] * carry
        carry = heads[i] + stops[i][0:1] * carry
    solved = jnp.concatenate(solved, axis=0)
    answers = []
    for start in range(0, total, depth):
        product = dot(both(solved[:, start : start + depth], 1), depth_mixed, ((1,), (0,)))
        answers.append(product[:, :depth] + product[:, depth:])
    return answers


class Heights:
    def __init__(self, strength, lanes):
        self.shape = (1, lanes)
        self.strength = jnp.full(self.shape, strength, F32)
        root = (1.0 + 2.0 * self.strength + jnp.sqrt(1.0 + 4.0 * self.strength)) * 0.5
        self.log_ratio = jnp.log(self.strength / root)

    def power(self, index):
        return jnp.exp(jnp.full(self.shape, index, jnp.int32).astype(F32) * self.log_ratio)

    def tail(self, count):
        return 1.0 - self.power(2 * count)

    def beside(self, count):
        return self.power(1) * self.tail(count) / self.tail(count + 1)

    def enter(self, count, j):
        return self.power(j + 1) * self.tail(count - j) / self.tail(count + 1)


def named(label):
    def wrap(function):
        def inner(*args):
            with jax.named_scope(label):
                return function(*args)
        return inner
    return wrap


def rows_solve(pieces, strength, width_ref, mixed_ref):
    count, size = width_ref.shape[:2]
    local = []
    for i in range(count):
        product = dot(both(pieces[i], 1), mixed_ref[i], ((1,), (1,)))
        local.append(product[:, :size] + product[:, size:])
    carry = jnp.zeros((pieces[0].shape[0], 1), F32)
    ahead, heads = [], []
    for i in range(count):
        start = strength * width_ref[i, 0:1]
        ahead.append(start * carry)
        heads.append(local[i][:, 0:1] + start[:, 0:1] * carry)
        carry = local[i][:, size - 1 :] + start[:, size - 1 :] * carry
    carry = jnp.zeros((pieces[0].shape[0], 1), F32)
    solved = [None] * count
    for i in reversed(range(count)):
        stop = strength * width_ref[i, size - 1 : size]
        solved[i] = local[i] + ahead[i] + stop * carry
        carry = heads[i] + stop[:, 0:1] * carry
    return solved


def step_kernel(
    group, pencils, slabs, chunk, lag,
    coupling_hbm, rho_hbm, source_hbm, width_hbm, depth_hbm,
    z_ref, face_ref, coef_ref,
    coupling, width_ref, depth_ref,
    rho_ref, source_ref, y_ref, mixed_ref, mixed_depth,
    rho_edges, z_edges, turned, columns,
    pair_out, pair_in, block, up_out, up_in, down_out, down_in, back_out, final,
    ends, gathered, carries, late, late_in,
    load_sem, table_sem, pair_send, pair_recv, up_send, up_recv, down_send, down_recv,
    back_send, back_recv, early_send, early_recv, late_send, late_recv,
):
    planes, width, depth = z_ref.shape
    groups = planes // group
    count, size = width_ref.shape[:2]
    half = width // 2
    seg = final.shape[1] // 2
    extra = seg - half
    chunks = seg // chunk
    strips = half // depth
    pad = 8
    me, slab = lax.axis_index("pencil"), lax.axis_index("slab")
    outer = pencils // 2
    z, x = lax.div(me, 2), lax.rem(me, 2)
    pair = z * 2 + 1 - x
    above_me = lax.rem(me + 2, pencils)
    below_me = lax.rem(me + pencils - 2, pencils)

    barrier = pltpu.get_barrier_semaphore()
    for peer in (pair, above_me, below_me):
        pl.semaphore_signal(barrier, inc=1, device_id={"pencil": peer}, device_id_type=MESH)
    for k in range(1, slabs):
        pl.semaphore_signal(
            barrier, inc=1, device_id={"slab": lax.rem(slab + k, slabs)}, device_id_type=MESH
        )

    loads = {}

    def load(key, src, dst, start, rows, shift):
        number = loads.setdefault(key, len(loads))
        return pltpu.make_async_copy(
            src.at[:, pl.ds(pl.multiple_of(start, 8), rows)],
            dst.at[:, pl.ds(pl.multiple_of(start + shift, 8), rows)],
            load_sem.at[number],
        )

    def rim(h, side):
        start = h * half + side * (half - 8)
        return load(("rim", h, side), rho_hbm, rho_ref, start, 8, pad)

    def main(turn, h, piece):
        low = 8 if piece == 0 else piece * depth
        high = half - 8 if piece == strips - 1 else (piece + 1) * depth
        return load(("rho", turn, piece), rho_hbm, rho_ref, h * half + low, high - low, pad)

    def other(turn, h, piece):
        start = h * half + piece * depth
        return load(("source", turn, piece), source_hbm, source_ref, start, depth, 0)

    tables = [
        pltpu.make_async_copy(src, dst, table_sem.at[k])
        for k, (src, dst) in enumerate(
            ((coupling_hbm, coupling), (width_hbm, width_ref), (depth_hbm, depth_ref))
        )
    ]
    tables[0].start()
    for h in (0, 1):
        for side in (0, 1):
            rim(h, side).start()
    for turn, h in ((0, 1 - x), (1, x)):
        for piece in range(strips):
            main(turn, h, piece).start()
            other(turn, h, piece).start()
        if turn == 0:
            tables[1].start()
            tables[2].start()

    rho_ref[:, :pad] = jnp.zeros((planes, pad, depth), F32)
    rho_ref[:, pad + width :] = jnp.zeros((planes, pad, depth), F32)
    tables[0].wait()
    heights = Heights(coupling[1], depth)
    for j in range(planes):
        coef_ref[j : j + 1] = heights.enter(planes, j)
    strength = heights.strength
    ahead = [heights.beside(j + 1) for j in range(planes)]
    pivot = [value / strength for value in ahead]
    near, far = heights.enter(planes, 0), heights.enter(planes, planes - 1)
    gain = 1.0 / (1.0 - near * near)
    near2, far2 = heights.enter(2 * planes, 0), heights.enter(2 * planes, 2 * planes - 1)
    under = heights.beside(2 * planes * z)
    over = heights.beside(2 * planes * (outer - 1 - z))
    under_gain, over_gain = 1.0 / (1.0 - under * near2), 1.0 / (1.0 - over * near2)
    det = 1.0 / ((1.0 - under * near2) * (1.0 - over * near2) - under * over * far2 * far2)
    k_uu, k_uo = (1.0 - over * near2) * det, under * far2 * det
    k_oo, k_ou = (1.0 - under * near2) * det, over * far2 * det

    lane = lax.broadcasted_iota(jnp.int32, (1, depth), 1)
    across, along = coupling[0], coupling[2]
    k_here = 2.0 - 4.0 * across - 4.0 * along
    k_before = jnp.where(lane == 0, 0.0, jnp.full((1, depth), 2.0 * along, F32))
    k_after = jnp.where(lane == depth - 1, 0.0, jnp.full((1, depth), 2.0 * along, F32))

    def back_sweep(at, value):
        for j in reversed(range(planes)):
            if j == planes - 1:
                y = pivot[j] * value
            else:
                y = pivot[j] * (y_ref[j, at] + strength * y)
            y_ref[j, at] = y
        return y

    @named("sweep")
    def sweep(h, row, rows):
        base = pl.multiple_of(pad + h * half + row, 8)
        at = pl.ds(pl.multiple_of(h * seg + row, 8), rows)
        from_source = pl.ds(pl.multiple_of(h * half + row, 8), rows)
        value = None
        edges = jnp.zeros((rows, depth), F32)
        for j in range(planes):
            rho = rho_ref[j, pl.ds(base, rows)]
            beside = rho_ref[j, pl.ds(base - 1, rows)] + rho_ref[j, pl.ds(base + 1, rows)]
            rhs = (
                source_ref[j, from_source]
                + k_here * rho
                + (2.0 * across) * beside
                + k_before * pltpu.roll(rho, 1, 1)
                + k_after * pltpu.roll(rho, depth - 1, 1)
            )
            edges = jnp.where(lax.div(lane, 2) == j, pltpu.roll(rho, 2 * j + 1, 1), edges)
            value = rhs if j == 0 else rhs + ahead[j - 1] * value
            y_ref[j, at] = value
        rho_edges[from_source] = edges
        last = pivot[planes - 1] * value
        first = back_sweep(at, value)
        return first, last

    @named("edge")
    def edge_sweep(h):
        at = pl.ds(pl.multiple_of(h * seg + half, 8), extra)
        value = None
        for strip in range(strips):
            start = pl.multiple_of(h * half + strip * depth, 8)
            rows = rho_edges[pl.ds(start, depth)].T
            for j in range(planes):
                to = pl.ds(h * seg + half + 2 * strip, 2)
                y_ref[j, to] = rows[2 * j : 2 * j + 2]
        spare = extra - 2 * strips
        y_ref[:, pl.ds(h * seg + half + 2 * strips, spare)] = jnp.zeros((planes, spare, depth), F32)
        for j in range(planes):
            rhs = y_ref[j, at]
            value = rhs if j == 0 else rhs + ahead[j - 1] * value
            y_ref[j, at] = value
        last = pivot[planes - 1] * value
        first = back_sweep(at, value)
        return first, last

    def remote(source, target, send, recv, peer, axis="pencil"):
        return pltpu.make_async_remote_copy(
            src_ref=source, dst_ref=target, send_sem=send, recv_sem=recv,
            device_id={axis: peer}, device_id_type=MESH,
        )

    def rows_at(c, shift=0):
        return pl.ds(pl.multiple_of(c * chunk + shift, 8), chunk)

    def to_pair(c):
        at = rows_at(c)
        return remote(
            pair_out.at[:, at], pair_in.at[:, at], pair_send.at[c], pair_recv.at[c], pair
        )

    def to_above(c):
        at = rows_at(c)
        return remote(up_out.at[at], up_in.at[at], up_send.at[c], up_recv.at[c], above_me)

    def to_below(c):
        at = rows_at(c)
        return remote(
            down_out.at[at], down_in.at[at], down_send.at[c], down_recv.at[c], below_me
        )

    def to_back(c):
        return remote(
            back_out.at[:, rows_at(c)], final.at[:, rows_at(c, x * seg)],
            back_send.at[c], back_recv.at[c], pair,
        )

    def keep(turn, at, faces):
        if turn == 0:
            pair_out[0, at], pair_out[1, at] = faces

    need = [min(strips, -(-(c * chunk + chunk + 1) // depth)) for c in range(chunks)]
    first_use = [next(c for c in range(chunks) if need[c] > piece) for piece in range(strips)]

    def whole_chunk(turn, h, c):
        for piece in range(strips):
            @pl.when(c == first_use[piece])
            def _():
                main(turn, h, piece).wait()
                other(turn, h, piece).wait()

        row = pl.multiple_of(c * chunk, 8)
        keep(turn, pl.ds(row, chunk), sweep(h, row, chunk))

    def last_chunk(turn, h):
        for piece in range(strips):
            if first_use[piece] == chunks - 1:
                main(turn, h, piece).wait()
                other(turn, h, piece).wait()
        row = (chunks - 1) * chunk
        keep(turn, pl.ds(row, half - row), sweep(h, row, half - row))
        keep(turn, pl.ds(half, extra), edge_sweep(h))

    for h in (0, 1):
        for side in (0, 1):
            rim(h, side).wait()

    def for_pair(c, unused):
        whole_chunk(0, 1 - x, c)

        @pl.when(c == 0)
        def _():
            pl.semaphore_wait(barrier, 3 + slabs - 1)

        to_pair(c).start()
        return unused

    lax.fori_loop(0, chunks - 1, for_pair, 0)
    last_chunk(0, 1 - x)
    to_pair(chunks - 1).start()
    tables[1].wait()
    tables[2].wait()
    for i in range(count):
        high, low = split(width_ref[i])
        mixed_ref[i, :size, :size] = high
        mixed_ref[i, :size, size:] = high
        mixed_ref[i, size:, :size] = low
        mixed_ref[i, size:, size:] = jnp.zeros_like(low)
    high, low = split(depth_ref[slab])
    mixed_depth[:size, :size] = high
    mixed_depth[size:, :size] = high
    mixed_depth[:size, size:] = low
    mixed_depth[size:, size:] = jnp.zeros_like(low)


    @pl.when(z == 0)
    def _():
        up_in[...] = jnp.zeros_like(up_in)

    @pl.when(z == outer - 1)
    def _():
        down_in[...] = jnp.zeros_like(down_in)

    def faces_of(c):
        at, mine = rows_at(c), rows_at(c, x * seg)
        own_first, own_last = y_ref[0, mine], y_ref[planes - 1, mine]
        its_first, its_last = pair_in[0, at], pair_in[1, at]
        lower = x == 0
        return (
            jnp.where(lower, own_first, its_first),
            jnp.where(lower, own_last, its_last),
            jnp.where(lower, its_first, own_first),
            jnp.where(lower, its_last, own_last),
        )

    @named("pair")
    def do_pair(c):
        to_pair(c).wait_recv()
        at = rows_at(c)
        f0, l0, f1, l1 = faces_of(c)
        block[0, at] = f0 + far * gain * (f1 + near * l0)
        block[1, at] = l1 + far * gain * (l0 + near * f1)

    @named("up")
    def do_up(c):
        @pl.when(z > 0)
        def _():
            to_above(c).wait_recv()

        at = rows_at(c)

        @pl.when(z < outer - 1)
        def _():
            up_out[at] = block[1, at] + far2 * under_gain * (up_in[at] + under * block[0, at])
            to_above(c).start()

    @named("down")
    def do_down(c):
        @pl.when(z < outer - 1)
        def _():
            to_below(c).wait_recv()

        at = rows_at(c)

        @pl.when(z > 0)
        def _():
            down_out[at] = block[0, at] + far2 * over_gain * (down_in[at] + over * block[1, at])
            to_below(c).start()

    @named("done")
    def do_final(c):
        at, mine = rows_at(c), rows_at(c, x * seg)
        low = up_in[at] + under * block[0, at]
        high = down_in[at] + over * block[1, at]
        enter = k_uu * low + k_uo * high
        leave = k_ou * low + k_oo * high
        f0, l0, f1, l1 = faces_of(c)
        l0 = l0 + far * enter
        f1 = f1 + far * leave
        inner_low = gain * (l0 + near * f1)
        inner_high = gain * (f1 + near * l0)
        lower = x == 0
        final[0, mine] = jnp.where(lower, enter, inner_low)
        final[1, mine] = jnp.where(lower, inner_high, leave)
        back_out[0, at] = jnp.where(lower, inner_low, enter)
        back_out[1, at] = jnp.where(lower, leave, inner_high)
        to_back(c).start()

    def blocks_at(i):
        return pl.ds(i // strips * seg + i % strips * size, size)

    @named("mid")
    def solve_planes(index):
        base = index * group
        rhs = jnp.concatenate(
            [
                jnp.concatenate(
                    [
                        y_ref[base + g, blocks_at(i)]
                        - 2.0 * rho_ref[base + g, pl.ds(pad + i * size, size)]
                        for i in range(count)
                    ],
                    axis=0,
                )
                for g in range(group)
            ],
            axis=1,
        )
        answers = solve_group(rhs, coupling[0], width_ref, mixed_ref, mixed_depth[...])
        for g in range(group):
            z_ref[base + g] = answers[g] + rho_ref[base + g, pl.ds(pad, width)]
            rolled = pltpu.roll(answers[g], 2 * (base + g) + 1, 1)
            z_edges[...] = jnp.where(lax.div(lane, 2) == base + g, rolled, z_edges[...])

    def turn_rows(source, i, rows):
        turned[i] = source[pl.ds(i * size, size)].T[: turned.shape[1]]
        return [turned[i, pl.ds(edge, rows, stride=2)] for edge in (1, 0)]

    before_me = jnp.where(slab > 0, slab - 1, 0)
    corner = depth_ref[before_me, size - 1 : size, size - 1 : size]
    corner = jnp.where(slab > 0, corner, jnp.zeros_like(corner))

    def link(d, row, column):
        return coupling[2] * depth_ref[d, row : row + 1, column : column + 1]

    def with_edges(edge, ends_value, v_first, v_own):
        row = 0 if edge == 0 else size - 1
        return ends_value + 2.0 * v_own + (2.0 * coupling[2] * corner * link(slab, row, 0)) * v_first

    @named("early")
    def early_edges():
        pieces = []
        for i in range(count):
            h, strip = i // strips, i % strips
            rows = [
                y_ref[:, h * seg + half + 2 * strip + 1 - edge, :] for edge in (0, 1)
            ]
            pieces.append(jnp.concatenate(rows, axis=0))
        value = jnp.concatenate(rows_solve(pieces, coupling[0], width_ref, mixed_ref), axis=1)
        first, last = value[:planes], value[planes:]
        carries[0] = first
        lines = [turn_rows(z_edges, i, planes) for i in range(count)]
        lines = [jnp.concatenate([line[edge] for line in lines], axis=1) for edge in (0, 1)]
        ends[0] = with_edges(0, lines[0], first, first)
        ends[1] = with_edges(1, lines[1], first, last)
        for k in range(1, slabs):
            early(k).start()
        gathered[slab] = ends[...]

    def early(k):
        return remote(
            ends, gathered.at[slab], early_send.at[k - 1], early_recv.at[k - 1],
            lax.rem(slab + k, slabs), "slab",
        )

    def last_link(k):
        return remote(
            late.at[pl.ds(0, 4)], late_in.at[slab, pl.ds(0, 4)],
            late_send.at[k - 1], late_recv.at[k - 1],
            lax.rem(slab + k, slabs), "slab",
        )

    def chain(first_of, last_of, v_first):
        zero = jnp.zeros_like(v_first)
        forward = [zero]
        for d in range(slabs - 1):
            forward.append(last_of(d) + link(d, size - 1, 0) * forward[d])
        backward = [zero] * slabs
        for d in range(slabs - 1, 0, -1):
            backward[d - 1] = (
                first_of(d) + link(d, 0, 0) * forward[d] + link(d, 0, size - 1) * backward[d]
            )
        carry_in, carry_next = forward[0], backward[0]
        for d in range(1, slabs):
            carry_in = jnp.where(slab == d, forward[d], carry_in)
            carry_next = jnp.where(slab == d, backward[d], carry_next)
        return carry_in + (2.0 * coupling[2] * corner) * v_first, carry_next

    reach = lag * (outer - 1)
    ticks = max(chunks + reach, groups + 2)
    ready = (chunks + 1) // 2

    def tick(t, unused):
        @pl.when(t < 2)
        def _():
            def ours(c, same):
                whole_chunk(1, x, c)
                return same

            lax.fori_loop(t * ready, jnp.minimum(t * ready + ready, chunks - 1), ours, 0)

        @pl.when(t == 1)
        def _():
            last_chunk(1, x)

        @pl.when(t < chunks)
        def _():
            do_pair(t)

        up = t - lag * z

        @pl.when((up >= 0) & (up < chunks))
        def _():
            do_up(up)

        down = t - lag * (outer - 1 - z)

        @pl.when((down >= 0) & (down < chunks))
        def _():
            do_down(down)

        done = t - lag * jnp.maximum(z, outer - 1 - z)

        @pl.when((done >= 0) & (done < chunks))
        def _():
            do_final(done)

        @pl.when((t >= 1) & (t <= groups))
        def _():
            solve_planes(t - 1)

        @pl.when(t == groups + 1)
        def _():
            early_edges()

        return unused

    lax.fori_loop(0, ticks, tick, 0)

    @named("back")
    def wait_back(c, unused):
        to_back(c).wait()
        return unused

    lax.fori_loop(0, chunks, wait_back, 0)
    with jax.named_scope("late_solve"):
        rhs = jnp.concatenate(
            [
                jnp.concatenate([final[side, blocks_at(i)] for i in range(count)], axis=0)
                for side in range(2)
            ],
            axis=1,
        )
        answers = solve_group(rhs, coupling[0], width_ref, mixed_ref, mixed_depth[...])
        pieces = []
        for i in range(count):
            h, strip = i // strips, i % strips
            rows = [
                final[side, h * seg + half + 2 * strip + 1 - edge, :].reshape(1, depth)
                for edge in (0, 1) for side in (0, 1)
            ]
            rows.append(jnp.zeros((4, depth), F32))
            pieces.append(jnp.concatenate(rows, axis=0))
        value = jnp.concatenate(rows_solve(pieces, coupling[0], width_ref, mixed_ref), axis=1)
        edges = jnp.where(lax.div(lane, 2) == 0, pltpu.roll(answers[0], 1, 1), pltpu.roll(answers[1], 3, 1))
        z_edges[...] = edges
        lines = [turn_rows(z_edges, i, 2) for i in range(count)]
        lines = [jnp.concatenate([line[edge] for line in lines], axis=1) for edge in (0, 1)]
        for edge in range(2):
            for side in range(2):
                own = value[edge * 2 + side : edge * 2 + side + 1]
                late[edge * 2 + side : edge * 2 + side + 1] = with_edges(
                    edge, lines[edge][side : side + 1], value[side : side + 1], own
                )
    for k in range(1, slabs):
        last_link(k).start()
    late_in[slab, 0:4] = late[0:4]

    with jax.named_scope("early_wait"):
        for k in range(1, slabs):
            early(k).wait()
    in_row = coupling[2] * depth_ref[slab, 0:1]
    next_row = coupling[2] * depth_ref[slab, size - 1 : size]
    (in_high, in_low), (next_high, next_low) = split(in_row), split(next_row)
    spots = lax.broadcasted_iota(jnp.int32, (2 * depth, depth), 0)
    number, spot = lax.div(spots, planes), lax.rem(spots, planes)
    lows = depth // planes
    base = jnp.zeros((2 * depth, depth), F32)
    for k, piece in (
        (0, in_high), (1, next_high), (2, in_low), (3, next_low),
        (lows, in_high), (lows + 1, next_high),
    ):
        base = jnp.where(number == k, piece.astype(F32), base)
    carry_in, carry_next = chain(
        lambda d: gathered[d, 0], lambda d: gathered[d, 1], carries[0]
    )
    lines = jnp.concatenate([carry_in, carry_next] * 2, axis=0)
    lines = jnp.concatenate([lines, jnp.zeros((depth - 4 * planes, width), F32)], axis=0)
    for i in range(count):
        part = slice(i * size, (i + 1) * size)
        columns[part] = both(lines[:, part].T, 1)

    @named("fix")
    def finish_planes(index, unused):
        j = index * group
        rhs = jnp.concatenate([jnp.where(spot == j + g, base, 0.0) for g in range(group)], axis=1)
        both_planes = dot(columns[...], rhs.astype(BF16), ((1,), (0,)))
        for g in range(group):
            z_ref[j + g] = z_ref[j + g] + both_planes[:, g * depth : (g + 1) * depth]
        return unused

    lax.fori_loop(0, groups, finish_planes, 0)
    with jax.named_scope("late_wait"):
        for k in range(1, slabs):
            last_link(k).wait()
    carry_in, carry_next = chain(
        lambda d: late_in[d, 0:2], lambda d: late_in[d, 2:4], value[0:2]
    )
    pieces = []
    for side in range(2):
        (a_high, a_low), (b_high, b_low) = split(carry_in[side : side + 1]), split(carry_next[side : side + 1])
        pieces += [a_high, a_low, a_high, b_high, b_low, b_high]
    six = (in_high, in_high, in_low, next_high, next_high, next_low)
    blank = jnp.zeros((1, depth), F32)
    row_pairs = [jnp.concatenate([piece.astype(F32), blank], axis=1) for piece in six]
    row_pairs += [jnp.concatenate([blank, piece.astype(F32)], axis=1) for piece in six]
    spread = dot(rows_of(pieces, width), rows_of(row_pairs, 2 * depth), ((0,), (0,)))
    for side in range(2):
        face_ref[side] = answers[side] + spread[:, side * depth : (side + 1) * depth]

    @named("sent")
    def wait_sent(c, unused):
        to_pair(c).wait_send()

        @pl.when(z < outer - 1)
        def _():
            to_above(c).wait_send()

        @pl.when(z > 0)
        def _():
            to_below(c).wait_send()

        return unused

    lax.fori_loop(0, chunks, wait_sent, 0)


def finish_kernel(parts, z_ref, face_ref, coef_ref, out_hbm, out_ref, sem):
    planes, width, depth = z_ref.shape
    rows = width // parts

    def store(c):
        at = pl.ds(pl.multiple_of(c * rows, 8), rows)
        return pltpu.make_async_copy(out_ref.at[:, at], out_hbm.at[:, at], sem.at[c])

    def part(c, unused):
        at = pl.ds(pl.multiple_of(c * rows, 8), rows)
        enter, leave = face_ref[0, at], face_ref[1, at]
        for j in range(planes):
            k = planes - 1 - j
            out_ref[j, at] = z_ref[j, at] + coef_ref[j : j + 1] * enter + coef_ref[k : k + 1] * leave
        store(c).start()
        return unused

    lax.fori_loop(0, parts, part, 0)

    def drain(c, unused):
        store(c).wait()
        return unused

    lax.fori_loop(0, parts, drain, 0)


def per_device(density, source, coupling, width_inverse, height_inverse, depth_inverse):
    planes, width, depth = density.shape
    pencils, slabs = lax.axis_size("pencil"), lax.axis_size("slab")
    blocks, size = width_inverse.shape[:2]
    group = 2
    half = width // 2
    extra = -(-2 * half // depth // 8) * 8
    seg = half + extra
    chunks = next(k for k in range(5, seg) if seg // 8 % k == 0)
    chunk = seg // chunks
    vmem = pl.BlockSpec(memory_space=pltpu.VMEM)
    hbm = pl.BlockSpec(memory_space=pl.ANY)
    far = pl.BlockSpec(memory_space=pltpu.HBM)
    dma = pltpu.SemaphoreType.DMA
    field = jax.ShapeDtypeStruct((planes, width, depth), F32)
    faces = jax.ShapeDtypeStruct((2, width, depth), F32)
    table = jax.ShapeDtypeStruct((planes, depth), F32)
    line = pltpu.VMEM((seg, depth), F32)
    two = pltpu.VMEM((2, seg, depth), F32)
    steps = dma((chunks,))
    peers = dma((slabs - 1,))
    z, face, table = pl.pallas_call(
        lambda *refs: step_kernel(group, pencils, slabs, chunk, 2, *refs),
        out_shape=(field, faces, table),
        in_specs=[far, far, far, far, far],
        out_specs=(vmem, vmem, vmem),
        scratch_shapes=[
            pltpu.SMEM(coupling.shape, F32),
            pltpu.VMEM(width_inverse.shape, F32),
            pltpu.VMEM(depth_inverse.shape, F32),
            pltpu.VMEM((planes, width + 16, depth), F32),
            pltpu.VMEM((planes, width, depth), F32),
            pltpu.VMEM((planes, 2 * seg, depth), F32),
            pltpu.VMEM((blocks, 2 * size, 2 * size), BF16),
            pltpu.VMEM((2 * size, 2 * size), BF16),
            pltpu.VMEM((width, depth), F32),
            pltpu.VMEM((width, depth), F32),
            pltpu.VMEM((blocks, 2 * planes, depth), F32),
            pltpu.VMEM((width, 2 * depth), BF16),
            two, two, two, line, line, line, line, two,
            pltpu.VMEM((2, 2 * seg, depth), F32),
            pltpu.VMEM((2, planes, width), F32),
            pltpu.VMEM((slabs, 2, planes, width), F32),
            pltpu.VMEM((2, planes, width), F32),
            pltpu.VMEM((8, width), F32),
            pltpu.VMEM((slabs, 8, width), F32),
            dma((4 + 4 * (half // depth),)), dma((3,)),
            steps, steps, steps, steps, steps, steps, steps, steps,
            peers, peers, peers, peers,
        ],
        compiler_params=pltpu.CompilerParams(
            vmem_limit_bytes=44 * 1024 * 1024, collective_id=0, has_side_effects=True
        ),
    )(coupling, density, source, width_inverse, depth_inverse)

    parts = 8
    return pl.pallas_call(
        lambda *refs: finish_kernel(parts, *refs),
        out_shape=field,
        in_specs=[vmem, vmem, vmem],
        out_specs=hbm,
        scratch_shapes=[pltpu.VMEM((planes, width, depth), F32), dma((parts,))],
        compiler_params=pltpu.CompilerParams(vmem_limit_bytes=32 * 1024 * 1024),
    )(z, face, table)


def solution(mesh):
    in_specs = (P("pencil", None, "slab"), P("pencil", None, "slab"), P(), P(), P(), P())
    out_specs = P("pencil", None, "slab")
    return jax.shard_map(
        per_device, mesh=mesh, in_specs=in_specs, out_specs=out_specs, check_vma=False
    )
```

```python
import jax
import jax.numpy as jnp
from jax import lax
from jax.experimental import pallas as pl
from jax.experimental.pallas import tpu as pltpu
from jax.sharding import PartitionSpec as P

F32, BF16 = jnp.float32, jnp.bfloat16
MESH = pl.DeviceIdType.MESH


def split(value):
    high = value.astype(BF16)
    return high, (value - high.astype(F32)).astype(BF16)


def both(value, axis):
    return jnp.concatenate(split(value), axis=axis)


def dot(a, b, dims):
    return lax.dot_general(a, b, (dims, ((), ())), preferred_element_type=F32)


def ends_of(plane):
    width, depth = plane.shape
    row = lax.broadcasted_iota(jnp.int32, (depth, depth), 0)
    lane = lax.broadcasted_iota(jnp.int32, (depth, depth), 1)
    lines = []
    for column in (0, depth - 1):
        pieces = []
        for start in range(0, width, depth):
            edge = plane[start : start + depth, column : column + 1]
            pieces.append(jnp.sum(jnp.where(row == lane, edge, 0.0), axis=0, keepdims=True))
        lines.append(jnp.concatenate(pieces, axis=1))
    return jnp.concatenate(lines, axis=0)


def rows_of(pieces, width):
    row = lax.broadcasted_iota(jnp.int32, (16, width), 0)
    value = jnp.zeros((16, width), F32)
    for number, piece in enumerate(pieces):
        value = jnp.where(row == number, piece.astype(F32), value)
    return value.astype(BF16)


def width_solve(rhs, strength, width_ref, mixed_ref):
    count, size = width_ref.shape[:2]
    total = rhs.shape[1]
    high, low = split(rhs)
    local, starts, stops = [], [], []
    for i in range(count):
        part = slice(i * size, (i + 1) * size)
        product = dot(mixed_ref[i], jnp.concatenate([high[part], low[part]], 0), ((1,), (0,)))
        local.append(product[:size] + product[size:])
        starts.append(strength * width_ref[i, :, 0:1])
        stops.append(strength * width_ref[i, :, size - 1 : size])
    carry = jnp.zeros((1, total), F32)
    ahead, heads = [], []
    for i in range(count):
        ahead.append(carry)
        heads.append(local[i][0:1] + starts[i][0:1] * carry)
        carry = local[i][size - 1 :] + starts[i][size - 1 :] * carry
    carry = jnp.zeros((1, total), F32)
    solved = [None] * count
    for i in reversed(range(count)):
        solved[i] = local[i] + starts[i] * ahead[i] + stops[i] * carry
        carry = heads[i] + stops[i][0:1] * carry
    return jnp.concatenate(solved, axis=0)


def depth_solve(value, mixed_depth):
    depth = value.shape[1]
    product = dot(both(value, 1), mixed_depth[...], ((1,), (0,)))
    return product[:, :depth] + product[:, depth:]


class Heights:
    def __init__(self, strength, lanes):
        self.shape = (1, lanes)
        self.strength = jnp.full(self.shape, strength, F32)
        root = (1.0 + 2.0 * self.strength + jnp.sqrt(1.0 + 4.0 * self.strength)) * 0.5
        self.log_ratio = jnp.log(self.strength / root)

    def power(self, index):
        return jnp.exp(jnp.full(self.shape, index, jnp.int32).astype(F32) * self.log_ratio)

    def tail(self, count):
        return 1.0 - self.power(2 * count)

    def beside(self, count):
        return self.power(1) * self.tail(count) / self.tail(count + 1)

    def enter(self, count, j):
        return self.power(j + 1) * self.tail(count - j) / self.tail(count + 1)


def named(label):
    def wrap(function):
        def inner(*args):
            with jax.named_scope(label):
                return function(*args)
        return inner
    return wrap


def rows_solve(pieces, strength, width_ref, mixed_ref):
    count, size = width_ref.shape[:2]
    local = []
    for i in range(count):
        product = dot(both(pieces[i], 1), mixed_ref[i], ((1,), (1,)))
        local.append(product[:, :size] + product[:, size:])
    carry = jnp.zeros((pieces[0].shape[0], 1), F32)
    ahead, heads = [], []
    for i in range(count):
        start = strength * width_ref[i, 0:1]
        ahead.append(start * carry)
        heads.append(local[i][:, 0:1] + start[:, 0:1] * carry)
        carry = local[i][:, size - 1 :] + start[:, size - 1 :] * carry
    carry = jnp.zeros((pieces[0].shape[0], 1), F32)
    solved = [None] * count
    for i in reversed(range(count)):
        stop = strength * width_ref[i, size - 1 : size]
        solved[i] = local[i] + ahead[i] + stop * carry
        carry = heads[i] + stop[:, 0:1] * carry
    return solved


def step_kernel(
    group, pencils, slabs, chunk, lag,
    coupling_hbm, rho_hbm, source_hbm, width_hbm, depth_hbm,
    z_ref, face_ref, coef_ref,
    coupling, width_ref, depth_ref,
    rho_ref, source_ref, y_ref, mixed_ref, mixed_depth,
    shifts, at_ends, rho_edges, z_edges, turned, columns,
    pair_out, pair_in, block, up_out, up_in, down_out, down_in, back_out, final,
    ends, gathered, carries, late, late_in,
    load_sem, table_sem, pair_send, pair_recv, up_send, up_recv, down_send, down_recv,
    back_send, back_recv, early_send, early_recv, own_send, own_recv, cross_send, cross_recv,
):
    planes, width, depth = z_ref.shape
    groups = planes // group
    count, size = width_ref.shape[:2]
    half = width // 2
    seg = final.shape[1] // 2
    extra = seg - half
    chunks = seg // chunk
    strips = half // depth
    pad = 8
    me, slab = lax.axis_index("pencil"), lax.axis_index("slab")
    outer = pencils // 2
    z, x = lax.div(me, 2), lax.rem(me, 2)
    pair = z * 2 + 1 - x
    above_me = lax.rem(me + 2, pencils)
    below_me = lax.rem(me + pencils - 2, pencils)

    barrier = pltpu.get_barrier_semaphore()
    for peer in (pair, above_me, below_me):
        pl.semaphore_signal(barrier, inc=1, device_id={"pencil": peer}, device_id_type=MESH)
    for k in range(1, slabs):
        peer = lax.rem(slab + k, slabs)
        for whom in ({"slab": peer}, {"pencil": pair, "slab": peer}):
            pl.semaphore_signal(barrier, inc=1, device_id=whom, device_id_type=MESH)

    loads = {}

    def load(key, src, dst, start, rows, shift):
        number = loads.setdefault(key, len(loads))
        return pltpu.make_async_copy(
            src.at[:, pl.ds(pl.multiple_of(start, 8), rows)],
            dst.at[:, pl.ds(pl.multiple_of(start + shift, 8), rows)],
            load_sem.at[number],
        )

    def rim(h, side):
        start = h * half + side * (half - 8)
        return load(("rim", h, side), rho_hbm, rho_ref, start, 8, pad)

    def main(turn, h, piece):
        low = 8 if piece == 0 else piece * depth
        high = half - 8 if piece == strips - 1 else (piece + 1) * depth
        return load(("rho", turn, piece), rho_hbm, rho_ref, h * half + low, high - low, pad)

    def other(turn, h, piece):
        start = h * half + piece * depth
        return load(("source", turn, piece), source_hbm, source_ref, start, depth, 0)

    tables = [
        pltpu.make_async_copy(src, dst, table_sem.at[k])
        for k, (src, dst) in enumerate(
            ((coupling_hbm, coupling), (width_hbm, width_ref), (depth_hbm, depth_ref))
        )
    ]
    tables[0].start()
    for h in (0, 1):
        for side in (0, 1):
            rim(h, side).start()
    for piece in range(strips):
        for turn, h in ((0, 1 - x), (1, x)):
            main(turn, h, piece).start()
            other(turn, h, piece).start()
        if piece == 0:
            tables[1].start()
            tables[2].start()

    rho_ref[:, :pad] = jnp.zeros((planes, pad, depth), F32)
    rho_ref[:, pad + width :] = jnp.zeros((planes, pad, depth), F32)
    tables[0].wait()
    heights = Heights(coupling[1], depth)
    for j in range(planes):
        coef_ref[j : j + 1] = heights.enter(planes, j)
    strength = heights.strength
    ahead = [heights.beside(j + 1) for j in range(planes)]
    pivot = [value / strength for value in ahead]
    near, far = heights.enter(planes, 0), heights.enter(planes, planes - 1)
    gain = 1.0 / (1.0 - near * near)
    near2, far2 = heights.enter(2 * planes, 0), heights.enter(2 * planes, 2 * planes - 1)
    under = heights.beside(2 * planes * z)
    over = heights.beside(2 * planes * (outer - 1 - z))
    under_gain, over_gain = 1.0 / (1.0 - under * near2), 1.0 / (1.0 - over * near2)
    det = 1.0 / ((1.0 - under * near2) * (1.0 - over * near2) - under * over * far2 * far2)
    k_uu, k_uo = (1.0 - over * near2) * det, under * far2 * det
    k_oo, k_ou = (1.0 - under * near2) * det, over * far2 * det

    lane = lax.broadcasted_iota(jnp.int32, (1, depth), 1)
    across, along = coupling[0], coupling[2]
    k_here = 2.0 - 4.0 * across - 4.0 * along
    source_row = lax.rem(lax.broadcasted_iota(jnp.int32, (2 * depth, depth), 0), depth)
    column = lax.broadcasted_iota(jnp.int32, (2 * depth, depth), 1)
    beside_it = (source_row == column + 1) | (source_row == column - 1)
    at_edge = source_row == jnp.where(lax.rem(column, 2) == 0, depth - 1, 0)
    shifts[:, :depth] = jnp.where(beside_it, 1.0, 0.0).astype(BF16)
    shifts[:, depth:] = jnp.where(at_edge, 1.0, 0.0).astype(BF16)

    def back_sweep(at, value):
        for j in reversed(range(planes)):
            if j == planes - 1:
                y = pivot[j] * value
            else:
                y = pivot[j] * (y_ref[j, at] + strength * y)
            y_ref[j, at] = y
        return y

    @named("sweep")
    def sweep(h, row, rows):
        base = pl.multiple_of(pad + h * half + row, 8)
        at = pl.ds(pl.multiple_of(h * seg + row, 8), rows)
        from_source = pl.ds(pl.multiple_of(h * half + row, 8), rows)
        value = None
        edges = jnp.zeros((rows, depth), F32)
        batch = 8
        for j in range(planes):
            if j % batch == 0:
                several = [rho_ref[j + k, pl.ds(base, rows)] for k in range(batch)]
                several = both(jnp.concatenate(several, axis=0), 1)
                all_shifted = dot(several, shifts[...], ((1,), (0,)))
            rho = rho_ref[j, pl.ds(base, rows)]
            beside = rho_ref[j, pl.ds(base - 1, rows)] + rho_ref[j, pl.ds(base + 1, rows)]
            shifted = all_shifted[j % batch * rows : (j % batch + 1) * rows]
            rhs = (
                source_ref[j, from_source]
                + k_here * rho
                + (2.0 * across) * beside
                + (2.0 * along) * shifted[:, :depth]
            )
            edges = jnp.where(lax.div(lane, 2) == j, shifted[:, depth:], edges)
            value = rhs if j == 0 else rhs + ahead[j - 1] * value
            y_ref[j, at] = value
        rho_edges[from_source] = edges
        last = pivot[planes - 1] * value
        first = back_sweep(at, value)
        return first, last

    @named("edge")
    def edge_sweep(h):
        at = pl.ds(pl.multiple_of(h * seg + half, 8), extra)
        value = None
        for strip in range(strips):
            start = pl.multiple_of(h * half + strip * depth, 8)
            rows = rho_edges[pl.ds(start, depth)].T
            for j in range(planes):
                to = pl.ds(h * seg + half + 2 * strip, 2)
                y_ref[j, to] = rows[2 * j : 2 * j + 2]
        spare = extra - 2 * strips
        y_ref[:, pl.ds(h * seg + half + 2 * strips, spare)] = jnp.zeros((planes, spare, depth), F32)
        for j in range(planes):
            rhs = y_ref[j, at]
            value = rhs if j == 0 else rhs + ahead[j - 1] * value
            y_ref[j, at] = value
        last = pivot[planes - 1] * value
        first = back_sweep(at, value)
        return first, last

    def remote(source, target, send, recv, peer):
        whom = peer if isinstance(peer, dict) else {"pencil": peer}
        return pltpu.make_async_remote_copy(
            src_ref=source, dst_ref=target, send_sem=send, recv_sem=recv,
            device_id=whom, device_id_type=MESH,
        )

    def rows_at(c, shift=0):
        return pl.ds(pl.multiple_of(c * chunk + shift, 8), chunk)

    def to_pair(c):
        at = rows_at(c)
        return remote(
            pair_out.at[:, at], pair_in.at[:, at], pair_send.at[c], pair_recv.at[c], pair
        )

    def to_above(c):
        at = rows_at(c)
        return remote(up_out.at[at], up_in.at[at], up_send.at[c], up_recv.at[c], above_me)

    def to_below(c):
        at = rows_at(c)
        return remote(
            down_out.at[at], down_in.at[at], down_send.at[c], down_recv.at[c], below_me
        )

    def to_back(c):
        return remote(
            back_out.at[:, rows_at(c)], final.at[:, rows_at(c, x * seg)],
            back_send.at[c], back_recv.at[c], pair,
        )

    def keep(turn, at, faces):
        if turn == 0:
            pair_out[0, at], pair_out[1, at] = faces

    need = [min(strips, -(-(c * chunk + chunk + 1) // depth)) for c in range(chunks)]
    first_use = [next(c for c in range(chunks) if need[c] > piece) for piece in range(strips)]

    def whole_chunk(turn, h, c):
        for piece in range(strips):
            @pl.when(c == first_use[piece])
            def _():
                main(turn, h, piece).wait()
                other(turn, h, piece).wait()

        row = pl.multiple_of(c * chunk, 8)
        keep(turn, pl.ds(row, chunk), sweep(h, row, chunk))

    def last_chunk(turn, h):
        for piece in range(strips):
            if first_use[piece] == chunks - 1:
                main(turn, h, piece).wait()
                other(turn, h, piece).wait()
        row = (chunks - 1) * chunk
        keep(turn, pl.ds(row, half - row), sweep(h, row, half - row))
        keep(turn, pl.ds(half, extra), edge_sweep(h))

    for h in (0, 1):
        for side in (0, 1):
            rim(h, side).wait()

    def prepare():
        tables[1].wait()
        tables[2].wait()
        for i in range(count):
            high, low = split(width_ref[i])
            mixed_ref[i, :size, :size] = high
            mixed_ref[i, :size, size:] = high
            mixed_ref[i, size:, :size] = low
            mixed_ref[i, size:, size:] = jnp.zeros_like(low)
        first_high, first_low = split(depth_ref[slab, 0:1])
        last_high, last_low = split(depth_ref[slab, size - 1 : size])
        nothing = jnp.zeros((1, depth), F32)
        at_ends[...] = rows_of(
            [
                jnp.concatenate([piece.astype(F32), tail], axis=1)
                for piece, tail in (
                    (first_high, first_high.astype(F32)), (last_high, last_high.astype(F32)),
                    (first_low, nothing), (last_low, nothing),
                )
            ],
            2 * depth,
        )
        high, low = split(depth_ref[slab])
        mixed_depth[:size, :size] = high
        mixed_depth[size:, :size] = high
        mixed_depth[:size, size:] = low
        mixed_depth[size:, size:] = jnp.zeros_like(low)

    @pl.when(z == 0)
    def _():
        up_in[...] = jnp.zeros_like(up_in)

    @pl.when(z == outer - 1)
    def _():
        down_in[...] = jnp.zeros_like(down_in)

    def faces_of(c):
        at, mine = rows_at(c), rows_at(c, x * seg)
        own_first, own_last = y_ref[0, mine], y_ref[planes - 1, mine]
        its_first, its_last = pair_in[0, at], pair_in[1, at]
        lower = x == 0
        return (
            jnp.where(lower, own_first, its_first),
            jnp.where(lower, own_last, its_last),
            jnp.where(lower, its_first, own_first),
            jnp.where(lower, its_last, own_last),
        )

    @named("pair")
    def do_pair(c):
        to_pair(c).wait_recv()
        at = rows_at(c)
        f0, l0, f1, l1 = faces_of(c)
        block[0, at] = f0 + far * gain * (f1 + near * l0)
        block[1, at] = l1 + far * gain * (l0 + near * f1)

    @named("up")
    def do_up(c):
        @pl.when(z > 0)
        def _():
            to_above(c).wait_recv()

        at = rows_at(c)

        @pl.when(z < outer - 1)
        def _():
            up_out[at] = block[1, at] + far2 * under_gain * (up_in[at] + under * block[0, at])
            to_above(c).start()

    @named("down")
    def do_down(c):
        @pl.when(z < outer - 1)
        def _():
            to_below(c).wait_recv()

        at = rows_at(c)

        @pl.when(z > 0)
        def _():
            down_out[at] = block[0, at] + far2 * over_gain * (down_in[at] + over * block[1, at])
            to_below(c).start()

    @named("done")
    def do_final(c):
        at, mine = rows_at(c), rows_at(c, x * seg)
        low = up_in[at] + under * block[0, at]
        high = down_in[at] + over * block[1, at]
        enter = k_uu * low + k_uo * high
        leave = k_ou * low + k_oo * high
        f0, l0, f1, l1 = faces_of(c)
        l0 = l0 + far * enter
        f1 = f1 + far * leave
        inner_low = gain * (l0 + near * f1)
        inner_high = gain * (f1 + near * l0)
        lower = x == 0
        final[0, mine] = jnp.where(lower, enter, inner_low)
        final[1, mine] = jnp.where(lower, inner_high, leave)
        back_out[0, at] = jnp.where(lower, inner_low, enter)
        back_out[1, at] = jnp.where(lower, leave, inner_high)
        to_back(c).start()

    def blocks_at(i):
        return pl.ds(i // strips * seg + i % strips * size, size)

    @named("mid")
    def solve_planes(index):
        base = index * group
        rhs = jnp.concatenate(
            [
                jnp.concatenate(
                    [
                        y_ref[base + g, blocks_at(i)]
                        - 2.0 * rho_ref[base + g, pl.ds(pad + i * size, size)]
                        for i in range(count)
                    ],
                    axis=0,
                )
                for g in range(group)
            ],
            axis=1,
        )
        solved = width_solve(rhs, coupling[0], width_ref, mixed_ref)
        answers = [
            depth_solve(solved[:, g * depth : (g + 1) * depth], mixed_depth) for g in range(group)
        ]
        for g in range(group):
            z_ref[base + g] = answers[g] + rho_ref[base + g, pl.ds(pad, width)]
            rolled = pltpu.roll(answers[g], 2 * (base + g) + 1, 1)
            z_edges[...] = jnp.where(lax.div(lane, 2) == base + g, rolled, z_edges[...])

    def turn_rows(source, i, rows):
        turned[i] = source[pl.ds(i * size, size)].T[: turned.shape[1]]
        return [turned[i, pl.ds(edge, rows, stride=2)] for edge in (1, 0)]

    def corner():
        value = depth_ref[jnp.where(slab > 0, slab - 1, 0), size - 1 : size, size - 1 : size]
        return jnp.where(slab > 0, value, jnp.zeros_like(value))

    def link(d, row, column):
        return coupling[2] * depth_ref[d, row : row + 1, column : column + 1]

    def with_edges(edge, ends_value, v_first, v_own):
        row = 0 if edge == 0 else size - 1
        return ends_value + 2.0 * v_own + (2.0 * coupling[2] * corner() * link(slab, row, 0)) * v_first

    @named("early")
    def early_edges():
        pieces = []
        for i in range(count):
            h, strip = i // strips, i % strips
            rows = [
                y_ref[:, h * seg + half + 2 * strip + 1 - edge, :] for edge in (0, 1)
            ]
            pieces.append(jnp.concatenate(rows, axis=0))
        value = jnp.concatenate(rows_solve(pieces, coupling[0], width_ref, mixed_ref), axis=1)
        first, last = value[:planes], value[planes:]
        carries[0] = first
        lines = [turn_rows(z_edges, i, planes) for i in range(count)]
        lines = [jnp.concatenate([line[edge] for line in lines], axis=1) for edge in (0, 1)]
        ends[0] = with_edges(0, lines[0], first, first)
        ends[1] = with_edges(1, lines[1], first, last)
        for k in range(1, slabs):
            early(k).start()
        gathered[slab] = ends[...]

    def early(k):
        return remote(
            ends, gathered.at[slab], early_send.at[k - 1], early_recv.at[k - 1],
            {"slab": lax.rem(slab + k, slabs)},
        )

    def late_own(k):
        return remote(
            late.at[pl.ds(0, 6)], late_in.at[x, slab, pl.ds(0, 6)],
            own_send.at[k - 1], own_recv.at[k - 1], {"slab": lax.rem(slab + k, slabs)},
        )

    def late_cross(k):
        return remote(
            late.at[pl.ds(8, 6)], late_in.at[x, slab, pl.ds(0, 6)],
            cross_send.at[k], cross_recv.at[k],
            {"pencil": pair, "slab": lax.rem(slab + k, slabs)},
        )

    @named("late_edges")
    def late_edges():
        for who in range(2):
            for side in range(2):
                if who == 0:
                    plane = final[side, pl.ds(pl.multiple_of(x * seg, 8), half)]
                    rows = final[side, pl.ds(pl.multiple_of(x * seg + half, 8), extra)]
                else:
                    plane = back_out[side, pl.ds(0, half)]
                    rows = back_out[side, pl.ds(half, extra)]
                lines = dot(at_ends[...], both(plane, 1), ((1,), (1,)))
                first, last = lines[0:1] + lines[2:3], lines[1:2] + lines[3:4]
                v_last, v_first = (
                    jnp.concatenate(
                        [rows[2 * strip + k : 2 * strip + k + 1] for strip in range(strips)], axis=1
                    )
                    for k in (0, 1)
                )
                row = 8 * who + side
                late[row : row + 1] = with_edges(0, first, v_first, v_first)
                late[row + 2 : row + 3] = with_edges(1, last, v_first, v_last)
                late[row + 4 : row + 5] = v_first
        for k in range(1, slabs):
            late_own(k).start()
        for k in range(slabs):
            late_cross(k).start()
        late_in[x, slab, 0:6] = late[0:6]

    def chain(first_of, last_of, v_first):
        zero = jnp.zeros_like(v_first)
        forward = [zero]
        for d in range(slabs - 1):
            forward.append(last_of(d) + link(d, size - 1, 0) * forward[d])
        backward = [zero] * slabs
        for d in range(slabs - 1, 0, -1):
            backward[d - 1] = (
                first_of(d) + link(d, 0, 0) * forward[d] + link(d, 0, size - 1) * backward[d]
            )
        carry_in, carry_next = forward[0], backward[0]
        for d in range(1, slabs):
            carry_in = jnp.where(slab == d, forward[d], carry_in)
            carry_next = jnp.where(slab == d, backward[d], carry_next)
        return carry_in + (2.0 * coupling[2] * corner()) * v_first, carry_next

    reach = lag * (outer - 1)
    settle = 3
    heavy = chunks
    ticks = max(settle + chunks + reach, heavy + groups + 1)

    def tick(t, unused):
        @pl.when(t < chunks - 1)
        def _():
            whole_chunk(0, 1 - x, t)

        @pl.when(t == chunks - 1)
        def _():
            last_chunk(0, 1 - x)

        @pl.when(t == 0)
        def _():
            pl.semaphore_wait(barrier, 3 + 2 * (slabs - 1))

        @pl.when(t < chunks)
        def _():
            to_pair(t).start()

        @pl.when((t >= 1) & (t < chunks))
        def _():
            whole_chunk(1, x, t - 1)

        @pl.when(t == chunks)
        def _():
            last_chunk(1, x)
            prepare()

        @pl.when((t >= settle) & (t < settle + chunks))
        def _():
            do_pair(t - settle)

        up = t - settle - lag * z
        down = t - settle - lag * (outer - 1 - z)
        done = t - settle - lag * jnp.maximum(z, outer - 1 - z)

        @pl.when((up >= 0) & (up < chunks))
        def _():
            do_up(up)

        @pl.when((down >= 0) & (down < chunks))
        def _():
            do_down(down)

        @pl.when((done >= 0) & (done < chunks))
        def _():
            do_final(done)

        @pl.when(done == chunks - 1)
        def _():
            late_edges()

        @pl.when((t >= heavy) & (t < heavy + groups))
        def _():
            solve_planes(t - heavy)

        @pl.when(t == heavy + groups)
        def _():
            early_edges()

        return unused

    lax.fori_loop(0, ticks, tick, 0)

    with jax.named_scope("early_wait"):
        for k in range(1, slabs):
            early(k).wait()
    in_row = coupling[2] * depth_ref[slab, 0:1]
    next_row = coupling[2] * depth_ref[slab, size - 1 : size]
    (in_high, in_low), (next_high, next_low) = split(in_row), split(next_row)
    spots = lax.broadcasted_iota(jnp.int32, (2 * depth, depth), 0)
    number, spot = lax.div(spots, planes), lax.rem(spots, planes)
    lows = depth // planes
    base = jnp.zeros((2 * depth, depth), F32)
    for k, piece in (
        (0, in_high), (1, next_high), (2, in_low), (3, next_low),
        (lows, in_high), (lows + 1, next_high),
    ):
        base = jnp.where(number == k, piece.astype(F32), base)
    carry_in, carry_next = chain(
        lambda d: gathered[d, 0], lambda d: gathered[d, 1], carries[0]
    )
    lines = jnp.concatenate([carry_in, carry_next] * 2, axis=0)
    lines = jnp.concatenate([lines, jnp.zeros((depth - 4 * planes, width), F32)], axis=0)
    for i in range(count):
        part = slice(i * size, (i + 1) * size)
        columns[part] = both(lines[:, part].T, 1)

    @named("fix")
    def finish_planes(index, unused):
        j = index * group
        rhs = jnp.concatenate([jnp.where(spot == j + g, base, 0.0) for g in range(group)], axis=1)
        both_planes = dot(columns[...], rhs.astype(BF16), ((1,), (0,)))
        for g in range(group):
            z_ref[j + g] = z_ref[j + g] + both_planes[:, g * depth : (g + 1) * depth]
        return unused

    lax.fori_loop(0, groups, finish_planes, 0)
    @named("back")
    def wait_back(c, unused):
        to_back(c).wait()
        return unused

    lax.fori_loop(0, chunks, wait_back, 0)
    with jax.named_scope("late_depth"):
        for side in range(2):
            rows = jnp.concatenate([final[side, blocks_at(i)] for i in range(count)], axis=0)
            face_ref[side] = depth_solve(rows, mixed_depth)

    with jax.named_scope("late_wait"):
        for k in range(1, slabs):
            late_own(k).wait()
        for k in range(slabs):
            late_cross(k).wait()

    def late_rows(d, row):
        return jnp.concatenate([late_in[h, d, row : row + 2] for h in range(2)], axis=1)

    with jax.named_scope("late_chain"):
        carry_in, carry_next = chain(
            lambda d: late_rows(d, 0), lambda d: late_rows(d, 2), late_rows(slab, 4)
        )
        pieces = []
        for side in range(2):
            (a_high, a_low), (b_high, b_low) = split(carry_in[side : side + 1]), split(carry_next[side : side + 1])
            pieces += [a_high, a_low, a_high, b_high, b_low, b_high]
        six = (in_high, in_high, in_low, next_high, next_high, next_low)
        blank = jnp.zeros((1, depth), F32)
        row_pairs = [jnp.concatenate([piece.astype(F32), blank], axis=1) for piece in six]
        row_pairs += [jnp.concatenate([blank, piece.astype(F32)], axis=1) for piece in six]
        spread = dot(rows_of(pieces, width), rows_of(row_pairs, 2 * depth), ((0,), (0,)))

    with jax.named_scope("late_solve"):
        sides = [face_ref[side] + spread[:, side * depth : (side + 1) * depth] for side in range(2)]
        solved = width_solve(jnp.concatenate(sides, axis=1), coupling[0], width_ref, mixed_ref)
        for side in range(2):
            face_ref[side] = solved[:, side * depth : (side + 1) * depth]

    @named("sent")
    def wait_sent(c, unused):
        to_pair(c).wait_send()

        @pl.when(z < outer - 1)
        def _():
            to_above(c).wait_send()

        @pl.when(z > 0)
        def _():
            to_below(c).wait_send()

        return unused

    lax.fori_loop(0, chunks, wait_sent, 0)


def finish_kernel(parts, z_ref, face_ref, coef_ref, out_hbm, out_ref, sem):
    planes, width, depth = z_ref.shape
    rows = width // parts

    def store(c):
        at = pl.ds(pl.multiple_of(c * rows, 8), rows)
        return pltpu.make_async_copy(out_ref.at[:, at], out_hbm.at[:, at], sem.at[c])

    def part(c, unused):
        at = pl.ds(pl.multiple_of(c * rows, 8), rows)
        enter, leave = face_ref[0, at], face_ref[1, at]
        for j in range(planes):
            k = planes - 1 - j
            out_ref[j, at] = z_ref[j, at] + coef_ref[j : j + 1] * enter + coef_ref[k : k + 1] * leave
        store(c).start()
        return unused

    lax.fori_loop(0, parts, part, 0)

    def drain(c, unused):
        store(c).wait()
        return unused

    lax.fori_loop(0, parts, drain, 0)


def per_device(density, source, coupling, width_inverse, height_inverse, depth_inverse):
    planes, width, depth = density.shape
    pencils, slabs = lax.axis_size("pencil"), lax.axis_size("slab")
    blocks, size = width_inverse.shape[:2]
    group = 4
    half = width // 2
    extra = -(-2 * half // depth // 8) * 8
    seg = half + extra
    chunks = next(k for k in range(5, seg) if seg // 8 % k == 0)
    chunk = seg // chunks
    vmem = pl.BlockSpec(memory_space=pltpu.VMEM)
    hbm = pl.BlockSpec(memory_space=pl.ANY)
    far = pl.BlockSpec(memory_space=pltpu.HBM)
    dma = pltpu.SemaphoreType.DMA
    field = jax.ShapeDtypeStruct((planes, width, depth), F32)
    faces = jax.ShapeDtypeStruct((2, width, depth), F32)
    table = jax.ShapeDtypeStruct((planes, depth), F32)
    line = pltpu.VMEM((seg, depth), F32)
    two = pltpu.VMEM((2, seg, depth), F32)
    steps = dma((chunks,))
    peers = dma((slabs - 1,))
    operands = (coupling, density, source, width_inverse, depth_inverse)
    z, face, table = pl.pallas_call(
        lambda *refs: step_kernel(group, pencils, slabs, chunk, 3, *refs),
        out_shape=(field, faces, table),
        in_specs=[far, far, far, far, far],
        out_specs=(vmem, vmem, vmem),
        scratch_shapes=[
            pltpu.SMEM(coupling.shape, F32),
            pltpu.VMEM(width_inverse.shape, F32),
            pltpu.VMEM(depth_inverse.shape, F32),
            pltpu.VMEM((planes, width + 16, depth), F32),
            pltpu.VMEM((planes, width, depth), F32),
            pltpu.VMEM((planes, 2 * seg, depth), F32),
            pltpu.VMEM((blocks, 2 * size, 2 * size), BF16),
            pltpu.VMEM((2 * size, 2 * size), BF16),
            pltpu.VMEM((2 * depth, 2 * depth), BF16),
            pltpu.VMEM((16, 2 * depth), BF16),
            pltpu.VMEM((width, depth), F32),
            pltpu.VMEM((width, depth), F32),
            pltpu.VMEM((blocks, 2 * planes, depth), F32),
            pltpu.VMEM((width, 2 * depth), BF16),
            two, two, two, line, line, line, line, two,
            pltpu.VMEM((2, 2 * seg, depth), F32),
            pltpu.VMEM((2, planes, width), F32),
            pltpu.VMEM((slabs, 2, planes, width), F32),
            pltpu.VMEM((2, planes, width), F32),
            pltpu.VMEM((16, half), F32),
            pltpu.VMEM((2, slabs, 8, half), F32),
            dma((4 + 4 * (half // depth),)), dma((3,)),
            steps, steps, steps, steps, steps, steps, steps, steps,
            peers, peers, peers, peers, dma((slabs,)), dma((slabs,)),
        ],
        compiler_params=pltpu.CompilerParams(
            vmem_limit_bytes=44 * 1024 * 1024, collective_id=0, has_side_effects=True
        ),
    )(*[pltpu.with_memory_space_constraint(array, pltpu.HBM) for array in operands])

    parts = 8
    return pl.pallas_call(
        lambda *refs: finish_kernel(parts, *refs),
        out_shape=field,
        in_specs=[vmem, vmem, vmem],
        out_specs=hbm,
        scratch_shapes=[pltpu.VMEM((planes, width, depth), F32), dma((parts,))],
        compiler_params=pltpu.CompilerParams(vmem_limit_bytes=32 * 1024 * 1024),
    )(z, face, table)


def solution(mesh):
    in_specs = (P("pencil", None, "slab"), P("pencil", None, "slab"), P(), P(), P(), P())
    out_specs = P("pencil", None, "slab")
    return jax.shard_map(
        per_device, mesh=mesh, in_specs=in_specs, out_specs=out_specs, check_vma=False
    )
```

```python
import jax
import jax.numpy as jnp
from jax import lax
from jax.experimental import pallas as pl
from jax.experimental.pallas import tpu as pltpu
from jax.sharding import PartitionSpec as P

F32, BF16 = jnp.float32, jnp.bfloat16
MESH = pl.DeviceIdType.MESH


def split(value):
    high = value.astype(BF16)
    return high, (value - high.astype(F32)).astype(BF16)


def both(value, axis):
    return jnp.concatenate(split(value), axis=axis)


def dot(a, b, dims):
    return lax.dot_general(a, b, (dims, ((), ())), preferred_element_type=F32)


def ends_of(plane):
    width, depth = plane.shape
    row = lax.broadcasted_iota(jnp.int32, (depth, depth), 0)
    lane = lax.broadcasted_iota(jnp.int32, (depth, depth), 1)
    lines = []
    for column in (0, depth - 1):
        pieces = []
        for start in range(0, width, depth):
            edge = plane[start : start + depth, column : column + 1]
            pieces.append(jnp.sum(jnp.where(row == lane, edge, 0.0), axis=0, keepdims=True))
        lines.append(jnp.concatenate(pieces, axis=1))
    return jnp.concatenate(lines, axis=0)


def rows_of(pieces, width):
    row = lax.broadcasted_iota(jnp.int32, (16, width), 0)
    value = jnp.zeros((16, width), F32)
    for number, piece in enumerate(pieces):
        value = jnp.where(row == number, piece.astype(F32), value)
    return value.astype(BF16)


def width_solve(rhs, strength, width_ref, mixed_ref):
    count, size = width_ref.shape[:2]
    total = rhs.shape[1]
    high, low = split(rhs)
    local, starts, stops = [], [], []
    for i in range(count):
        part = slice(i * size, (i + 1) * size)
        product = dot(mixed_ref[i], jnp.concatenate([high[part], low[part]], 0), ((1,), (0,)))
        local.append(product[:size] + product[size:])
        starts.append(strength * width_ref[i, :, 0:1])
        stops.append(strength * width_ref[i, :, size - 1 : size])
    carry = jnp.zeros((1, total), F32)
    ahead, heads = [], []
    for i in range(count):
        ahead.append(carry)
        heads.append(local[i][0:1] + starts[i][0:1] * carry)
        carry = local[i][size - 1 :] + starts[i][size - 1 :] * carry
    carry = jnp.zeros((1, total), F32)
    solved = [None] * count
    for i in reversed(range(count)):
        solved[i] = local[i] + starts[i] * ahead[i] + stops[i] * carry
        carry = heads[i] + stops[i][0:1] * carry
    return jnp.concatenate(solved, axis=0)


def depth_solve(value, mixed_depth):
    depth = value.shape[1]
    product = dot(both(value, 1), mixed_depth[...], ((1,), (0,)))
    return product[:, :depth] + product[:, depth:]


class Heights:
    def __init__(self, strength, lanes):
        self.shape = (1, lanes)
        self.strength = jnp.full(self.shape, strength, F32)
        root = (1.0 + 2.0 * self.strength + jnp.sqrt(1.0 + 4.0 * self.strength)) * 0.5
        self.log_ratio = jnp.log(self.strength / root)

    def power(self, index):
        return jnp.exp(jnp.full(self.shape, index, jnp.int32).astype(F32) * self.log_ratio)

    def tail(self, count):
        return 1.0 - self.power(2 * count)

    def beside(self, count):
        return self.power(1) * self.tail(count) / self.tail(count + 1)

    def enter(self, count, j):
        return self.power(j + 1) * self.tail(count - j) / self.tail(count + 1)


def named(label):
    def wrap(function):
        def inner(*args):
            with jax.named_scope(label):
                return function(*args)
        return inner
    return wrap


def rows_solve(pieces, strength, width_ref, mixed_ref):
    count, size = width_ref.shape[:2]
    local = []
    for i in range(count):
        product = dot(both(pieces[i], 1), mixed_ref[i], ((1,), (1,)))
        local.append(product[:, :size] + product[:, size:])
    carry = jnp.zeros((pieces[0].shape[0], 1), F32)
    ahead, heads = [], []
    for i in range(count):
        start = strength * width_ref[i, 0:1]
        ahead.append(start * carry)
        heads.append(local[i][:, 0:1] + start[:, 0:1] * carry)
        carry = local[i][:, size - 1 :] + start[:, size - 1 :] * carry
    carry = jnp.zeros((pieces[0].shape[0], 1), F32)
    solved = [None] * count
    for i in reversed(range(count)):
        stop = strength * width_ref[i, size - 1 : size]
        solved[i] = local[i] + ahead[i] + stop * carry
        carry = heads[i] + stop[:, 0:1] * carry
    return solved


def step_kernel(
    group, pencils, slabs, chunk, lag,
    coupling_hbm, rho_hbm, source_hbm, width_hbm, depth_hbm,
    z_ref, face_ref, coef_ref,
    coupling, width_ref, depth_ref,
    rho_ref, source_ref, y_ref, mixed_ref, mixed_depth,
    shifts, at_ends, links, rho_edges, z_edges, turned, columns,
    pair_out, pair_in, block, up_out, up_in, down_out, down_in, back_out, final,
    ends, gathered, carries, late, late_in,
    load_sem, table_sem, pair_send, pair_recv, up_send, up_recv, down_send, down_recv,
    back_send, back_recv, early_send, early_recv, own_send, own_recv, cross_send, cross_recv,
):
    planes, width, depth = z_ref.shape
    groups = planes // group
    count, size = width_ref.shape[:2]
    half = width // 2
    seg = final.shape[1] // 2
    extra = seg - half
    chunks = seg // chunk
    strips = half // depth
    step = depth // 2
    cuts = half // step
    pad = 8
    me, slab = lax.axis_index("pencil"), lax.axis_index("slab")
    outer = pencils // 2
    z, x = lax.div(me, 2), lax.rem(me, 2)
    pair = z * 2 + 1 - x
    bottom, top = z == 0, z == outer - 1
    inside = (z > 0) & (z < outer - 1)
    gives_more = (bottom & (x == 0)) | (top & (x == 1))
    above_me = lax.rem(me + 2, pencils)
    below_me = lax.rem(me + pencils - 2, pencils)

    barrier = pltpu.get_barrier_semaphore()
    pl.semaphore_signal(barrier, inc=1, device_id={"pencil": pair}, device_id_type=MESH)

    @pl.when(z < outer - 1)
    def _():
        pl.semaphore_signal(barrier, inc=1, device_id={"pencil": above_me}, device_id_type=MESH)

    @pl.when(z > 0)
    def _():
        pl.semaphore_signal(barrier, inc=1, device_id={"pencil": below_me}, device_id_type=MESH)

    for k in range(1, slabs):
        peer = lax.rem(slab + k, slabs)
        for whom in ({"slab": peer}, {"pencil": pair, "slab": peer}):
            pl.semaphore_signal(barrier, inc=1, device_id=whom, device_id_type=MESH)

    loads = {}

    def load(key, src, dst, start, rows, shift):
        number = loads.setdefault(key, len(loads))
        return pltpu.make_async_copy(
            src.at[:, pl.ds(pl.multiple_of(start, 8), rows)],
            dst.at[:, pl.ds(pl.multiple_of(start + shift, 8), rows)],
            load_sem.at[number],
        )

    def rim(h, side):
        start = h * half + side * (half - 8)
        return load(("rim", h, side), rho_hbm, rho_ref, start, 8, pad)

    def main(turn, h, piece):
        low = 8 if piece == 0 else piece * step
        high = half - 8 if piece == cuts - 1 else (piece + 1) * step
        return load(("rho", turn, piece), rho_hbm, rho_ref, h * half + low, high - low, pad)

    def other(turn, h, piece):
        start = h * half + piece * step
        return load(("source", turn, piece), source_hbm, source_ref, start, step, 0)

    tables = [
        pltpu.make_async_copy(src, dst, table_sem.at[k])
        for k, (src, dst) in enumerate(
            ((coupling_hbm, coupling), (width_hbm, width_ref), (depth_hbm, depth_ref))
        )
    ]
    tables[0].start()
    for h in (0, 1):
        for side in (0, 1):
            rim(h, side).start()
    for piece in range(cuts):
        for turn, h in ((0, 1 - x), (1, x)):
            main(turn, h, piece).start()
            other(turn, h, piece).start()
        if piece == 0:
            tables[1].start()
            tables[2].start()

    rho_ref[:, :pad] = jnp.zeros((planes, pad, depth), F32)
    rho_ref[:, pad + width :] = jnp.zeros((planes, pad, depth), F32)
    tables[0].wait()
    heights = Heights(coupling[1], depth)
    for j in range(planes):
        coef_ref[j : j + 1] = heights.enter(planes, j)
    strength = heights.strength
    ahead = [heights.beside(j + 1) for j in range(planes)]
    pivot = [value / strength for value in ahead]
    near, far = heights.enter(planes, 0), heights.enter(planes, planes - 1)
    gain = 1.0 / (1.0 - near * near)
    near2, far2 = heights.enter(2 * planes, 0), heights.enter(2 * planes, 2 * planes - 1)
    under = heights.beside(2 * planes * z)
    over = heights.beside(2 * planes * (outer - 1 - z))
    under_gain, over_gain = 1.0 / (1.0 - under * near2), 1.0 / (1.0 - over * near2)
    det = 1.0 / ((1.0 - under * near2) * (1.0 - over * near2) - under * over * far2 * far2)
    k_uu, k_uo = (1.0 - over * near2) * det, under * far2 * det
    k_oo, k_ou = (1.0 - under * near2) * det, over * far2 * det

    lane = lax.broadcasted_iota(jnp.int32, (1, depth), 1)
    across, along = coupling[0], coupling[2]
    k_here = 2.0 - 4.0 * across - 4.0 * along
    source_row = lax.rem(lax.broadcasted_iota(jnp.int32, (2 * depth, depth), 0), depth)
    column = lax.broadcasted_iota(jnp.int32, (2 * depth, depth), 1)
    beside_it = (source_row == column + 1) | (source_row == column - 1)
    at_edge = source_row == jnp.where(lax.rem(column, 2) == 0, depth - 1, 0)
    shifts[:, :depth] = jnp.where(beside_it, 1.0, 0.0).astype(BF16)
    shifts[:, depth:] = jnp.where(at_edge, 1.0, 0.0).astype(BF16)

    def back_sweep(at, value):
        for j in reversed(range(planes)):
            if j == planes - 1:
                y = pivot[j] * value
            else:
                y = pivot[j] * (y_ref[j, at] + strength * y)
            y_ref[j, at] = y
        return y

    @named("sweep")
    def sweep(h, row, rows):
        base = pl.multiple_of(pad + h * half + row, 8)
        at = pl.ds(pl.multiple_of(h * seg + row, 8), rows)
        from_source = pl.ds(pl.multiple_of(h * half + row, 8), rows)
        value = None
        edges = jnp.zeros((rows, depth), F32)
        batch = 8
        for j in range(planes):
            if j % batch == 0:
                several = [rho_ref[j + k, pl.ds(base, rows)] for k in range(batch)]
                several = both(jnp.concatenate(several, axis=0), 1)
                all_shifted = dot(several, shifts[...], ((1,), (0,)))
            rho = rho_ref[j, pl.ds(base, rows)]
            beside = rho_ref[j, pl.ds(base - 1, rows)] + rho_ref[j, pl.ds(base + 1, rows)]
            shifted = all_shifted[j % batch * rows : (j % batch + 1) * rows]
            rhs = (
                source_ref[j, from_source]
                + k_here * rho
                + (2.0 * across) * beside
                + (2.0 * along) * shifted[:, :depth]
            )
            edges = jnp.where(lax.div(lane, 2) == j, shifted[:, depth:], edges)
            value = rhs if j == 0 else rhs + ahead[j - 1] * value
            y_ref[j, at] = value
        rho_edges[from_source] = edges
        last = pivot[planes - 1] * value
        first = back_sweep(at, value)
        return first, last

    @named("edge")
    def edge_sweep(h):
        at = pl.ds(pl.multiple_of(h * seg + half, 8), extra)
        value = None
        for strip in range(strips):
            start = pl.multiple_of(h * half + strip * depth, 8)
            rows = rho_edges[pl.ds(start, depth)].T
            for j in range(planes):
                to = pl.ds(h * seg + half + 2 * strip, 2)
                y_ref[j, to] = rows[2 * j : 2 * j + 2]
        spare = extra - 2 * strips
        y_ref[:, pl.ds(h * seg + half + 2 * strips, spare)] = jnp.zeros((planes, spare, depth), F32)
        for j in range(planes):
            rhs = y_ref[j, at]
            value = rhs if j == 0 else rhs + ahead[j - 1] * value
            y_ref[j, at] = value
        last = pivot[planes - 1] * value
        first = back_sweep(at, value)
        return first, last

    def remote(source, target, send, recv, peer):
        whom = peer if isinstance(peer, dict) else {"pencil": peer}
        return pltpu.make_async_remote_copy(
            src_ref=source, dst_ref=target, send_sem=send, recv_sem=recv,
            device_id=whom, device_id_type=MESH,
        )

    def rows_at(c, shift=0):
        return pl.ds(pl.multiple_of(c * chunk + shift, 8), chunk)

    def to_pair(c):
        at = rows_at(c)
        return remote(
            pair_out.at[:, at], pair_in.at[:, at], pair_send.at[c], pair_recv.at[c], pair
        )

    def to_above(c):
        at = rows_at(c)
        return remote(up_out.at[at], up_in.at[at], up_send.at[c], up_recv.at[c], above_me)

    def to_below(c):
        at = rows_at(c)
        return remote(
            down_out.at[at], down_in.at[at], down_send.at[c], down_recv.at[c], below_me
        )

    def to_back(c, slots):
        return remote(
            back_out.at[slots, rows_at(c)], final.at[slots, rows_at(c, x * seg)],
            back_send.at[c], back_recv.at[c], pair,
        )

    def each_back(act):
        @pl.when(inside)
        def _():
            act(pl.ds(0, 2))

        @pl.when(bottom)
        def _():
            act(pl.ds(1, 1))

        @pl.when(top)
        def _():
            act(pl.ds(0, 1))

    def keep(turn, at, faces):
        first, last = faces
        if turn == 0:
            pair_out[0, at] = first
            pair_out[1, at] = last
        else:
            @pl.when(bottom & (x == 0))
            def _():
                pair_out[0, at] = last

            @pl.when(top & (x == 1))
            def _():
                pair_out[1, at] = first

    need = [min(cuts, -(-(c * chunk + chunk + 1) // step)) for c in range(chunks)]
    first_use = [next(c for c in range(chunks) if need[c] > piece) for piece in range(cuts)]

    def whole_chunk(turn, h, c):
        for piece in range(cuts):
            @pl.when(c == first_use[piece])
            def _():
                main(turn, h, piece).wait()
                other(turn, h, piece).wait()

        row = pl.multiple_of(c * chunk, 8)
        keep(turn, pl.ds(row, chunk), sweep(h, row, chunk))

    def last_chunk(turn, h):
        for piece in range(cuts):
            if first_use[piece] == chunks - 1:
                main(turn, h, piece).wait()
                other(turn, h, piece).wait()
        row = (chunks - 1) * chunk
        keep(turn, pl.ds(row, half - row), sweep(h, row, half - row))
        keep(turn, pl.ds(half, extra), edge_sweep(h))

    for h in (0, 1):
        for side in (0, 1):
            rim(h, side).wait()

    def prepare():
        tables[1].wait()
        tables[2].wait()
        for i in range(count):
            high, low = split(width_ref[i])
            mixed_ref[i, :size, :size] = high
            mixed_ref[i, :size, size:] = high
            mixed_ref[i, size:, :size] = low
            mixed_ref[i, size:, size:] = jnp.zeros_like(low)
        def spot(d, row, column):
            return depth_ref[d, row : row + 1, column : column + 1]

        for d in range(slabs):
            for k, (row, column) in enumerate(((0, 0), (0, size - 1), (size - 1, 0))):
                value = coupling[2] * spot(d, row, column)
                links[3 * d + k : 3 * d + k + 1] = jnp.broadcast_to(value, (1, depth))
        corner = spot(jnp.where(slab > 0, slab - 1, 0), size - 1, size - 1)
        corner = 2.0 * coupling[2] * jnp.where(slab > 0, corner, jnp.zeros_like(corner))
        for k, value in enumerate(
            (
                corner, corner * coupling[2] * spot(slab, 0, 0),
                corner * coupling[2] * spot(slab, size - 1, 0),
            )
        ):
            links[3 * slabs + k : 3 * slabs + k + 1] = jnp.broadcast_to(value, (1, depth))
        first_high, first_low = split(depth_ref[slab, 0:1])
        last_high, last_low = split(depth_ref[slab, size - 1 : size])
        nothing = jnp.zeros((1, depth), F32)
        at_ends[...] = rows_of(
            [
                jnp.concatenate([piece.astype(F32), tail], axis=1)
                for piece, tail in (
                    (first_high, first_high.astype(F32)), (last_high, last_high.astype(F32)),
                    (first_low, nothing), (last_low, nothing),
                )
            ],
            2 * depth,
        )
        high, low = split(depth_ref[slab])
        mixed_depth[:size, :size] = high
        mixed_depth[size:, :size] = high
        mixed_depth[:size, size:] = low
        mixed_depth[size:, size:] = jnp.zeros_like(low)

    @pl.when(z == 0)
    def _():
        up_in[...] = jnp.zeros_like(up_in)

    @pl.when(z == outer - 1)
    def _():
        down_in[...] = jnp.zeros_like(down_in)

    def faces_of(c):
        at, mine = rows_at(c), rows_at(c, x * seg)
        own_first, own_last = y_ref[0, mine], y_ref[planes - 1, mine]
        its_first, its_last = pair_in[0, at], pair_in[1, at]
        lower = x == 0
        return (
            jnp.where(lower, own_first, its_first),
            jnp.where(lower, own_last, its_last),
            jnp.where(lower, its_first, own_first),
            jnp.where(lower, its_last, own_last),
        )

    @named("pair")
    def do_pair(c):
        to_pair(c).wait_recv()
        at = rows_at(c)
        f0, l0, f1, l1 = faces_of(c)
        block[0, at] = f0 + far * gain * (f1 + near * l0)
        block[1, at] = l1 + far * gain * (l0 + near * f1)

    @named("up")
    def do_up(c):
        @pl.when(z > 0)
        def _():
            to_above(c).wait_recv()

        at = rows_at(c)

        @pl.when(z < outer - 1)
        def _():
            up_out[at] = block[1, at] + far2 * under_gain * (up_in[at] + under * block[0, at])
            to_above(c).start()

    @named("down")
    def do_down(c):
        @pl.when(z < outer - 1)
        def _():
            to_below(c).wait_recv()

        at = rows_at(c)

        @pl.when(z > 0)
        def _():
            down_out[at] = block[0, at] + far2 * over_gain * (down_in[at] + over * block[1, at])
            to_below(c).start()

    @named("done")
    def do_final(c):
        at, mine = rows_at(c), rows_at(c, x * seg)
        low = up_in[at] + under * block[0, at]
        high = down_in[at] + over * block[1, at]
        enter = k_uu * low + k_uo * high
        leave = k_ou * low + k_oo * high
        f0, l0, f1, l1 = faces_of(c)
        l0 = l0 + far * enter
        f1 = f1 + far * leave
        inner_low = gain * (l0 + near * f1)
        inner_high = gain * (f1 + near * l0)
        lower = x == 0
        final[0, mine] = jnp.where(lower, enter, inner_low)
        final[1, mine] = jnp.where(lower, inner_high, leave)
        back_out[0, at] = jnp.where(lower, inner_low, enter)
        back_out[1, at] = jnp.where(lower, leave, inner_high)
        each_back(lambda slots: to_back(c, slots).start())

    def blocks_at(i):
        return pl.ds(i // strips * seg + i % strips * size, size)

    @named("mid")
    def solve_planes(index):
        base = index * group
        rhs = jnp.concatenate(
            [
                jnp.concatenate(
                    [
                        y_ref[base + g, blocks_at(i)]
                        - 2.0 * rho_ref[base + g, pl.ds(pad + i * size, size)]
                        for i in range(count)
                    ],
                    axis=0,
                )
                for g in range(group)
            ],
            axis=1,
        )
        solved = width_solve(rhs, coupling[0], width_ref, mixed_ref)
        answers = [
            depth_solve(solved[:, g * depth : (g + 1) * depth], mixed_depth) for g in range(group)
        ]
        for g in range(group):
            z_ref[base + g] = answers[g] + rho_ref[base + g, pl.ds(pad, width)]
            rolled = pltpu.roll(answers[g], 2 * (base + g) + 1, 1)
            z_edges[...] = jnp.where(lax.div(lane, 2) == base + g, rolled, z_edges[...])

    def turn_rows(source, i, rows):
        turned[i] = source[pl.ds(i * size, size)].T[: turned.shape[1]]
        return [turned[i, pl.ds(edge, rows, stride=2)] for edge in (1, 0)]

    def link(d, row, column):
        return like(3 * d + 2 * (row > 0) + (column > 0))

    def like(number, lanes=width):
        return jnp.concatenate([links[number : number + 1]] * (lanes // depth), axis=1)

    def with_edges(edge, ends_value, v_first, v_own):
        return ends_value + 2.0 * v_own + like(3 * slabs + 1 + (edge > 0), v_first.shape[1]) * v_first

    @named("early")
    def early_edges():
        pieces = []
        for i in range(count):
            h, strip = i // strips, i % strips
            rows = [
                y_ref[:, h * seg + half + 2 * strip + 1 - edge, :] for edge in (0, 1)
            ]
            pieces.append(jnp.concatenate(rows, axis=0))
        value = jnp.concatenate(rows_solve(pieces, coupling[0], width_ref, mixed_ref), axis=1)
        first, last = value[:planes], value[planes:]
        carries[0] = first
        lines = [turn_rows(z_edges, i, planes) for i in range(count)]
        lines = [jnp.concatenate([line[edge] for line in lines], axis=1) for edge in (0, 1)]
        ends[0] = with_edges(0, lines[0], first, first)
        ends[1] = with_edges(1, lines[1], first, last)
        for k in range(1, slabs):
            early(k).start()
        gathered[slab] = ends[...]

    def early(k):
        return remote(
            ends, gathered.at[slab], early_send.at[k - 1], early_recv.at[k - 1],
            {"slab": lax.rem(slab + k, slabs)},
        )

    def late_own(k):
        return remote(
            late.at[pl.ds(0, 6)], late_in.at[x, slab, pl.ds(0, 6)],
            own_send.at[k - 1], own_recv.at[k - 1], {"slab": lax.rem(slab + k, slabs)},
        )

    def late_cross(k):
        return remote(
            late.at[pl.ds(8, 6)], late_in.at[x, slab, pl.ds(0, 6)],
            cross_send.at[k], cross_recv.at[k],
            {"pencil": pair, "slab": lax.rem(slab + k, slabs)},
        )

    @named("late_edges")
    def late_edges():
        for who in range(2):
            for side in range(2):
                if who == 0:
                    plane = final[side, pl.ds(pl.multiple_of(x * seg, 8), half)]
                    rows = final[side, pl.ds(pl.multiple_of(x * seg + half, 8), extra)]
                else:
                    plane = back_out[side, pl.ds(0, half)]
                    rows = back_out[side, pl.ds(half, extra)]
                lines = dot(at_ends[...], both(plane, 1), ((1,), (1,)))
                first, last = lines[0:1] + lines[2:3], lines[1:2] + lines[3:4]
                v_last, v_first = (
                    jnp.concatenate(
                        [rows[2 * strip + k : 2 * strip + k + 1] for strip in range(strips)], axis=1
                    )
                    for k in (0, 1)
                )
                row = 8 * who + side
                late[row : row + 1] = with_edges(0, first, v_first, v_first)
                late[row + 2 : row + 3] = with_edges(1, last, v_first, v_last)
                late[row + 4 : row + 5] = v_first
        for k in range(1, slabs):
            late_own(k).start()
        for k in range(slabs):
            late_cross(k).start()
        late_in[x, slab, 0:6] = late[0:6]

    def chain(first_of, last_of, v_first):
        zero = jnp.zeros_like(v_first)
        forward = [zero]
        for d in range(slabs - 1):
            forward.append(last_of(d) + link(d, size - 1, 0) * forward[d])
        backward = [zero] * slabs
        for d in range(slabs - 1, 0, -1):
            backward[d - 1] = (
                first_of(d) + link(d, 0, 0) * forward[d] + link(d, 0, size - 1) * backward[d]
            )
        carry_in, carry_next = forward[0], backward[0]
        for d in range(1, slabs):
            carry_in = jnp.where(slab == d, forward[d], carry_in)
            carry_next = jnp.where(slab == d, backward[d], carry_next)
        return carry_in + like(3 * slabs) * v_first, carry_next

    reach = lag * (outer - 1)
    settle = 3
    heavy = chunks - 1
    ticks = max(settle + chunks + reach, heavy + groups + 1)

    def tick(t, unused):
        @pl.when(t < chunks - 1)
        def _():
            whole_chunk(0, 1 - x, t)

        @pl.when(t == chunks - 1)
        def _():
            last_chunk(0, 1 - x)

        @pl.when(t == 0)
        def _():
            @pl.when(inside)
            def _():
                pl.semaphore_wait(barrier, 3 + 2 * (slabs - 1))

            @pl.when(jnp.logical_not(inside))
            def _():
                pl.semaphore_wait(barrier, 2 + 2 * (slabs - 1))

        @pl.when((t < chunks) & jnp.logical_not(gives_more))
        def _():
            to_pair(t).start()

        @pl.when(t < chunks - 1)
        def _():
            whole_chunk(1, x, t)

        @pl.when(t == chunks - 1)
        def _():
            last_chunk(1, x)
            prepare()

        @pl.when((t < chunks) & gives_more)
        def _():
            to_pair(t).start()

        @pl.when((t >= settle) & (t < settle + chunks))
        def _():
            do_pair(t - settle)

        def chunk_after(hops):
            number = t - settle - lag * hops
            return jnp.where(number < chunks, number, -1)

        up = chunk_after(z)
        down = chunk_after(outer - 1 - z)
        done = chunk_after(jnp.maximum(z, outer - 1 - z))

        @pl.when(up >= 0)
        def _():
            do_up(up)

        @pl.when(down >= 0)
        def _():
            do_down(down)

        @pl.when(done >= 0)
        def _():
            do_final(done)

        @pl.when(done == chunks - 1)
        def _():
            late_edges()

        @pl.when((t >= heavy) & (t < heavy + groups))
        def _():
            solve_planes(t - heavy)

        @pl.when(t == heavy + groups)
        def _():
            early_edges()

        return unused

    lax.fori_loop(0, ticks, tick, 0)

    with jax.named_scope("early_wait"):
        for k in range(1, slabs):
            early(k).wait()
    wide = 4
    in_row = coupling[2] * depth_ref[slab, 0:1]
    next_row = coupling[2] * depth_ref[slab, size - 1 : size]
    (in_high, in_low), (next_high, next_low) = split(in_row), split(next_row)
    spots = lax.broadcasted_iota(jnp.int32, (2 * depth, depth), 0)
    number, spot = lax.div(spots, planes), lax.rem(spots, planes)
    lows = depth // planes
    base = jnp.zeros((2 * depth, depth), F32)
    for k, piece in (
        (0, in_high), (1, next_high), (2, in_low), (3, next_low),
        (lows, in_high), (lows + 1, next_high),
    ):
        base = jnp.where(number == k, piece.astype(F32), base)
    carry_in, carry_next = chain(
        lambda d: gathered[d, 0], lambda d: gathered[d, 1], carries[0]
    )
    lines = jnp.concatenate([carry_in, carry_next] * 2, axis=0)
    lines = jnp.concatenate([lines, jnp.zeros((depth - 4 * planes, width), F32)], axis=0)
    for i in range(count):
        part = slice(i * size, (i + 1) * size)
        columns[part] = both(lines[:, part].T, 1)

    @named("fix")
    def finish_planes(index, unused):
        j = index * wide
        rhs = jnp.concatenate([jnp.where(spot == j + g, base, 0.0) for g in range(wide)], axis=1)
        both_planes = dot(columns[...], rhs.astype(BF16), ((1,), (0,)))
        for g in range(wide):
            z_ref[j + g] = z_ref[j + g] + both_planes[:, g * depth : (g + 1) * depth]
        return unused

    lax.fori_loop(0, planes // wide, finish_planes, 0)
    def depth_part(h):
        for side in range(2):
            rows = final[side, pl.ds(pl.multiple_of(h * seg, 8), half)]
            to = pl.ds(pl.multiple_of(h * half, 8), half)
            face_ref[side, to] = depth_solve(rows, mixed_depth)

    depth_part(x)

    @named("back")
    def wait_back(c, unused):
        each_back(lambda slots: to_back(c, slots).wait())
        at, theirs = rows_at(c), rows_at(c, (1 - x) * seg)

        @pl.when(bottom & (x == 0))
        def _():
            final[0, theirs] = jnp.zeros((chunk, depth), F32)

        @pl.when(bottom & (x == 1))
        def _():
            leave = y_ref[0, theirs] + far * final[1, theirs]
            final[0, theirs] = gain * (pair_in[0, at] + near * leave)

        @pl.when(top & (x == 0))
        def _():
            enter = y_ref[planes - 1, theirs] + far * final[0, theirs]
            final[1, theirs] = gain * (pair_in[1, at] + near * enter)

        @pl.when(top & (x == 1))
        def _():
            final[1, theirs] = jnp.zeros((chunk, depth), F32)

        return unused

    lax.fori_loop(0, chunks, wait_back, 0)
    with jax.named_scope("late_depth"):
        depth_part(1 - x)

    with jax.named_scope("late_wait"):
        for k in range(1, slabs):
            late_own(k).wait()
        for k in range(slabs):
            late_cross(k).wait()

    def late_rows(d, row):
        return jnp.concatenate([late_in[h, d, row : row + 2] for h in range(2)], axis=1)

    with jax.named_scope("late_chain"):
        carry_in, carry_next = chain(
            lambda d: late_rows(d, 0), lambda d: late_rows(d, 2), late_rows(slab, 4)
        )
        pieces = []
        for side in range(2):
            (a_high, a_low), (b_high, b_low) = split(carry_in[side : side + 1]), split(carry_next[side : side + 1])
            pieces += [a_high, a_low, a_high, b_high, b_low, b_high]
        six = (in_high, in_high, in_low, next_high, next_high, next_low)
        blank = jnp.zeros((1, depth), F32)
        row_pairs = [jnp.concatenate([piece.astype(F32), blank], axis=1) for piece in six]
        row_pairs += [jnp.concatenate([blank, piece.astype(F32)], axis=1) for piece in six]
        spread = dot(rows_of(pieces, width), rows_of(row_pairs, 2 * depth), ((0,), (0,)))

    with jax.named_scope("late_solve"):
        sides = [face_ref[side] + spread[:, side * depth : (side + 1) * depth] for side in range(2)]
        solved = width_solve(jnp.concatenate(sides, axis=1), coupling[0], width_ref, mixed_ref)
        for side in range(2):
            face_ref[side] = solved[:, side * depth : (side + 1) * depth]

    @named("sent")
    def wait_sent(c, unused):
        to_pair(c).wait_send()

        @pl.when(z < outer - 1)
        def _():
            to_above(c).wait_send()

        @pl.when(z > 0)
        def _():
            to_below(c).wait_send()

        return unused

    lax.fori_loop(0, chunks, wait_sent, 0)


def finish_kernel(parts, z_ref, face_ref, coef_ref, out_hbm, out_ref, sem):
    planes, width, depth = z_ref.shape
    rows = width // parts

    def store(c):
        at = pl.ds(pl.multiple_of(c * rows, 8), rows)
        return pltpu.make_async_copy(out_ref.at[:, at], out_hbm.at[:, at], sem.at[c])

    def part(c, unused):
        at = pl.ds(pl.multiple_of(c * rows, 8), rows)
        enter, leave = face_ref[0, at], face_ref[1, at]
        for j in range(planes):
            k = planes - 1 - j
            out_ref[j, at] = z_ref[j, at] + coef_ref[j : j + 1] * enter + coef_ref[k : k + 1] * leave
        store(c).start()
        return unused

    lax.fori_loop(0, parts, part, 0)

    def drain(c, unused):
        store(c).wait()
        return unused

    lax.fori_loop(0, parts, drain, 0)


def per_device(density, source, coupling, width_inverse, height_inverse, depth_inverse):
    planes, width, depth = density.shape
    pencils, slabs = lax.axis_size("pencil"), lax.axis_size("slab")
    blocks, size = width_inverse.shape[:2]
    group = 2
    half = width // 2
    extra = -(-2 * half // depth // 8) * 8
    seg = half + extra
    chunks = next(k for k in range(5, seg) if seg // 8 % k == 0)
    chunk = seg // chunks
    vmem = pl.BlockSpec(memory_space=pltpu.VMEM)
    hbm = pl.BlockSpec(memory_space=pl.ANY)
    far = pl.BlockSpec(memory_space=pltpu.HBM)
    dma = pltpu.SemaphoreType.DMA
    field = jax.ShapeDtypeStruct((planes, width, depth), F32)
    faces = jax.ShapeDtypeStruct((2, width, depth), F32)
    table = jax.ShapeDtypeStruct((planes, depth), F32)
    line = pltpu.VMEM((seg, depth), F32)
    two = pltpu.VMEM((2, seg, depth), F32)
    steps = dma((chunks,))
    peers = dma((slabs - 1,))
    operands = (coupling, density, source, width_inverse, depth_inverse)
    z, face, table = pl.pallas_call(
        lambda *refs: step_kernel(group, pencils, slabs, chunk, 4, *refs),
        out_shape=(field, faces, table),
        in_specs=[far, far, far, far, far],
        out_specs=(vmem, vmem, vmem),
        scratch_shapes=[
            pltpu.SMEM(coupling.shape, F32),
            pltpu.VMEM(width_inverse.shape, F32),
            pltpu.VMEM(depth_inverse.shape, F32),
            pltpu.VMEM((planes, width + 16, depth), F32),
            pltpu.VMEM((planes, width, depth), F32),
            pltpu.VMEM((planes, 2 * seg, depth), F32),
            pltpu.VMEM((blocks, 2 * size, 2 * size), BF16),
            pltpu.VMEM((2 * size, 2 * size), BF16),
            pltpu.VMEM((2 * depth, 2 * depth), BF16),
            pltpu.VMEM((16, 2 * depth), BF16),
            pltpu.VMEM((-(-(3 * slabs + 3) // 8) * 8, depth), F32),
            pltpu.VMEM((width, depth), F32),
            pltpu.VMEM((width, depth), F32),
            pltpu.VMEM((blocks, 2 * planes, depth), F32),
            pltpu.VMEM((width, 2 * depth), BF16),
            two, two, two, line, line, line, line, two,
            pltpu.VMEM((2, 2 * seg, depth), F32),
            pltpu.VMEM((2, planes, width), F32),
            pltpu.VMEM((slabs, 2, planes, width), F32),
            pltpu.VMEM((2, planes, width), F32),
            pltpu.VMEM((16, half), F32),
            pltpu.VMEM((2, slabs, 8, half), F32),
            dma((4 + 8 * (half // depth),)), dma((3,)),
            steps, steps, steps, steps, steps, steps, steps, steps,
            peers, peers, peers, peers, dma((slabs,)), dma((slabs,)),
        ],
        compiler_params=pltpu.CompilerParams(
            vmem_limit_bytes=44 * 1024 * 1024, collective_id=0, has_side_effects=True
        ),
    )(*[pltpu.with_memory_space_constraint(array, pltpu.HBM) for array in operands])

    parts = 8
    return pl.pallas_call(
        lambda *refs: finish_kernel(parts, *refs),
        out_shape=field,
        in_specs=[vmem, vmem, vmem],
        out_specs=hbm,
        scratch_shapes=[pltpu.VMEM((planes, width, depth), F32), dma((parts,))],
        compiler_params=pltpu.CompilerParams(vmem_limit_bytes=32 * 1024 * 1024),
    )(z, face, table)


def solution(mesh):
    in_specs = (P("pencil", None, "slab"), P("pencil", None, "slab"), P(), P(), P(), P())
    out_specs = P("pencil", None, "slab")
    return jax.shard_map(
        per_device, mesh=mesh, in_specs=in_specs, out_specs=out_specs, check_vma=False
    )
```

```python
import jax
import jax.numpy as jnp
from jax import lax
from jax.experimental import pallas as pl
from jax.experimental.pallas import tpu as pltpu
from jax.sharding import PartitionSpec as P

F32, BF16 = jnp.float32, jnp.bfloat16
MESH = pl.DeviceIdType.MESH


def split(value):
    high = value.astype(BF16)
    return high, (value - high.astype(F32)).astype(BF16)


def both(value, axis):
    return jnp.concatenate(split(value), axis=axis)


def dot(a, b, dims):
    return lax.dot_general(a, b, (dims, ((), ())), preferred_element_type=F32)


def ends_of(plane):
    width, depth = plane.shape
    row = lax.broadcasted_iota(jnp.int32, (depth, depth), 0)
    lane = lax.broadcasted_iota(jnp.int32, (depth, depth), 1)
    lines = []
    for column in (0, depth - 1):
        pieces = []
        for start in range(0, width, depth):
            edge = plane[start : start + depth, column : column + 1]
            pieces.append(jnp.sum(jnp.where(row == lane, edge, 0.0), axis=0, keepdims=True))
        lines.append(jnp.concatenate(pieces, axis=1))
    return jnp.concatenate(lines, axis=0)


def rows_of(pieces, width):
    row = lax.broadcasted_iota(jnp.int32, (16, width), 0)
    value = jnp.zeros((16, width), F32)
    for number, piece in enumerate(pieces):
        value = jnp.where(row == number, piece.astype(F32), value)
    return value.astype(BF16)


def width_solve(rhs, strength, width_ref, mixed_ref):
    count, size = width_ref.shape[:2]
    total = rhs.shape[1]
    high, low = split(rhs)
    local, starts, stops = [], [], []
    for i in range(count):
        part = slice(i * size, (i + 1) * size)
        product = dot(mixed_ref[i], jnp.concatenate([high[part], low[part]], 0), ((1,), (0,)))
        local.append(product[:size] + product[size:])
        starts.append(strength * width_ref[i, :, 0:1])
        stops.append(strength * width_ref[i, :, size - 1 : size])
    carry = jnp.zeros((1, total), F32)
    ahead, heads = [], []
    for i in range(count):
        ahead.append(carry)
        heads.append(local[i][0:1] + starts[i][0:1] * carry)
        carry = local[i][size - 1 :] + starts[i][size - 1 :] * carry
    carry = jnp.zeros((1, total), F32)
    solved = [None] * count
    for i in reversed(range(count)):
        solved[i] = local[i] + starts[i] * ahead[i] + stops[i] * carry
        carry = heads[i] + stops[i][0:1] * carry
    return jnp.concatenate(solved, axis=0)


def depth_solve(value, mixed_depth):
    depth = value.shape[1]
    product = dot(both(value, 1), mixed_depth[...], ((1,), (0,)))
    return product[:, :depth] + product[:, depth:]


class Heights:
    def __init__(self, strength, lanes):
        self.shape = (1, lanes)
        self.strength = jnp.full(self.shape, strength, F32)
        root = (1.0 + 2.0 * self.strength + jnp.sqrt(1.0 + 4.0 * self.strength)) * 0.5
        self.log_ratio = jnp.log(self.strength / root)

    def power(self, index):
        return jnp.exp(jnp.full(self.shape, index, jnp.int32).astype(F32) * self.log_ratio)

    def tail(self, count):
        return 1.0 - self.power(2 * count)

    def beside(self, count):
        return self.power(1) * self.tail(count) / self.tail(count + 1)

    def enter(self, count, j):
        return self.power(j + 1) * self.tail(count - j) / self.tail(count + 1)


def named(label):
    def wrap(function):
        def inner(*args):
            with jax.named_scope(label):
                return function(*args)
        return inner
    return wrap


def rows_solve(pieces, strength, width_ref, mixed_ref):
    count, size = width_ref.shape[:2]
    local = []
    for i in range(count):
        product = dot(both(pieces[i], 1), mixed_ref[i], ((1,), (1,)))
        local.append(product[:, :size] + product[:, size:])
    carry = jnp.zeros((pieces[0].shape[0], 1), F32)
    ahead, heads = [], []
    for i in range(count):
        start = strength * width_ref[i, 0:1]
        ahead.append(start * carry)
        heads.append(local[i][:, 0:1] + start[:, 0:1] * carry)
        carry = local[i][:, size - 1 :] + start[:, size - 1 :] * carry
    carry = jnp.zeros((pieces[0].shape[0], 1), F32)
    solved = [None] * count
    for i in reversed(range(count)):
        stop = strength * width_ref[i, size - 1 : size]
        solved[i] = local[i] + ahead[i] + stop * carry
        carry = heads[i] + stop[:, 0:1] * carry
    return solved


def step_kernel(
    group, pencils, slabs, chunk, lag,
    coupling_hbm, rho_hbm, source_hbm, width_hbm, depth_hbm,
    z_ref, face_ref, coef_ref,
    coupling, width_ref, depth_ref,
    rho_ref, source_ref, y_ref, mixed_ref, mixed_depth,
    shifts, at_ends, links, rho_edges, z_edges, turned, columns,
    pair_out, pair_in, block, up_out, up_in, down_out, down_in, back_out, final,
    ends, gathered, carries, late, late_in,
    load_sem, table_sem, pair_send, pair_recv, up_send, up_recv, down_send, down_recv,
    back_send, back_recv, early_send, early_recv, own_send, own_recv, cross_send, cross_recv,
    more_send, more_recv,
):
    planes, width, depth = z_ref.shape
    groups = planes // group
    count, size = width_ref.shape[:2]
    half = width // 2
    seg = final.shape[1] // 2
    extra = seg - half
    chunks = seg // chunk
    strips = half // depth
    step = depth // 2
    cuts = half // step
    pad = 8
    me, slab = lax.axis_index("pencil"), lax.axis_index("slab")
    outer = pencils // 2
    z, x = lax.div(me, 2), lax.rem(me, 2)
    pair = z * 2 + 1 - x
    bottom, top = z == 0, z == outer - 1
    inside = (z > 0) & (z < outer - 1)
    outside = jnp.logical_not(inside)
    above_me = lax.rem(me + 2, pencils)
    below_me = lax.rem(me + pencils - 2, pencils)

    barrier = pltpu.get_barrier_semaphore()
    pl.semaphore_signal(barrier, inc=1, device_id={"pencil": pair}, device_id_type=MESH)

    @pl.when(z < outer - 1)
    def _():
        pl.semaphore_signal(barrier, inc=1, device_id={"pencil": above_me}, device_id_type=MESH)

    @pl.when(z > 0)
    def _():
        pl.semaphore_signal(barrier, inc=1, device_id={"pencil": below_me}, device_id_type=MESH)

    for k in range(1, slabs):
        peer = lax.rem(slab + k, slabs)
        for whom in ({"slab": peer}, {"pencil": pair, "slab": peer}):
            pl.semaphore_signal(barrier, inc=1, device_id=whom, device_id_type=MESH)

    loads = {}

    def load(key, src, dst, start, rows, shift):
        number = loads.setdefault(key, len(loads))
        return pltpu.make_async_copy(
            src.at[:, pl.ds(pl.multiple_of(start, 8), rows)],
            dst.at[:, pl.ds(pl.multiple_of(start + shift, 8), rows)],
            load_sem.at[number],
        )

    def rim(h, side):
        start = h * half + side * (half - 8)
        return load(("rim", h, side), rho_hbm, rho_ref, start, 8, pad)

    def main(turn, h, piece):
        low = 8 if piece == 0 else piece * step
        high = half - 8 if piece == cuts - 1 else (piece + 1) * step
        return load(("rho", turn, piece), rho_hbm, rho_ref, h * half + low, high - low, pad)

    def other(turn, h, piece):
        start = h * half + piece * step
        return load(("source", turn, piece), source_hbm, source_ref, start, step, 0)

    tables = [
        pltpu.make_async_copy(src, dst, table_sem.at[k])
        for k, (src, dst) in enumerate(
            ((coupling_hbm, coupling), (width_hbm, width_ref), (depth_hbm, depth_ref))
        )
    ]
    tables[0].start()
    for h in (0, 1):
        for side in (0, 1):
            rim(h, side).start()
    for turn, h in ((0, 1 - x), (1, x)):
        for piece in range(cuts):
            main(turn, h, piece).start()
            other(turn, h, piece).start()
        if turn == 0:
            tables[1].start()
            tables[2].start()

    rho_ref[:, :pad] = jnp.zeros((planes, pad, depth), F32)
    rho_ref[:, pad + width :] = jnp.zeros((planes, pad, depth), F32)
    tables[0].wait()
    heights = Heights(coupling[1], depth)
    for j in range(planes):
        coef_ref[j : j + 1] = heights.enter(planes, j)
    strength = heights.strength
    ahead = [heights.beside(j + 1) for j in range(planes)]
    pivot = [value / strength for value in ahead]
    near, far = heights.enter(planes, 0), heights.enter(planes, planes - 1)
    gain = 1.0 / (1.0 - near * near)
    near2, far2 = heights.enter(2 * planes, 0), heights.enter(2 * planes, 2 * planes - 1)
    under = heights.beside(2 * planes * z)
    over = heights.beside(2 * planes * (outer - 1 - z))
    under_gain, over_gain = 1.0 / (1.0 - under * near2), 1.0 / (1.0 - over * near2)
    det = 1.0 / ((1.0 - under * near2) * (1.0 - over * near2) - under * over * far2 * far2)
    k_uu, k_uo = (1.0 - over * near2) * det, under * far2 * det
    k_oo, k_ou = (1.0 - under * near2) * det, over * far2 * det

    lane = lax.broadcasted_iota(jnp.int32, (1, depth), 1)
    across, along = coupling[0], coupling[2]
    k_here = 2.0 - 4.0 * across - 4.0 * along
    source_row = lax.rem(lax.broadcasted_iota(jnp.int32, (2 * depth, depth), 0), depth)
    column = lax.broadcasted_iota(jnp.int32, (2 * depth, depth), 1)
    beside_it = (source_row == column + 1) | (source_row == column - 1)
    at_edge = source_row == jnp.where(lax.rem(column, 2) == 0, depth - 1, 0)
    shifts[:, :depth] = jnp.where(beside_it, 1.0, 0.0).astype(BF16)
    shifts[:, depth:] = jnp.where(at_edge, 1.0, 0.0).astype(BF16)

    def back_sweep(at, value):
        for j in reversed(range(planes)):
            if j == planes - 1:
                y = pivot[j] * value
            else:
                y = pivot[j] * (y_ref[j, at] + strength * y)
            y_ref[j, at] = y
        return y

    @named("sweep")
    def sweep(h, row, rows):
        base = pl.multiple_of(pad + h * half + row, 8)
        at = pl.ds(pl.multiple_of(h * seg + row, 8), rows)
        from_source = pl.ds(pl.multiple_of(h * half + row, 8), rows)
        value = None
        edges = jnp.zeros((rows, depth), F32)
        batch = 8
        for j in range(planes):
            if j % batch == 0:
                several = [rho_ref[j + k, pl.ds(base, rows)] for k in range(batch)]
                several = both(jnp.concatenate(several, axis=0), 1)
                all_shifted = dot(several, shifts[...], ((1,), (0,)))
            rho = rho_ref[j, pl.ds(base, rows)]
            beside = rho_ref[j, pl.ds(base - 1, rows)] + rho_ref[j, pl.ds(base + 1, rows)]
            shifted = all_shifted[j % batch * rows : (j % batch + 1) * rows]
            rhs = (
                source_ref[j, from_source]
                + k_here * rho
                + (2.0 * across) * beside
                + (2.0 * along) * shifted[:, :depth]
            )
            edges = jnp.where(lax.div(lane, 2) == j, shifted[:, depth:], edges)
            value = rhs if j == 0 else rhs + ahead[j - 1] * value
            y_ref[j, at] = value
        rho_edges[from_source] = edges
        last = pivot[planes - 1] * value
        first = back_sweep(at, value)
        return first, last

    @named("edge")
    def edge_sweep(h):
        at = pl.ds(pl.multiple_of(h * seg + half, 8), extra)
        value = None
        for strip in range(strips):
            start = pl.multiple_of(h * half + strip * depth, 8)
            rows = rho_edges[pl.ds(start, depth)].T
            for j in range(planes):
                to = pl.ds(h * seg + half + 2 * strip, 2)
                y_ref[j, to] = rows[2 * j : 2 * j + 2]
        spare = extra - 2 * strips
        y_ref[:, pl.ds(h * seg + half + 2 * strips, spare)] = jnp.zeros((planes, spare, depth), F32)
        for j in range(planes):
            rhs = y_ref[j, at]
            value = rhs if j == 0 else rhs + ahead[j - 1] * value
            y_ref[j, at] = value
        last = pivot[planes - 1] * value
        first = back_sweep(at, value)
        return first, last

    def remote(source, target, send, recv, peer):
        whom = peer if isinstance(peer, dict) else {"pencil": peer}
        return pltpu.make_async_remote_copy(
            src_ref=source, dst_ref=target, send_sem=send, recv_sem=recv,
            device_id=whom, device_id_type=MESH,
        )

    def rows_at(c, shift=0):
        return pl.ds(pl.multiple_of(c * chunk + shift, 8), chunk)

    def to_pair(c, slots):
        at = rows_at(c)
        return remote(
            pair_out.at[slots, at], pair_in.at[slots, at], pair_send.at[c], pair_recv.at[c], pair
        )

    def to_pair_later(c, slots):
        at = rows_at(c)
        return remote(
            pair_out.at[slots, at], pair_in.at[slots, at], more_send.at[c], more_recv.at[c], pair
        )

    def each_pair(act):
        @pl.when(inside)
        def _():
            act(pl.ds(0, 2))

        @pl.when(bottom)
        def _():
            act(pl.ds(1, 1))

        @pl.when(top)
        def _():
            act(pl.ds(0, 1))

    def each_more(act):
        @pl.when(bottom)
        def _():
            act(pl.ds(0, 1))

        @pl.when(top)
        def _():
            act(pl.ds(1, 1))

    def to_above(c):
        at = rows_at(c)
        return remote(up_out.at[at], up_in.at[at], up_send.at[c], up_recv.at[c], above_me)

    def to_below(c):
        at = rows_at(c)
        return remote(
            down_out.at[at], down_in.at[at], down_send.at[c], down_recv.at[c], below_me
        )

    def to_back(c, slots):
        return remote(
            back_out.at[slots, rows_at(c)], final.at[slots, rows_at(c, x * seg)],
            back_send.at[c], back_recv.at[c], pair,
        )

    def each_back(act):
        @pl.when(inside)
        def _():
            act(pl.ds(0, 2))

        @pl.when(bottom)
        def _():
            act(pl.ds(1, 1))

        @pl.when(top)
        def _():
            act(pl.ds(0, 1))

    def keep(turn, at, faces):
        first, last = faces
        if turn == 0:
            pair_out[0, at] = first
            pair_out[1, at] = last

            @pl.when(bottom & (x == 1))
            def _():
                pair_out[1, at] = last + far * gain * near * first

            @pl.when(top & (x == 0))
            def _():
                pair_out[0, at] = first + far * gain * near * last
        else:
            @pl.when(bottom & (x == 0))
            def _():
                pair_out[0, at] = last

            @pl.when(top & (x == 1))
            def _():
                pair_out[1, at] = first

    need = [min(cuts, -(-(c * chunk + chunk + 1) // step)) for c in range(chunks)]
    first_use = [next(c for c in range(chunks) if need[c] > piece) for piece in range(cuts)]

    def whole_chunk(turn, h, c):
        for piece in range(cuts):
            @pl.when(c == first_use[piece])
            def _():
                main(turn, h, piece).wait()
                other(turn, h, piece).wait()

        row = pl.multiple_of(c * chunk, 8)
        keep(turn, pl.ds(row, chunk), sweep(h, row, chunk))

    def last_chunk(turn, h):
        for piece in range(cuts):
            if first_use[piece] == chunks - 1:
                main(turn, h, piece).wait()
                other(turn, h, piece).wait()
        row = (chunks - 1) * chunk
        keep(turn, pl.ds(row, half - row), sweep(h, row, half - row))
        keep(turn, pl.ds(half, extra), edge_sweep(h))

    for h in (0, 1):
        for side in (0, 1):
            rim(h, side).wait()

    def prepare():
        tables[1].wait()
        tables[2].wait()
        for i in range(count):
            high, low = split(width_ref[i])
            mixed_ref[i, :size, :size] = high
            mixed_ref[i, :size, size:] = high
            mixed_ref[i, size:, :size] = low
            mixed_ref[i, size:, size:] = jnp.zeros_like(low)
        def spot(d, row, column):
            return depth_ref[d, row : row + 1, column : column + 1]

        for d in range(slabs):
            for k, (row, column) in enumerate(((0, 0), (0, size - 1), (size - 1, 0))):
                value = coupling[2] * spot(d, row, column)
                links[3 * d + k : 3 * d + k + 1] = jnp.broadcast_to(value, (1, depth))
        corner = spot(jnp.where(slab > 0, slab - 1, 0), size - 1, size - 1)
        corner = 2.0 * coupling[2] * jnp.where(slab > 0, corner, jnp.zeros_like(corner))
        for k, value in enumerate(
            (
                corner, corner * coupling[2] * spot(slab, 0, 0),
                corner * coupling[2] * spot(slab, size - 1, 0),
            )
        ):
            links[3 * slabs + k : 3 * slabs + k + 1] = jnp.broadcast_to(value, (1, depth))
        first_high, first_low = split(depth_ref[slab, 0:1])
        last_high, last_low = split(depth_ref[slab, size - 1 : size])
        nothing = jnp.zeros((1, depth), F32)
        at_ends[...] = rows_of(
            [
                jnp.concatenate([piece.astype(F32), tail], axis=1)
                for piece, tail in (
                    (first_high, first_high.astype(F32)), (last_high, last_high.astype(F32)),
                    (first_low, nothing), (last_low, nothing),
                )
            ],
            2 * depth,
        )
        high, low = split(depth_ref[slab])
        mixed_depth[:size, :size] = high
        mixed_depth[size:, :size] = high
        mixed_depth[:size, size:] = low
        mixed_depth[size:, size:] = jnp.zeros_like(low)

    @pl.when(z == 0)
    def _():
        up_in[...] = jnp.zeros_like(up_in)

    @pl.when(z == outer - 1)
    def _():
        down_in[...] = jnp.zeros_like(down_in)

    @pl.when(outside)
    def _():
        block[...] = jnp.zeros_like(block)

    @named("pair")
    def do_pair(c):
        each_pair(lambda slots: to_pair(c, slots).wait_recv())
        at, mine = rows_at(c), rows_at(c, x * seg)
        own_first, own_last = y_ref[0, mine], y_ref[planes - 1, mine]
        lower = x == 0

        @pl.when(inside)
        def _():
            its_first, its_last = pair_in[0, at], pair_in[1, at]
            f0, l0 = jnp.where(lower, own_first, its_first), jnp.where(lower, own_last, its_last)
            f1, l1 = jnp.where(lower, its_first, own_first), jnp.where(lower, its_last, own_last)
            block[0, at] = f0 + far * gain * (f1 + near * l0)
            block[1, at] = l1 + far * gain * (l0 + near * f1)

        @pl.when(bottom)
        def _():
            its = pair_in[1, at]
            block[1, at] = jnp.where(
                lower, its + far * gain * own_last, own_last + far * gain * (its + near * own_first)
            )

        @pl.when(top)
        def _():
            its = pair_in[0, at]
            block[0, at] = jnp.where(
                lower, own_first + far * gain * (its + near * own_last), its + far * gain * own_first
            )

    @named("up")
    def do_up(c):
        @pl.when(z > 0)
        def _():
            to_above(c).wait_recv()

        at = rows_at(c)

        @pl.when(z < outer - 1)
        def _():
            up_out[at] = block[1, at] + far2 * under_gain * (up_in[at] + under * block[0, at])
            to_above(c).start()

    @named("down")
    def do_down(c):
        @pl.when(z < outer - 1)
        def _():
            to_below(c).wait_recv()

        at = rows_at(c)

        @pl.when(z > 0)
        def _():
            down_out[at] = block[0, at] + far2 * over_gain * (down_in[at] + over * block[1, at])
            to_below(c).start()

    @named("done")
    def do_final(c):
        at, mine = rows_at(c), rows_at(c, x * seg)
        low = up_in[at] + under * block[0, at]
        high = down_in[at] + over * block[1, at]
        enter = k_uu * low + k_uo * high
        leave = k_ou * low + k_oo * high
        each_more(lambda slots: to_pair_later(c, slots).wait_recv())
        l0 = jnp.where(x == 0, y_ref[planes - 1, mine], pair_in[1, at]) + far * enter
        f1 = jnp.where(x == 0, pair_in[0, at], y_ref[0, mine]) + far * leave
        inner_low = gain * (l0 + near * f1)
        inner_high = gain * (f1 + near * l0)
        lower = x == 0
        final[0, mine] = jnp.where(lower, enter, inner_low)
        final[1, mine] = jnp.where(lower, inner_high, leave)
        back_out[0, at] = jnp.where(lower, inner_low, enter)
        back_out[1, at] = jnp.where(lower, leave, inner_high)
        each_back(lambda slots: to_back(c, slots).start())

    def blocks_at(i):
        return pl.ds(i // strips * seg + i % strips * size, size)

    @named("mid")
    def solve_planes(index):
        base = index * group
        rhs = jnp.concatenate(
            [
                jnp.concatenate(
                    [
                        y_ref[base + g, blocks_at(i)]
                        - 2.0 * rho_ref[base + g, pl.ds(pad + i * size, size)]
                        for i in range(count)
                    ],
                    axis=0,
                )
                for g in range(group)
            ],
            axis=1,
        )
        solved = width_solve(rhs, coupling[0], width_ref, mixed_ref)
        answers = [
            depth_solve(solved[:, g * depth : (g + 1) * depth], mixed_depth) for g in range(group)
        ]
        for g in range(group):
            z_ref[base + g] = answers[g] + rho_ref[base + g, pl.ds(pad, width)]
            rolled = pltpu.roll(answers[g], 2 * (base + g) + 1, 1)
            z_edges[...] = jnp.where(lax.div(lane, 2) == base + g, rolled, z_edges[...])

    def turn_rows(source, i, rows):
        turned[i] = source[pl.ds(i * size, size)].T[: turned.shape[1]]
        return [turned[i, pl.ds(edge, rows, stride=2)] for edge in (1, 0)]

    def link(d, row, column):
        return like(3 * d + 2 * (row > 0) + (column > 0))

    def like(number, lanes=width):
        return jnp.concatenate([links[number : number + 1]] * (lanes // depth), axis=1)

    def with_edges(edge, ends_value, v_first, v_own):
        return ends_value + 2.0 * v_own + like(3 * slabs + 1 + (edge > 0), v_first.shape[1]) * v_first

    @named("early")
    def early_edges():
        pieces = []
        for i in range(count):
            h, strip = i // strips, i % strips
            rows = [
                y_ref[:, h * seg + half + 2 * strip + 1 - edge, :] for edge in (0, 1)
            ]
            pieces.append(jnp.concatenate(rows, axis=0))
        value = jnp.concatenate(rows_solve(pieces, coupling[0], width_ref, mixed_ref), axis=1)
        first, last = value[:planes], value[planes:]
        carries[0] = first
        lines = [turn_rows(z_edges, i, planes) for i in range(count)]
        lines = [jnp.concatenate([line[edge] for line in lines], axis=1) for edge in (0, 1)]
        ends[0] = with_edges(0, lines[0], first, first)
        ends[1] = with_edges(1, lines[1], first, last)
        for k in range(1, slabs):
            early(k).start()
        gathered[slab] = ends[...]

    def early(k):
        return remote(
            ends, gathered.at[slab], early_send.at[k - 1], early_recv.at[k - 1],
            {"slab": lax.rem(slab + k, slabs)},
        )

    def late_own(k):
        return remote(
            late.at[pl.ds(0, 6)], late_in.at[x, slab, pl.ds(0, 6)],
            own_send.at[k - 1], own_recv.at[k - 1], {"slab": lax.rem(slab + k, slabs)},
        )

    def late_cross(k):
        return remote(
            late.at[pl.ds(8, 6)], late_in.at[x, slab, pl.ds(0, 6)],
            cross_send.at[k], cross_recv.at[k],
            {"pencil": pair, "slab": lax.rem(slab + k, slabs)},
        )

    @named("late_edges")
    def late_edges():
        for who in range(2):
            for side in range(2):
                if who == 0:
                    plane = final[side, pl.ds(pl.multiple_of(x * seg, 8), half)]
                    rows = final[side, pl.ds(pl.multiple_of(x * seg + half, 8), extra)]
                else:
                    plane = back_out[side, pl.ds(0, half)]
                    rows = back_out[side, pl.ds(half, extra)]
                lines = dot(at_ends[...], both(plane, 1), ((1,), (1,)))
                first, last = lines[0:1] + lines[2:3], lines[1:2] + lines[3:4]
                v_last, v_first = (
                    jnp.concatenate(
                        [rows[2 * strip + k : 2 * strip + k + 1] for strip in range(strips)], axis=1
                    )
                    for k in (0, 1)
                )
                row = 8 * who + side
                late[row : row + 1] = with_edges(0, first, v_first, v_first)
                late[row + 2 : row + 3] = with_edges(1, last, v_first, v_last)
                late[row + 4 : row + 5] = v_first
        for k in range(1, slabs):
            late_own(k).start()
        for k in range(slabs):
            late_cross(k).start()
        late_in[x, slab, 0:6] = late[0:6]

    def chain(first_of, last_of, v_first):
        zero = jnp.zeros_like(v_first)
        forward = [zero]
        for d in range(slabs - 1):
            forward.append(last_of(d) + link(d, size - 1, 0) * forward[d])
        backward = [zero] * slabs
        for d in range(slabs - 1, 0, -1):
            backward[d - 1] = (
                first_of(d) + link(d, 0, 0) * forward[d] + link(d, 0, size - 1) * backward[d]
            )
        carry_in, carry_next = forward[0], backward[0]
        for d in range(1, slabs):
            carry_in = jnp.where(slab == d, forward[d], carry_in)
            carry_next = jnp.where(slab == d, backward[d], carry_next)
        return carry_in + like(3 * slabs) * v_first, carry_next

    n = chunks - 1
    turn_tick = (n + 1) // 2
    first_pair = turn_tick + 2
    pairs = (chunks + 1) // 2
    heavy = chunks - 1
    ticks = max(first_pair + lag * (outer - 1) + pairs, heavy + groups + 1)

    def tick(t, unused):
        def for_pair(c, same):
            whole_chunk(0, 1 - x, c)

            @pl.when(c == 0)
            def _():
                @pl.when(inside)
                def _():
                    pl.semaphore_wait(barrier, 3 + 2 * (slabs - 1))

                @pl.when(outside)
                def _():
                    pl.semaphore_wait(barrier, 2 + 2 * (slabs - 1))

            each_pair(lambda slots: to_pair(c, slots).start())
            return same

        def for_us(c, same):
            whole_chunk(1, x, c)
            return same

        lax.fori_loop(jnp.minimum(2 * t, n), jnp.minimum(2 * t + 2, n), for_pair, 0)

        @pl.when(t == turn_tick)
        def _():
            last_chunk(0, 1 - x)
            each_pair(lambda slots: to_pair(n, slots).start())

        ours = 2 * (t - turn_tick)
        lax.fori_loop(jnp.clip(ours - 1, 0, n), jnp.clip(ours + 1, 0, n), for_us, 0)

        @pl.when(t == turn_tick + n // 2)
        def _():
            last_chunk(1, x)
            prepare()

            def more(c, same):
                each_more(lambda slots: to_pair_later(c, slots).start())
                return same

            lax.fori_loop(0, chunks, more, 0)

        rel = t - first_pair
        low = jnp.where(rel < 2, 2 * rel, rel + 1)
        high = low + jnp.where(rel < 2, 2, jnp.where(rel == 2, 0, 1))

        @pl.when(inside)
        def _():
            def one_pair(c, same):
                do_pair(c)
                return same

            lax.fori_loop(jnp.clip(low, 0, chunks), jnp.clip(high, 0, chunks), one_pair, 0)

        def in_twos(hops, act):
            number = 2 * (t - first_pair - lag * hops)

            def one(c, same):
                act(c)
                return same

            lax.fori_loop(jnp.clip(number, 0, chunks), jnp.clip(number + 2, 0, chunks), one, 0)
            return number

        @pl.when(outside)
        def _():
            in_twos(0, do_pair)

        in_twos(z, do_up)
        in_twos(outer - 1 - z, do_down)
        most = in_twos(jnp.maximum(z, outer - 1 - z), do_final)

        @pl.when((most < chunks) & (most + 2 >= chunks))
        def _():
            late_edges()

        @pl.when((t >= heavy) & (t < heavy + groups))
        def _():
            solve_planes(t - heavy)

        @pl.when(t == heavy + groups)
        def _():
            early_edges()

        return unused

    lax.fori_loop(0, ticks, tick, 0)

    with jax.named_scope("early_wait"):
        for k in range(1, slabs):
            early(k).wait()
    wide = 4
    in_row = coupling[2] * depth_ref[slab, 0:1]
    next_row = coupling[2] * depth_ref[slab, size - 1 : size]
    (in_high, in_low), (next_high, next_low) = split(in_row), split(next_row)
    spots = lax.broadcasted_iota(jnp.int32, (2 * depth, depth), 0)
    number, spot = lax.div(spots, planes), lax.rem(spots, planes)
    lows = depth // planes
    base = jnp.zeros((2 * depth, depth), F32)
    for k, piece in (
        (0, in_high), (1, next_high), (2, in_low), (3, next_low),
        (lows, in_high), (lows + 1, next_high),
    ):
        base = jnp.where(number == k, piece.astype(F32), base)
    carry_in, carry_next = chain(
        lambda d: gathered[d, 0], lambda d: gathered[d, 1], carries[0]
    )
    lines = jnp.concatenate([carry_in, carry_next] * 2, axis=0)
    lines = jnp.concatenate([lines, jnp.zeros((depth - 4 * planes, width), F32)], axis=0)
    for i in range(count):
        part = slice(i * size, (i + 1) * size)
        columns[part] = both(lines[:, part].T, 1)

    @named("fix")
    def finish_planes(index, unused):
        j = index * wide
        rhs = jnp.concatenate([jnp.where(spot == j + g, base, 0.0) for g in range(wide)], axis=1)
        both_planes = dot(columns[...], rhs.astype(BF16), ((1,), (0,)))
        for g in range(wide):
            z_ref[j + g] = z_ref[j + g] + both_planes[:, g * depth : (g + 1) * depth]
        return unused

    lax.fori_loop(0, planes // wide, finish_planes, 0)
    def depth_part(h):
        for side in range(2):
            rows = final[side, pl.ds(pl.multiple_of(h * seg, 8), half)]
            to = pl.ds(pl.multiple_of(h * half, 8), half)
            face_ref[side, to] = depth_solve(rows, mixed_depth)

    depth_part(x)

    @named("back")
    def wait_back(c, unused):
        each_back(lambda slots: to_back(c, slots).wait())
        at, theirs = rows_at(c), rows_at(c, (1 - x) * seg)

        @pl.when(bottom & (x == 0))
        def _():
            final[0, theirs] = jnp.zeros((chunk, depth), F32)

        @pl.when(bottom & (x == 1))
        def _():
            leave = y_ref[0, theirs] + far * final[1, theirs]
            final[0, theirs] = gain * (pair_in[0, at] + near * leave)

        @pl.when(top & (x == 0))
        def _():
            enter = y_ref[planes - 1, theirs] + far * final[0, theirs]
            final[1, theirs] = gain * (pair_in[1, at] + near * enter)

        @pl.when(top & (x == 1))
        def _():
            final[1, theirs] = jnp.zeros((chunk, depth), F32)

        return unused

    lax.fori_loop(0, chunks, wait_back, 0)
    with jax.named_scope("late_depth"):
        depth_part(1 - x)

    with jax.named_scope("late_wait"):
        for k in range(1, slabs):
            late_own(k).wait()
        for k in range(slabs):
            late_cross(k).wait()

    def late_rows(d, row):
        return jnp.concatenate([late_in[h, d, row : row + 2] for h in range(2)], axis=1)

    with jax.named_scope("late_chain"):
        carry_in, carry_next = chain(
            lambda d: late_rows(d, 0), lambda d: late_rows(d, 2), late_rows(slab, 4)
        )
        pieces = []
        for side in range(2):
            (a_high, a_low), (b_high, b_low) = split(carry_in[side : side + 1]), split(carry_next[side : side + 1])
            pieces += [a_high, a_low, a_high, b_high, b_low, b_high]
        six = (in_high, in_high, in_low, next_high, next_high, next_low)
        blank = jnp.zeros((1, depth), F32)
        row_pairs = [jnp.concatenate([piece.astype(F32), blank], axis=1) for piece in six]
        row_pairs += [jnp.concatenate([blank, piece.astype(F32)], axis=1) for piece in six]
        spread = dot(rows_of(pieces, width), rows_of(row_pairs, 2 * depth), ((0,), (0,)))

    with jax.named_scope("late_solve"):
        sides = [face_ref[side] + spread[:, side * depth : (side + 1) * depth] for side in range(2)]
        solved = width_solve(jnp.concatenate(sides, axis=1), coupling[0], width_ref, mixed_ref)
        for side in range(2):
            face_ref[side] = solved[:, side * depth : (side + 1) * depth]

    @named("sent")
    def wait_sent(c, unused):
        each_pair(lambda slots: to_pair(c, slots).wait_send())
        each_more(lambda slots: to_pair_later(c, slots).wait_send())

        @pl.when(z < outer - 1)
        def _():
            to_above(c).wait_send()

        @pl.when(z > 0)
        def _():
            to_below(c).wait_send()

        return unused

    lax.fori_loop(0, chunks, wait_sent, 0)


def finish_kernel(parts, z_ref, face_ref, coef_ref, out_hbm, out_ref, sem):
    planes, width, depth = z_ref.shape
    rows = width // parts

    def store(c):
        at = pl.ds(pl.multiple_of(c * rows, 8), rows)
        return pltpu.make_async_copy(out_ref.at[:, at], out_hbm.at[:, at], sem.at[c])

    def part(c, unused):
        at = pl.ds(pl.multiple_of(c * rows, 8), rows)
        enter, leave = face_ref[0, at], face_ref[1, at]
        for j in range(planes):
            k = planes - 1 - j
            out_ref[j, at] = z_ref[j, at] + coef_ref[j : j + 1] * enter + coef_ref[k : k + 1] * leave
        store(c).start()
        return unused

    lax.fori_loop(0, parts, part, 0)

    def drain(c, unused):
        store(c).wait()
        return unused

    lax.fori_loop(0, parts, drain, 0)


def per_device(density, source, coupling, width_inverse, height_inverse, depth_inverse):
    planes, width, depth = density.shape
    pencils, slabs = lax.axis_size("pencil"), lax.axis_size("slab")
    blocks, size = width_inverse.shape[:2]
    group = 2
    half = width // 2
    extra = -(-2 * half // depth // 8) * 8
    seg = half + extra
    chunks = next(k for k in range(5, seg) if seg // 8 % k == 0)
    chunk = seg // chunks
    vmem = pl.BlockSpec(memory_space=pltpu.VMEM)
    hbm = pl.BlockSpec(memory_space=pl.ANY)
    far = pl.BlockSpec(memory_space=pltpu.HBM)
    dma = pltpu.SemaphoreType.DMA
    field = jax.ShapeDtypeStruct((planes, width, depth), F32)
    faces = jax.ShapeDtypeStruct((2, width, depth), F32)
    table = jax.ShapeDtypeStruct((planes, depth), F32)
    line = pltpu.VMEM((seg, depth), F32)
    two = pltpu.VMEM((2, seg, depth), F32)
    steps = dma((chunks,))
    peers = dma((slabs - 1,))
    operands = (coupling, density, source, width_inverse, depth_inverse)
    z, face, table = pl.pallas_call(
        lambda *refs: step_kernel(group, pencils, slabs, chunk, 3, *refs),
        out_shape=(field, faces, table),
        in_specs=[far, far, far, far, far],
        out_specs=(vmem, vmem, vmem),
        scratch_shapes=[
            pltpu.SMEM(coupling.shape, F32),
            pltpu.VMEM(width_inverse.shape, F32),
            pltpu.VMEM(depth_inverse.shape, F32),
            pltpu.VMEM((planes, width + 16, depth), F32),
            pltpu.VMEM((planes, width, depth), F32),
            pltpu.VMEM((planes, 2 * seg, depth), F32),
            pltpu.VMEM((blocks, 2 * size, 2 * size), BF16),
            pltpu.VMEM((2 * size, 2 * size), BF16),
            pltpu.VMEM((2 * depth, 2 * depth), BF16),
            pltpu.VMEM((16, 2 * depth), BF16),
            pltpu.VMEM((-(-(3 * slabs + 3) // 8) * 8, depth), F32),
            pltpu.VMEM((width, depth), F32),
            pltpu.VMEM((width, depth), F32),
            pltpu.VMEM((blocks, 2 * planes, depth), F32),
            pltpu.VMEM((width, 2 * depth), BF16),
            two, two, two, line, line, line, line, two,
            pltpu.VMEM((2, 2 * seg, depth), F32),
            pltpu.VMEM((2, planes, width), F32),
            pltpu.VMEM((slabs, 2, planes, width), F32),
            pltpu.VMEM((2, planes, width), F32),
            pltpu.VMEM((16, half), F32),
            pltpu.VMEM((2, slabs, 8, half), F32),
            dma((4 + 8 * (half // depth),)), dma((3,)),
            steps, steps, steps, steps, steps, steps, steps, steps,
            peers, peers, peers, peers, dma((slabs,)), dma((slabs,)), steps, steps,
        ],
        compiler_params=pltpu.CompilerParams(
            vmem_limit_bytes=44 * 1024 * 1024, collective_id=0, has_side_effects=True
        ),
    )(*[pltpu.with_memory_space_constraint(array, pltpu.HBM) for array in operands])

    parts = 8
    return pl.pallas_call(
        lambda *refs: finish_kernel(parts, *refs),
        out_shape=field,
        in_specs=[vmem, vmem, vmem],
        out_specs=hbm,
        scratch_shapes=[pltpu.VMEM((planes, width, depth), F32), dma((parts,))],
        compiler_params=pltpu.CompilerParams(vmem_limit_bytes=32 * 1024 * 1024),
    )(z, face, table)


def solution(mesh):
    in_specs = (P("pencil", None, "slab"), P("pencil", None, "slab"), P(), P(), P(), P())
    out_specs = P("pencil", None, "slab")
    return jax.shard_map(
        per_device, mesh=mesh, in_specs=in_specs, out_specs=out_specs, check_vma=False
    )
```

```python
import jax
import jax.numpy as jnp
from jax import lax
from jax.experimental import pallas as pl
from jax.experimental.pallas import tpu as pltpu
from jax.sharding import PartitionSpec as P

F32, BF16 = jnp.float32, jnp.bfloat16
MESH = pl.DeviceIdType.MESH


def split(value):
    high = value.astype(BF16)
    return high, (value - high.astype(F32)).astype(BF16)


def both(value, axis):
    return jnp.concatenate(split(value), axis=axis)


def dot(a, b, dims):
    return lax.dot_general(a, b, (dims, ((), ())), preferred_element_type=F32)


def ends_of(plane):
    width, depth = plane.shape
    row = lax.broadcasted_iota(jnp.int32, (depth, depth), 0)
    lane = lax.broadcasted_iota(jnp.int32, (depth, depth), 1)
    lines = []
    for column in (0, depth - 1):
        pieces = []
        for start in range(0, width, depth):
            edge = plane[start : start + depth, column : column + 1]
            pieces.append(jnp.sum(jnp.where(row == lane, edge, 0.0), axis=0, keepdims=True))
        lines.append(jnp.concatenate(pieces, axis=1))
    return jnp.concatenate(lines, axis=0)


def rows_of(pieces, width):
    row = lax.broadcasted_iota(jnp.int32, (16, width), 0)
    value = jnp.zeros((16, width), F32)
    for number, piece in enumerate(pieces):
        value = jnp.where(row == number, piece.astype(F32), value)
    return value.astype(BF16)


def width_solve(rhs, strength, width_ref, mixed_ref):
    count, size = width_ref.shape[:2]
    total = rhs.shape[1]
    high, low = split(rhs)
    local, starts, stops = [], [], []
    for i in range(count):
        part = slice(i * size, (i + 1) * size)
        product = dot(mixed_ref[i], jnp.concatenate([high[part], low[part]], 0), ((1,), (0,)))
        local.append(product[:size] + product[size:])
        starts.append(strength * width_ref[i, :, 0:1])
        stops.append(strength * width_ref[i, :, size - 1 : size])
    carry = jnp.zeros((1, total), F32)
    ahead, heads = [], []
    for i in range(count):
        ahead.append(carry)
        heads.append(local[i][0:1] + starts[i][0:1] * carry)
        carry = local[i][size - 1 :] + starts[i][size - 1 :] * carry
    carry = jnp.zeros((1, total), F32)
    solved = [None] * count
    for i in reversed(range(count)):
        solved[i] = local[i] + starts[i] * ahead[i] + stops[i] * carry
        carry = heads[i] + stops[i][0:1] * carry
    return jnp.concatenate(solved, axis=0)


def depth_solve(value, mixed_depth):
    depth = value.shape[1]
    product = dot(both(value, 1), mixed_depth[...], ((1,), (0,)))
    return product[:, :depth] + product[:, depth:]


class Heights:
    def __init__(self, strength, lanes):
        self.shape = (1, lanes)
        self.strength = jnp.full(self.shape, strength, F32)
        root = (1.0 + 2.0 * self.strength + jnp.sqrt(1.0 + 4.0 * self.strength)) * 0.5
        self.log_ratio = jnp.log(self.strength / root)

    def power(self, index):
        return jnp.exp(jnp.full(self.shape, index, jnp.int32).astype(F32) * self.log_ratio)

    def tail(self, count):
        return 1.0 - self.power(2 * count)

    def beside(self, count):
        return self.power(1) * self.tail(count) / self.tail(count + 1)

    def enter(self, count, j):
        return self.power(j + 1) * self.tail(count - j) / self.tail(count + 1)


def named(label):
    def wrap(function):
        def inner(*args):
            with jax.named_scope(label):
                return function(*args)
        return inner
    return wrap


def rows_solve(pieces, strength, width_ref, mixed_ref):
    count, size = width_ref.shape[:2]
    local = []
    for i in range(count):
        product = dot(both(pieces[i], 1), mixed_ref[i], ((1,), (1,)))
        local.append(product[:, :size] + product[:, size:])
    carry = jnp.zeros((pieces[0].shape[0], 1), F32)
    ahead, heads = [], []
    for i in range(count):
        start = strength * width_ref[i, 0:1]
        ahead.append(start * carry)
        heads.append(local[i][:, 0:1] + start[:, 0:1] * carry)
        carry = local[i][:, size - 1 :] + start[:, size - 1 :] * carry
    carry = jnp.zeros((pieces[0].shape[0], 1), F32)
    solved = [None] * count
    for i in reversed(range(count)):
        stop = strength * width_ref[i, size - 1 : size]
        solved[i] = local[i] + ahead[i] + stop * carry
        carry = heads[i] + stop[:, 0:1] * carry
    return solved


def step_kernel(
    group, pencils, slabs, chunk, lag,
    coupling_hbm, rho_hbm, source_hbm, width_hbm, depth_hbm,
    z_ref, face_ref, coef_ref,
    coupling, width_ref, depth_ref,
    rho_ref, source_ref, y_ref, mixed_ref, mixed_depth,
    shifts, at_ends, links, rho_edges, z_edges, turned, columns,
    pair_out, pair_in, block, up_out, up_in, down_out, down_in, back_out, final,
    ends, gathered, carries, late, late_in,
    load_sem, table_sem, pair_send, pair_recv, up_send, up_recv, down_send, down_recv,
    back_send, back_recv, early_send, early_recv, own_send, own_recv, cross_send, cross_recv,
):
    planes, width, depth = z_ref.shape
    groups = planes // group
    count, size = width_ref.shape[:2]
    half = width // 2
    seg = final.shape[1] // 2
    extra = seg - half
    chunks = seg // chunk
    strips = half // depth
    step = depth // 2
    cuts = half // step
    pad = 8
    me, slab = lax.axis_index("pencil"), lax.axis_index("slab")
    outer = pencils // 2
    z, x = lax.div(me, 2), lax.rem(me, 2)
    pair = z * 2 + 1 - x
    bottom, top = z == 0, z == outer - 1
    inside = (z > 0) & (z < outer - 1)
    gives_more = (bottom & (x == 0)) | (top & (x == 1))
    above_me = lax.rem(me + 2, pencils)
    below_me = lax.rem(me + pencils - 2, pencils)

    barrier = pltpu.get_barrier_semaphore()
    pl.semaphore_signal(barrier, inc=1, device_id={"pencil": pair}, device_id_type=MESH)

    @pl.when(z < outer - 1)
    def _():
        pl.semaphore_signal(barrier, inc=1, device_id={"pencil": above_me}, device_id_type=MESH)

    @pl.when(z > 0)
    def _():
        pl.semaphore_signal(barrier, inc=1, device_id={"pencil": below_me}, device_id_type=MESH)

    for k in range(1, slabs):
        peer = lax.rem(slab + k, slabs)
        for whom in ({"slab": peer}, {"pencil": pair, "slab": peer}):
            pl.semaphore_signal(barrier, inc=1, device_id=whom, device_id_type=MESH)

    loads = {}

    def load(key, src, dst, start, rows, shift):
        number = loads.setdefault(key, len(loads))
        return pltpu.make_async_copy(
            src.at[:, pl.ds(pl.multiple_of(start, 8), rows)],
            dst.at[:, pl.ds(pl.multiple_of(start + shift, 8), rows)],
            load_sem.at[number],
        )

    def rim(h, side):
        start = h * half + side * (half - 8)
        return load(("rim", h, side), rho_hbm, rho_ref, start, 8, pad)

    def main(turn, h, piece):
        low = 8 if piece == 0 else piece * step
        high = half - 8 if piece == cuts - 1 else (piece + 1) * step
        return load(("rho", turn, piece), rho_hbm, rho_ref, h * half + low, high - low, pad)

    def other(turn, h, piece):
        start = h * half + piece * step
        return load(("source", turn, piece), source_hbm, source_ref, start, step, 0)

    tables = [
        pltpu.make_async_copy(src, dst, table_sem.at[k])
        for k, (src, dst) in enumerate(
            ((coupling_hbm, coupling), (width_hbm, width_ref), (depth_hbm, depth_ref))
        )
    ]
    tables[0].start()
    for h in (0, 1):
        for side in (0, 1):
            rim(h, side).start()
    for piece in range(cuts):
        for turn, h in ((0, 1 - x), (1, x)):
            main(turn, h, piece).start()
            other(turn, h, piece).start()
        if piece == 0:
            tables[1].start()
            tables[2].start()

    rho_ref[:, :pad] = jnp.zeros((planes, pad, depth), F32)
    rho_ref[:, pad + width :] = jnp.zeros((planes, pad, depth), F32)
    tables[0].wait()
    heights = Heights(coupling[1], depth)
    for j in range(planes):
        coef_ref[j : j + 1] = heights.enter(planes, j)
    strength = heights.strength
    ahead = [heights.beside(j + 1) for j in range(planes)]
    pivot = [value / strength for value in ahead]
    near, far = heights.enter(planes, 0), heights.enter(planes, planes - 1)
    gain = 1.0 / (1.0 - near * near)
    near2, far2 = heights.enter(2 * planes, 0), heights.enter(2 * planes, 2 * planes - 1)
    under = heights.beside(2 * planes * z)
    over = heights.beside(2 * planes * (outer - 1 - z))
    under_gain, over_gain = 1.0 / (1.0 - under * near2), 1.0 / (1.0 - over * near2)
    det = 1.0 / ((1.0 - under * near2) * (1.0 - over * near2) - under * over * far2 * far2)
    k_uu, k_uo = (1.0 - over * near2) * det, under * far2 * det
    k_oo, k_ou = (1.0 - under * near2) * det, over * far2 * det

    lane = lax.broadcasted_iota(jnp.int32, (1, depth), 1)
    across, along = coupling[0], coupling[2]
    k_here = 2.0 - 4.0 * across - 4.0 * along
    source_row = lax.rem(lax.broadcasted_iota(jnp.int32, (2 * depth, depth), 0), depth)
    column = lax.broadcasted_iota(jnp.int32, (2 * depth, depth), 1)
    beside_it = (source_row == column + 1) | (source_row == column - 1)
    at_edge = source_row == jnp.where(lax.rem(column, 2) == 0, depth - 1, 0)
    shifts[:, :depth] = jnp.where(beside_it, 1.0, 0.0).astype(BF16)
    shifts[:, depth:] = jnp.where(at_edge, 1.0, 0.0).astype(BF16)

    def back_sweep(at, value):
        for j in reversed(range(planes)):
            if j == planes - 1:
                y = pivot[j] * value
            else:
                y = pivot[j] * (y_ref[j, at] + strength * y)
            y_ref[j, at] = y
        return y

    @named("sweep")
    def sweep(h, row, rows):
        base = pl.multiple_of(pad + h * half + row, 8)
        at = pl.ds(pl.multiple_of(h * seg + row, 8), rows)
        from_source = pl.ds(pl.multiple_of(h * half + row, 8), rows)
        value = None
        edges = jnp.zeros((rows, depth), F32)
        batch = 8
        for j in range(planes):
            if j % batch == 0:
                several = [rho_ref[j + k, pl.ds(base, rows)] for k in range(batch)]
                several = both(jnp.concatenate(several, axis=0), 1)
                all_shifted = dot(several, shifts[...], ((1,), (0,)))
            rho = rho_ref[j, pl.ds(base, rows)]
            beside = rho_ref[j, pl.ds(base - 1, rows)] + rho_ref[j, pl.ds(base + 1, rows)]
            shifted = all_shifted[j % batch * rows : (j % batch + 1) * rows]
            rhs = (
                source_ref[j, from_source]
                + k_here * rho
                + (2.0 * across) * beside
                + (2.0 * along) * shifted[:, :depth]
            )
            edges = jnp.where(lax.div(lane, 2) == j, shifted[:, depth:], edges)
            value = rhs if j == 0 else rhs + ahead[j - 1] * value
            y_ref[j, at] = value
        rho_edges[from_source] = edges
        last = pivot[planes - 1] * value
        first = back_sweep(at, value)
        return first, last

    @named("edge")
    def edge_sweep(h):
        at = pl.ds(pl.multiple_of(h * seg + half, 8), extra)
        value = None
        for strip in range(strips):
            start = pl.multiple_of(h * half + strip * depth, 8)
            rows = rho_edges[pl.ds(start, depth)].T
            for j in range(planes):
                to = pl.ds(h * seg + half + 2 * strip, 2)
                y_ref[j, to] = rows[2 * j : 2 * j + 2]
        spare = extra - 2 * strips
        y_ref[:, pl.ds(h * seg + half + 2 * strips, spare)] = jnp.zeros((planes, spare, depth), F32)
        for j in range(planes):
            rhs = y_ref[j, at]
            value = rhs if j == 0 else rhs + ahead[j - 1] * value
            y_ref[j, at] = value
        last = pivot[planes - 1] * value
        first = back_sweep(at, value)
        return first, last

    def remote(source, target, send, recv, peer):
        whom = peer if isinstance(peer, dict) else {"pencil": peer}
        return pltpu.make_async_remote_copy(
            src_ref=source, dst_ref=target, send_sem=send, recv_sem=recv,
            device_id=whom, device_id_type=MESH,
        )

    def rows_at(c, shift=0):
        return pl.ds(pl.multiple_of(c * chunk + shift, 8), chunk)

    def to_pair(c):
        at = rows_at(c)
        return remote(
            pair_out.at[:, at], pair_in.at[:, at], pair_send.at[c], pair_recv.at[c], pair
        )

    def to_above(c):
        at = rows_at(c)
        return remote(up_out.at[at], up_in.at[at], up_send.at[c], up_recv.at[c], above_me)

    def to_below(c):
        at = rows_at(c)
        return remote(
            down_out.at[at], down_in.at[at], down_send.at[c], down_recv.at[c], below_me
        )

    def to_back(c, slots):
        return remote(
            back_out.at[slots, rows_at(c)], final.at[slots, rows_at(c, x * seg)],
            back_send.at[c], back_recv.at[c], pair,
        )

    def each_back(act):
        @pl.when(inside)
        def _():
            act(pl.ds(0, 2))

        @pl.when(bottom)
        def _():
            act(pl.ds(1, 1))

        @pl.when(top)
        def _():
            act(pl.ds(0, 1))

    def keep(turn, at, faces):
        first, last = faces
        if turn == 0:
            pair_out[0, at] = first
            pair_out[1, at] = last
        else:
            @pl.when(bottom & (x == 0))
            def _():
                pair_out[0, at] = last

            @pl.when(top & (x == 1))
            def _():
                pair_out[1, at] = first

    need = [min(cuts, -(-(c * chunk + chunk + 1) // step)) for c in range(chunks)]
    first_use = [next(c for c in range(chunks) if need[c] > piece) for piece in range(cuts)]

    def whole_chunk(turn, h, c):
        for piece in range(cuts):
            @pl.when(c == first_use[piece])
            def _():
                main(turn, h, piece).wait()
                other(turn, h, piece).wait()

        row = pl.multiple_of(c * chunk, 8)
        keep(turn, pl.ds(row, chunk), sweep(h, row, chunk))

    def last_chunk(turn, h):
        for piece in range(cuts):
            if first_use[piece] == chunks - 1:
                main(turn, h, piece).wait()
                other(turn, h, piece).wait()
        row = (chunks - 1) * chunk
        keep(turn, pl.ds(row, half - row), sweep(h, row, half - row))
        keep(turn, pl.ds(half, extra), edge_sweep(h))

    for h in (0, 1):
        for side in (0, 1):
            rim(h, side).wait()

    def prepare():
        tables[1].wait()
        tables[2].wait()
        for i in range(count):
            high, low = split(width_ref[i])
            mixed_ref[i, :size, :size] = high
            mixed_ref[i, :size, size:] = high
            mixed_ref[i, size:, :size] = low
            mixed_ref[i, size:, size:] = jnp.zeros_like(low)
        def spot(d, row, column):
            return depth_ref[d, row : row + 1, column : column + 1]

        for d in range(slabs):
            for k, (row, column) in enumerate(((0, 0), (0, size - 1), (size - 1, 0))):
                value = coupling[2] * spot(d, row, column)
                links[3 * d + k : 3 * d + k + 1] = jnp.broadcast_to(value, (1, depth))
        corner = spot(jnp.where(slab > 0, slab - 1, 0), size - 1, size - 1)
        corner = 2.0 * coupling[2] * jnp.where(slab > 0, corner, jnp.zeros_like(corner))
        for k, value in enumerate(
            (
                corner, corner * coupling[2] * spot(slab, 0, 0),
                corner * coupling[2] * spot(slab, size - 1, 0),
            )
        ):
            links[3 * slabs + k : 3 * slabs + k + 1] = jnp.broadcast_to(value, (1, depth))
        first_high, first_low = split(depth_ref[slab, 0:1])
        last_high, last_low = split(depth_ref[slab, size - 1 : size])
        nothing = jnp.zeros((1, depth), F32)
        at_ends[...] = rows_of(
            [
                jnp.concatenate([piece.astype(F32), tail], axis=1)
                for piece, tail in (
                    (first_high, first_high.astype(F32)), (last_high, last_high.astype(F32)),
                    (first_low, nothing), (last_low, nothing),
                )
            ],
            2 * depth,
        )
        high, low = split(depth_ref[slab])
        mixed_depth[:size, :size] = high
        mixed_depth[size:, :size] = high
        mixed_depth[:size, size:] = low
        mixed_depth[size:, size:] = jnp.zeros_like(low)

    @pl.when(z == 0)
    def _():
        up_in[...] = jnp.zeros_like(up_in)

    @pl.when(z == outer - 1)
    def _():
        down_in[...] = jnp.zeros_like(down_in)

    def faces_of(c):
        at, mine = rows_at(c), rows_at(c, x * seg)
        own_first, own_last = y_ref[0, mine], y_ref[planes - 1, mine]
        its_first, its_last = pair_in[0, at], pair_in[1, at]
        lower = x == 0
        return (
            jnp.where(lower, own_first, its_first),
            jnp.where(lower, own_last, its_last),
            jnp.where(lower, its_first, own_first),
            jnp.where(lower, its_last, own_last),
        )

    @named("pair")
    def do_pair(c):
        to_pair(c).wait_recv()
        at = rows_at(c)
        f0, l0, f1, l1 = faces_of(c)
        block[0, at] = f0 + far * gain * (f1 + near * l0)
        block[1, at] = l1 + far * gain * (l0 + near * f1)

    @named("up")
    def do_up(c):
        @pl.when(z > 0)
        def _():
            to_above(c).wait_recv()

        at = rows_at(c)

        @pl.when(z < outer - 1)
        def _():
            up_out[at] = block[1, at] + far2 * under_gain * (up_in[at] + under * block[0, at])
            to_above(c).start()

    @named("down")
    def do_down(c):
        @pl.when(z < outer - 1)
        def _():
            to_below(c).wait_recv()

        at = rows_at(c)

        @pl.when(z > 0)
        def _():
            down_out[at] = block[0, at] + far2 * over_gain * (down_in[at] + over * block[1, at])
            to_below(c).start()

    @named("done")
    def do_final(c):
        at, mine = rows_at(c), rows_at(c, x * seg)
        low = up_in[at] + under * block[0, at]
        high = down_in[at] + over * block[1, at]
        enter = k_uu * low + k_uo * high
        leave = k_ou * low + k_oo * high
        f0, l0, f1, l1 = faces_of(c)
        l0 = l0 + far * enter
        f1 = f1 + far * leave
        inner_low = gain * (l0 + near * f1)
        inner_high = gain * (f1 + near * l0)
        lower = x == 0
        final[0, mine] = jnp.where(lower, enter, inner_low)
        final[1, mine] = jnp.where(lower, inner_high, leave)
        back_out[0, at] = jnp.where(lower, inner_low, enter)
        back_out[1, at] = jnp.where(lower, leave, inner_high)
        each_back(lambda slots: to_back(c, slots).start())

    def blocks_at(i):
        return pl.ds(i // strips * seg + i % strips * size, size)

    @named("mid")
    def solve_planes(index):
        base = index * group
        rhs = jnp.concatenate(
            [
                jnp.concatenate(
                    [
                        y_ref[base + g, blocks_at(i)]
                        - 2.0 * rho_ref[base + g, pl.ds(pad + i * size, size)]
                        for i in range(count)
                    ],
                    axis=0,
                )
                for g in range(group)
            ],
            axis=1,
        )
        solved = width_solve(rhs, coupling[0], width_ref, mixed_ref)
        answers = [
            depth_solve(solved[:, g * depth : (g + 1) * depth], mixed_depth) for g in range(group)
        ]
        for g in range(group):
            z_ref[base + g] = answers[g] + rho_ref[base + g, pl.ds(pad, width)]
            rolled = pltpu.roll(answers[g], 2 * (base + g) + 1, 1)
            z_edges[...] = jnp.where(lax.div(lane, 2) == base + g, rolled, z_edges[...])

    def turn_rows(source, i, rows):
        turned[i] = source[pl.ds(i * size, size)].T[: turned.shape[1]]
        return [turned[i, pl.ds(edge, rows, stride=2)] for edge in (1, 0)]

    def link(d, row, column):
        return like(3 * d + 2 * (row > 0) + (column > 0))

    def like(number, lanes=width):
        return jnp.concatenate([links[number : number + 1]] * (lanes // depth), axis=1)

    def with_edges(edge, ends_value, v_first, v_own):
        return ends_value + 2.0 * v_own + like(3 * slabs + 1 + (edge > 0), v_first.shape[1]) * v_first

    @named("early")
    def early_edges():
        pieces = []
        for i in range(count):
            h, strip = i // strips, i % strips
            rows = [
                y_ref[:, h * seg + half + 2 * strip + 1 - edge, :] for edge in (0, 1)
            ]
            pieces.append(jnp.concatenate(rows, axis=0))
        value = jnp.concatenate(rows_solve(pieces, coupling[0], width_ref, mixed_ref), axis=1)
        first, last = value[:planes], value[planes:]
        carries[0] = first
        lines = [turn_rows(z_edges, i, planes) for i in range(count)]
        lines = [jnp.concatenate([line[edge] for line in lines], axis=1) for edge in (0, 1)]
        ends[0] = with_edges(0, lines[0], first, first)
        ends[1] = with_edges(1, lines[1], first, last)
        for k in range(1, slabs):
            early(k).start()
        gathered[slab] = ends[...]

    def early(k):
        return remote(
            ends, gathered.at[slab], early_send.at[k - 1], early_recv.at[k - 1],
            {"slab": lax.rem(slab + k, slabs)},
        )

    def late_own(k):
        return remote(
            late.at[pl.ds(0, 6)], late_in.at[x, slab, pl.ds(0, 6)],
            own_send.at[k - 1], own_recv.at[k - 1], {"slab": lax.rem(slab + k, slabs)},
        )

    def late_cross(k):
        return remote(
            late.at[pl.ds(8, 6)], late_in.at[x, slab, pl.ds(0, 6)],
            cross_send.at[k], cross_recv.at[k],
            {"pencil": pair, "slab": lax.rem(slab + k, slabs)},
        )

    @named("late_edges")
    def late_edges():
        for who in range(2):
            for side in range(2):
                if who == 0:
                    plane = final[side, pl.ds(pl.multiple_of(x * seg, 8), half)]
                    rows = final[side, pl.ds(pl.multiple_of(x * seg + half, 8), extra)]
                else:
                    plane = back_out[side, pl.ds(0, half)]
                    rows = back_out[side, pl.ds(half, extra)]
                lines = dot(at_ends[...], both(plane, 1), ((1,), (1,)))
                first, last = lines[0:1] + lines[2:3], lines[1:2] + lines[3:4]
                v_last, v_first = (
                    jnp.concatenate(
                        [rows[2 * strip + k : 2 * strip + k + 1] for strip in range(strips)], axis=1
                    )
                    for k in (0, 1)
                )
                row = 8 * who + side
                late[row : row + 1] = with_edges(0, first, v_first, v_first)
                late[row + 2 : row + 3] = with_edges(1, last, v_first, v_last)
                late[row + 4 : row + 5] = v_first
        for k in range(1, slabs):
            late_own(k).start()
        for k in range(slabs):
            late_cross(k).start()
        late_in[x, slab, 0:6] = late[0:6]

    def chain(first_of, last_of, v_first):
        zero = jnp.zeros_like(v_first)
        forward = [zero]
        for d in range(slabs - 1):
            forward.append(last_of(d) + link(d, size - 1, 0) * forward[d])
        backward = [zero] * slabs
        for d in range(slabs - 1, 0, -1):
            backward[d - 1] = (
                first_of(d) + link(d, 0, 0) * forward[d] + link(d, 0, size - 1) * backward[d]
            )
        carry_in, carry_next = forward[0], backward[0]
        for d in range(1, slabs):
            carry_in = jnp.where(slab == d, forward[d], carry_in)
            carry_next = jnp.where(slab == d, backward[d], carry_next)
        return carry_in + like(3 * slabs) * v_first, carry_next

    reach = lag * (outer - 1)
    settle = 3
    heavy = chunks - 1
    ticks = max(settle + chunks + reach, heavy + groups + 1)

    def tick(t, unused):
        @pl.when(t < chunks - 1)
        def _():
            whole_chunk(0, 1 - x, t)

        @pl.when(t == chunks - 1)
        def _():
            last_chunk(0, 1 - x)

        @pl.when(t == 0)
        def _():
            @pl.when(inside)
            def _():
                pl.semaphore_wait(barrier, 3 + 2 * (slabs - 1))

            @pl.when(jnp.logical_not(inside))
            def _():
                pl.semaphore_wait(barrier, 2 + 2 * (slabs - 1))

        @pl.when((t < chunks) & jnp.logical_not(gives_more))
        def _():
            to_pair(t).start()

        @pl.when(t < chunks - 1)
        def _():
            whole_chunk(1, x, t)

        @pl.when(t == chunks - 1)
        def _():
            last_chunk(1, x)
            prepare()

        @pl.when((t < chunks) & gives_more)
        def _():
            to_pair(t).start()

        @pl.when((t >= settle) & (t < settle + chunks))
        def _():
            do_pair(t - settle)

        def chunk_after(hops):
            number = t - settle - lag * hops
            return jnp.where(number < chunks, number, -1)

        up = chunk_after(z)
        down = chunk_after(outer - 1 - z)
        done = chunk_after(jnp.maximum(z, outer - 1 - z))

        @pl.when(up >= 0)
        def _():
            do_up(up)

        @pl.when(down >= 0)
        def _():
            do_down(down)

        @pl.when(done >= 0)
        def _():
            do_final(done)

        @pl.when(done == chunks - 1)
        def _():
            late_edges()

        @pl.when((t >= heavy) & (t < heavy + groups))
        def _():
            solve_planes(t - heavy)

        @pl.when(t == heavy + groups)
        def _():
            early_edges()

        return unused

    lax.fori_loop(0, ticks, tick, 0)

    with jax.named_scope("early_wait"):
        for k in range(1, slabs):
            early(k).wait()
    wide = 4
    in_row = coupling[2] * depth_ref[slab, 0:1]
    next_row = coupling[2] * depth_ref[slab, size - 1 : size]
    (in_high, in_low), (next_high, next_low) = split(in_row), split(next_row)
    spots = lax.broadcasted_iota(jnp.int32, (2 * depth, depth), 0)
    number, spot = lax.div(spots, planes), lax.rem(spots, planes)
    lows = depth // planes
    base = jnp.zeros((2 * depth, depth), F32)
    for k, piece in (
        (0, in_high), (1, next_high), (2, in_low), (3, next_low),
        (lows, in_high), (lows + 1, next_high),
    ):
        base = jnp.where(number == k, piece.astype(F32), base)
    carry_in, carry_next = chain(
        lambda d: gathered[d, 0], lambda d: gathered[d, 1], carries[0]
    )
    lines = jnp.concatenate([carry_in, carry_next] * 2, axis=0)
    lines = jnp.concatenate([lines, jnp.zeros((depth - 4 * planes, width), F32)], axis=0)
    for i in range(count):
        part = slice(i * size, (i + 1) * size)
        columns[part] = both(lines[:, part].T, 1)

    @named("fix")
    def finish_planes(index, unused):
        j = index * wide
        rhs = jnp.concatenate([jnp.where(spot == j + g, base, 0.0) for g in range(wide)], axis=1)
        both_planes = dot(columns[...], rhs.astype(BF16), ((1,), (0,)))
        for g in range(wide):
            z_ref[j + g] = z_ref[j + g] + both_planes[:, g * depth : (g + 1) * depth]
        return unused

    lax.fori_loop(0, planes // wide, finish_planes, 0)
    def depth_part(h):
        for side in range(2):
            rows = final[side, pl.ds(pl.multiple_of(h * seg, 8), half)]
            to = pl.ds(pl.multiple_of(h * half, 8), half)
            face_ref[side, to] = depth_solve(rows, mixed_depth)

    depth_part(x)

    @named("back")
    def wait_back(c, unused):
        each_back(lambda slots: to_back(c, slots).wait())
        at, theirs = rows_at(c), rows_at(c, (1 - x) * seg)

        @pl.when(bottom & (x == 0))
        def _():
            final[0, theirs] = jnp.zeros((chunk, depth), F32)

        @pl.when(bottom & (x == 1))
        def _():
            leave = y_ref[0, theirs] + far * final[1, theirs]
            final[0, theirs] = gain * (pair_in[0, at] + near * leave)

        @pl.when(top & (x == 0))
        def _():
            enter = y_ref[planes - 1, theirs] + far * final[0, theirs]
            final[1, theirs] = gain * (pair_in[1, at] + near * enter)

        @pl.when(top & (x == 1))
        def _():
            final[1, theirs] = jnp.zeros((chunk, depth), F32)

        return unused

    lax.fori_loop(0, chunks, wait_back, 0)
    with jax.named_scope("late_depth"):
        depth_part(1 - x)

    with jax.named_scope("late_wait"):
        for k in range(1, slabs):
            late_own(k).wait()
        for k in range(slabs):
            late_cross(k).wait()

    def late_rows(d, row):
        return jnp.concatenate([late_in[h, d, row : row + 2] for h in range(2)], axis=1)

    with jax.named_scope("late_chain"):
        carry_in, carry_next = chain(
            lambda d: late_rows(d, 0), lambda d: late_rows(d, 2), late_rows(slab, 4)
        )
        pieces = []
        for side in range(2):
            (a_high, a_low), (b_high, b_low) = split(carry_in[side : side + 1]), split(carry_next[side : side + 1])
            pieces += [a_high, a_low, a_high, b_high, b_low, b_high]
        six = (in_high, in_high, in_low, next_high, next_high, next_low)
        blank = jnp.zeros((1, depth), F32)
        row_pairs = [jnp.concatenate([piece.astype(F32), blank], axis=1) for piece in six]
        row_pairs += [jnp.concatenate([blank, piece.astype(F32)], axis=1) for piece in six]
        spread = dot(rows_of(pieces, width), rows_of(row_pairs, 2 * depth), ((0,), (0,)))

    with jax.named_scope("late_solve"):
        sides = [face_ref[side] + spread[:, side * depth : (side + 1) * depth] for side in range(2)]
        solved = width_solve(jnp.concatenate(sides, axis=1), coupling[0], width_ref, mixed_ref)
        for side in range(2):
            face_ref[side] = solved[:, side * depth : (side + 1) * depth]

    @named("sent")
    def wait_sent(c, unused):
        to_pair(c).wait_send()

        @pl.when(z < outer - 1)
        def _():
            to_above(c).wait_send()

        @pl.when(z > 0)
        def _():
            to_below(c).wait_send()

        return unused

    lax.fori_loop(0, chunks, wait_sent, 0)


def finish_kernel(parts, z_ref, face_ref, coef_ref, out_hbm, out_ref, sem):
    planes, width, depth = z_ref.shape
    rows = width // parts

    def store(c):
        at = pl.ds(pl.multiple_of(c * rows, 8), rows)
        return pltpu.make_async_copy(out_ref.at[:, at], out_hbm.at[:, at], sem.at[c])

    def part(c, unused):
        at = pl.ds(pl.multiple_of(c * rows, 8), rows)
        enter, leave = face_ref[0, at], face_ref[1, at]
        for j in range(planes):
            k = planes - 1 - j
            out_ref[j, at] = z_ref[j, at] + coef_ref[j : j + 1] * enter + coef_ref[k : k + 1] * leave
        store(c).start()
        return unused

    lax.fori_loop(0, parts, part, 0)

    def drain(c, unused):
        store(c).wait()
        return unused

    lax.fori_loop(0, parts, drain, 0)


def per_device(density, source, coupling, width_inverse, height_inverse, depth_inverse):
    planes, width, depth = density.shape
    pencils, slabs = lax.axis_size("pencil"), lax.axis_size("slab")
    blocks, size = width_inverse.shape[:2]
    group = 2
    half = width // 2
    extra = -(-2 * half // depth // 8) * 8
    seg = half + extra
    chunks = next(k for k in range(5, seg) if seg // 8 % k == 0)
    chunk = seg // chunks
    vmem = pl.BlockSpec(memory_space=pltpu.VMEM)
    hbm = pl.BlockSpec(memory_space=pl.ANY)
    far = pl.BlockSpec(memory_space=pltpu.HBM)
    dma = pltpu.SemaphoreType.DMA
    field = jax.ShapeDtypeStruct((planes, width, depth), F32)
    faces = jax.ShapeDtypeStruct((2, width, depth), F32)
    table = jax.ShapeDtypeStruct((planes, depth), F32)
    line = pltpu.VMEM((seg, depth), F32)
    two = pltpu.VMEM((2, seg, depth), F32)
    steps = dma((chunks,))
    peers = dma((slabs - 1,))
    operands = (coupling, density, source, width_inverse, depth_inverse)
    z, face, table = pl.pallas_call(
        lambda *refs: step_kernel(group, pencils, slabs, chunk, 4, *refs),
        out_shape=(field, faces, table),
        in_specs=[far, far, far, far, far],
        out_specs=(vmem, vmem, vmem),
        scratch_shapes=[
            pltpu.SMEM(coupling.shape, F32),
            pltpu.VMEM(width_inverse.shape, F32),
            pltpu.VMEM(depth_inverse.shape, F32),
            pltpu.VMEM((planes, width + 16, depth), F32),
            pltpu.VMEM((planes, width, depth), F32),
            pltpu.VMEM((planes, 2 * seg, depth), F32),
            pltpu.VMEM((blocks, 2 * size, 2 * size), BF16),
            pltpu.VMEM((2 * size, 2 * size), BF16),
            pltpu.VMEM((2 * depth, 2 * depth), BF16),
            pltpu.VMEM((16, 2 * depth), BF16),
            pltpu.VMEM((-(-(3 * slabs + 3) // 8) * 8, depth), F32),
            pltpu.VMEM((width, depth), F32),
            pltpu.VMEM((width, depth), F32),
            pltpu.VMEM((blocks, 2 * planes, depth), F32),
            pltpu.VMEM((width, 2 * depth), BF16),
            two, two, two, line, line, line, line, two,
            pltpu.VMEM((2, 2 * seg, depth), F32),
            pltpu.VMEM((2, planes, width), F32),
            pltpu.VMEM((slabs, 2, planes, width), F32),
            pltpu.VMEM((2, planes, width), F32),
            pltpu.VMEM((16, half), F32),
            pltpu.VMEM((2, slabs, 8, half), F32),
            dma((4 + 8 * (half // depth),)), dma((3,)),
            steps, steps, steps, steps, steps, steps, steps, steps,
            peers, peers, peers, peers, dma((slabs,)), dma((slabs,)),
        ],
        compiler_params=pltpu.CompilerParams(
            vmem_limit_bytes=44 * 1024 * 1024, collective_id=0, has_side_effects=True
        ),
    )(*[pltpu.with_memory_space_constraint(array, pltpu.HBM) for array in operands])

    parts = 16
    return pl.pallas_call(
        lambda *refs: finish_kernel(parts, *refs),
        out_shape=field,
        in_specs=[vmem, vmem, vmem],
        out_specs=hbm,
        scratch_shapes=[pltpu.VMEM((planes, width, depth), F32), dma((parts,))],
        compiler_params=pltpu.CompilerParams(vmem_limit_bytes=32 * 1024 * 1024),
    )(z, face, table)


def solution(mesh):
    in_specs = (P("pencil", None, "slab"), P("pencil", None, "slab"), P(), P(), P(), P())
    out_specs = P("pencil", None, "slab")
    return jax.shard_map(
        per_device, mesh=mesh, in_specs=in_specs, out_specs=out_specs, check_vma=False
    )
```
